32 devices in a mesh: gx: 4 (over y, x), gy: 4 (over z), gz: 2 (over core).
Axes of the slice: x: 2, y: 2, z: 4, core: 2. Of those that a mesh axis runs over, the one named last changes fastest.
Arguments:
- force: float32 [3, 128, 64, 256], P(None, 'gx', 'gy', 'gz'), may hold values from -6 to 6
- phase: int32 [128, 64, 256], P('gx', 'gy', 'gz'), may hold values from 0 to 7
- viscosity_table: float32 [8], replicated, may hold values from 0.1 to 10
- boundary_flags: int32 [6], replicated, may hold values from 0 to 1
Outputs:
- pressure: float32 [128, 64, 256], P('gx', 'gy', 'gz')
- residual: float32 [128, 64, 256], P('gx', 'gy', 'gz')
- res_norms: float32 [3], replicated
The draws below stay inside these ranges and needn't reach their ends.
Inputs may be any that keep to these rules, and one draw needn't show every extreme that they name: phase ids index viscosity_table. `boundary_flags`: 0 marks a no-slip face, 1 a free-slip face.
All inputs are finite; a program needn't handle non-finite values.
Results may differ from the reference program's by a relative error of at most 0.0003.
Values sent between devices are 32-bit elements; how exact they have to be, the bound alone decides.
No kernel may reach another device: no remote copies, remote signals or barrier semaphores. Data moves between devices by JAX's collectives and lax.ppermute only.
A program may use at most 192 MiB of HBM per device.

```python
import math
import jax
import jax.numpy as jnp
from jax import lax

ITERS = 3
SWEEPS = 4
PHASES = 8
NX = 128
NY = 64
NZ = 256


def touch_ends(values, stream_key, low, high):
    dims = values.shape
    spot = [jax.random.randint(jax.random.fold_in(stream_key, axis), (), 0, dims[axis]) for axis in range(len(dims))]
    values = values.at[tuple(spot)].set(low)
    longest = dims.index(max(dims))
    spot[longest] = (spot[longest] + 1) % dims[longest]
    return values.at[tuple(spot)].set(high)


def level_of(own_key, shape, pieces, low, largest):
    gain, own = 1.0, jax.random.fold_in(own_key, 6)
    for axis_at, blocks in pieces:
        heights = jnp.exp(jax.random.uniform(jax.random.fold_in(own, axis_at), (blocks,), jnp.float32, low / len(pieces), largest / len(pieces)))
        gain = gain * jnp.repeat(heights, shape[axis_at] // blocks).reshape([-1 if axis == axis_at else 1 for axis in range(len(shape))])
    return gain


def normal_values(stream_key, dims, spread, reach, shards=(), kind=jnp.bfloat16):
    values = jax.random.normal(stream_key, dims, jnp.float32) * spread
    if len(shards) > 0:
        values = level_of(stream_key, dims, shards, -0.22, 0.18) * values
    return jnp.clip(values, min=-reach, max=reach).astype(kind)


def setup_inputs(seed: int = 0) -> dict:
    splits = jax.random.split(jax.random.key(seed), 5)
    force = normal_values(splits[0], (3, NX, NY, NZ), 1.0, 6.0, ((1, 4), (2, 4), (3, 2)), jnp.float32)
    phase = touch_ends(jax.random.randint(splits[1], (NX, NY, NZ), 0, PHASES), jax.random.fold_in(splits[1], 1), 0, PHASES - 1).astype(jnp.int32)
    viscosity_table = jnp.clip(jnp.exp(jax.random.uniform(splits[2], (PHASES,), jnp.float32, math.log(0.1), math.log(10.0))), 0.1, 10.0)
    boundary_flags = touch_ends(jax.random.randint(splits[3], (6,), 0, 2), jax.random.fold_in(splits[3], 1), 0, 1).astype(jnp.int32)
    return dict(force=force, phase=phase, viscosity_table=viscosity_table, boundary_flags=boundary_flags)


OMEGA = 0.8


def lookup(phase, table):
    eta = jnp.zeros(phase.shape, jnp.float32)
    for level in range(table.shape[0]):
        eta = eta + jnp.where(phase == level, table[level], jnp.float32(0.0))
    return eta


def trim(array, keep):
    for dim in range(3):
        if dim != keep:
            array = lax.slice_in_dim(array, 1, array.shape[dim] - 1, axis=dim)
    return array


def coefficients(eta_wide, flags, starts, totals):
    walls = (flags == 0).astype(jnp.float32)
    inner = eta_wide[1:-1, 1:-1, 1:-1]
    faces = []
    diag = [jnp.zeros_like(inner) for comp in range(3)]
    for axis in range(3):
        length = eta_wide.shape[axis]
        spots = starts[axis] + jnp.arange(length, dtype=jnp.int32)
        inside = (spots >= 0) & (spots < totals[axis])
        shape = [1, 1, 1]
        shape[axis] = length - 2
        upper_in = inside[2:].reshape(shape)
        lower_in = inside[:-2].reshape(shape)
        sides = trim(eta_wide, axis)
        middle = lax.slice_in_dim(sides, 1, length - 1, axis=axis)
        upper = 0.5 * (middle + lax.slice_in_dim(sides, 2, length, axis=axis))
        lower = 0.5 * (middle + lax.slice_in_dim(sides, 0, length - 2, axis=axis))
        faces.append((jnp.where(upper_in, upper, 0.0), jnp.where(lower_in, lower, 0.0)))
        for comp in range(3):
            normal = 1.0 if comp == axis else 0.0
            wall_low = jnp.maximum(walls[2 * axis], normal)
            wall_high = jnp.maximum(walls[2 * axis + 1], normal)
            diag[comp] = diag[comp] + jnp.where(upper_in, upper, wall_high * inner) + jnp.where(lower_in, lower, wall_low * inner)
    return faces, jnp.stack(diag)


def viscous(wide, faces, diag):
    result = diag * wide[:, 1:-1, 1:-1, 1:-1]
    for axis in range(3):
        dim = axis + 1
        sides = wide
        for other in range(1, 4):
            if other != dim:
                sides = lax.slice_in_dim(sides, 1, sides.shape[other] - 1, axis=other)
        length = wide.shape[dim]
        result = result - faces[axis][0] * lax.slice_in_dim(sides, 2, length, axis=dim)
        result = result - faces[axis][1] * lax.slice_in_dim(sides, 0, length - 2, axis=dim)
    return result


def smooth(source, faces, diag, inverse):
    state = OMEGA * inverse * source
    for sweep in range(SWEEPS - 1):
        wide = jnp.pad(state, ((0, 0), (1, 1), (1, 1), (1, 1)))
        state = state + OMEGA * inverse * (source - viscous(wide, faces, diag))
    return state


def gradient(field):
    padded = jnp.pad(field, ((0, 1), (0, 1), (0, 1)))
    return jnp.stack([padded[1:, :-1, :-1] - field, padded[:-1, 1:, :-1] - field, padded[:-1, :-1, 1:] - field])


def divergence(velocity):
    total = jnp.zeros(velocity.shape[1:], jnp.float32)
    for axis in range(3):
        comp = velocity[axis]
        widths = [(0, 0), (0, 0), (0, 0)]
        widths[axis] = (1, 0)
        before = lax.slice_in_dim(jnp.pad(comp, widths), 0, comp.shape[axis], axis=axis)
        total = total + before - comp
    return total


def reference(force, phase, viscosity_table, boundary_flags):
    eta = lookup(phase, viscosity_table)
    faces, diag = coefficients(jnp.pad(eta, 1), boundary_flags, (-1, -1, -1), (NX, NY, NZ))
    inverse = 1.0 / diag

    def schur(field):
        return divergence(smooth(gradient(field), faces, diag, inverse))

    rhs = divergence(smooth(force, faces, diag, inverse))
    cells = float(NX * NY * NZ)
    pressure = jnp.zeros_like(rhs)
    residual = rhs
    scaled = eta * residual
    search = scaled
    gamma = jnp.sum(residual * scaled)
    squares = jnp.sum(residual * residual)
    norms = []
    for step in range(ITERS):
        norms.append(squares / cells)
        image = schur(search)
        alpha = gamma / jnp.sum(search * image)
        pressure = pressure + alpha * search
        residual = residual - alpha * image
        if step + 1 < ITERS:
            scaled = eta * residual
            gamma_new = jnp.sum(residual * scaled)
            squares = jnp.sum(residual * residual)
            search = scaled + (gamma_new / gamma) * search
            gamma = gamma_new
    return pressure, residual, jnp.stack(norms)
```

```python
import functools

import jax
import jax.numpy as jnp
from jax import lax
from jax.experimental import pallas as pl
from jax.experimental.pallas import tpu as pltpu
from jax.sharding import PartitionSpec as P

ITERS = 3
SWEEPS = 4
OMEGA = 0.8
HALO = 4
LANES = 128
F32 = jnp.float32

VMEM = pl.BlockSpec(memory_space=pltpu.VMEM)
SMEM = pl.BlockSpec(memory_space=pltpu.SMEM)


def sds(*shape):
    return jax.ShapeDtypeStruct(shape, F32)


def call(kernel, outs, ins, specs=None, scratch=(), flops=10**6, name=None):
    return pl.pallas_call(
        kernel,
        out_shape=outs,
        in_specs=specs or [VMEM] * len(ins),
        out_specs=jax.tree.map(lambda _: VMEM, outs),
        scratch_shapes=list(scratch),
        compiler_params=pltpu.CompilerParams(vmem_limit_bytes=24 * 2**20),
        cost_estimate=pl.CostEstimate(flops=flops, bytes_accessed=2**20, transcendentals=0),
        name=name,
    )(*ins)


def pick(items, index):
    value = items[0]
    for k in range(1, len(items)):
        value = jnp.where(index == k, items[k], value)
    return value


def split_z(value, core, n):
    blocks = [value[..., t * LANES : (t + 1) * LANES] for t in range(n)]
    return [pick(blocks, lax.rem(core + j, n)) for j in range(n)]


def join_own(parts, core):
    n = len(parts)
    return jnp.concatenate([pick(parts, lax.rem(t - core + n, n)) for t in range(n)], -1)


def join_received(parts, core):
    n = len(parts)
    return jnp.concatenate([pick(parts, lax.rem(core - t + n, n)) for t in range(n)], -1)


def up_y(row):
    return pltpu.roll(row, row.shape[0] - 1, 0)


def down_y(row):
    return pltpu.roll(row, 1, 0)


def up_z(row):
    return pltpu.roll(row, row.shape[1] - 1, 1)


def down_z(row):
    return pltpu.roll(row, 1, 1)


def rows_loop(start, stop, body, step=3):
    count = stop - start
    whole = count // step

    def chunk(i, carry):
        for k in range(step):
            body(start + i * step + k)
        return carry

    if whole > 1:
        lax.fori_loop(0, whole, chunk, 0)
        rest = start + whole * step
    else:
        rest = start
    for r in range(rest, stop):
        body(r)


def pair_perm(n, first):
    pairs = []
    for i in range(first, n - 1, 2):
        pairs += [(i, i + 1), (i + 1, i)]
    return pairs


def exchange(axis, n, a, b):
    return (
        lax.ppermute(a, axis, pair_perm(n, 0)),
        lax.ppermute(b, axis, pair_perm(n, 1)),
    )


def core_shift(value, n, j):
    return lax.ppermute(value, "gz", [(i, (i + j) % n) for i in range(n)])


def prep_kernel(n, force, phase, table, *outs):
    core = lax.axis_index("gz")
    rows = outs[0].shape[1]
    eta_out = outs[n]
    levels = table.shape[0]

    def one(r):
        ids = phase[r]
        eta = jnp.zeros(ids.shape, F32)
        for level in range(levels):
            eta = jnp.where(ids == level, table[level], eta)
        eta_out[r] = eta

    rows_loop(0, phase.shape[0], one, 4)
    for j in range(n):
        base = lax.rem(core + j, n) * rows

        def two(r, j=j, base=base):
            for c in range(3):
                outs[j][c, r] = force[c, base + r]
            outs[j][3, r] = eta_out[base + r]

        rows_loop(0, rows, two, 4)


def gather_kernel(n, *refs):
    parts = refs[:n]
    full, send_a, send_b = refs[n:]
    core = lax.axis_index("gz")
    odd = lax.rem(lax.axis_index("gy"), 2) == 1
    fields, rows, ys, _ = full.shape
    h = HALO

    for c in range(fields):

        def one(r, c=c):
            row = join_received([p[c, r] for p in parts], core)
            full[c, r] = row
            low, high = row[:h], row[ys - h :]
            send_a[c * rows + r] = jnp.where(odd, low, high)
            send_b[c * rows + r] = jnp.where(odd, high, low)

        rows_loop(0, rows, one, 4)
    for r in range(rows):
        line = full[3, r, ys - h - 1 : ys - h, :]
        send_a[fields * rows + r // 4, r % 4 : r % 4 + 1, :] = line
        send_b[fields * rows + r // 4, r % 4 : r % 4 + 1, :] = line


def force_edges_kernel(full, got_a, got_b, send_a, send_b):
    odd_y = lax.rem(lax.axis_index("gy"), 2) == 1
    place = lax.axis_index("gx") * lax.axis_size("gz") + lax.axis_index("gz")
    odd_x = lax.rem(place, 2) == 1
    fields, rows, ys, _ = full.shape
    h = HALO
    for send, first in ((send_a, odd_x), (send_b, jnp.logical_not(odd_x))):
        start = jnp.where(first, 0, rows - h)
        for c in range(fields):
            for k in range(h):
                r = start + k
                t = 3 * (c * h + k)
                row = full[c, r]
                a, b = got_a[c * rows + r], got_b[c * rows + r]
                send[t] = row[:8]
                send[t + 1] = row[8:]
                send[t + 2, :4, :] = jnp.where(odd_y, b, a)
                send[t + 2, 4:, :] = jnp.where(odd_y, a, b)
        t = 3 * fields * h
        r = jnp.where(first, h, rows - h - 1)
        row = full[3, r]
        a, b = got_a[3 * rows + r], got_b[3 * rows + r]
        send[t] = row[:8]
        send[t + 1] = row[8:]
        send[t + 2, :4, :] = jnp.where(odd_y, b, a)
        send[t + 2, 4:, :] = jnp.where(odd_y, a, b)
        line = fields * rows + start // 4
        send[t + 3, :4, :] = jnp.where(odd_y, got_a[line], got_b[line])
        send[t + 3, 4:, :] = jnp.zeros_like(send[t + 3, 4:, :])


def edges_kernel(p, got_a, got_b, send_a, send_b):
    odd_y = lax.rem(lax.axis_index("gy"), 2) == 1
    place = lax.axis_index("gx") * lax.axis_size("gz") + lax.axis_index("gz")
    odd_x = lax.rem(place, 2) == 1
    rows, ys, _ = p.shape
    h = HALO
    for send, first in ((send_a, odd_x), (send_b, jnp.logical_not(odd_x))):
        start = jnp.where(first, 0, rows - h)
        for k in range(h):
            r = start + k
            a, b = got_a[r], got_b[r]
            send[k, :ys, :] = p[r]
            send[k, ys : ys + h, :] = jnp.where(odd_y, b, a)
            send[k, ys + h :, :] = jnp.where(odd_y, a, b)


def sweep(source, target, b, w, kx, ky, kz, start, stop):
    keep = 1.0 - OMEGA

    def one(r):
        here_x, past_x, here_y, here_z = kx[r], kx[r - 1], ky[r], kz[r]
        for c in range(3):
            u = source[c, r]
            near = here_x * source[c, r + 1] + past_x * source[c, r - 1]
            near = near + here_y * up_y(u) + down_y(here_y * u)
            near = near + here_z * up_z(u) + down_z(here_z * u)
            target[c, r] = keep * u + (b[c, r] + w[c, r] * near)

    rows_loop(start, stop, one)


def solve_and_diverge(b, one_buf, two_buf, w, kx, ky, kz, emit):
    total = b.shape[1]
    source, target = b, one_buf
    for s in range(1, SWEEPS):
        sweep(source, target, b, w, kx, ky, kz, s, total - 1 - s)
        source, target = target, (two_buf if s % 2 == 1 else one_buf)
    v = source
    h = SWEEPS

    def one(r):
        vy, vz = v[1, r], v[2, r]
        lane = lax.broadcasted_iota(jnp.int32, vz.shape, 1)
        out = v[0, r - 1] - v[0, r]
        out = out + (down_y(vy) - vy)
        out = out + (jnp.where(lane == 0, 0.0, down_z(vz)) - vz)
        emit(r - h, out)

    rows_loop(h, total - h, one, 2)


def emit_result(v_own, v_others, p_out, send_a, send_b, eta_at, sums):
    n = 1 + len(v_others)
    core = lax.axis_index("gz")
    odd = lax.rem(lax.axis_index("gy"), 2) == 1
    h = HALO

    def emit(r, out):
        ys = v_own.shape[1]
        out = out[:ys]
        parts = split_z(out, core, n)
        v_own[r] = parts[0]
        for ref, part in zip(v_others, parts[1:]):
            ref[r] = part
        p = eta_at(r) * out
        if p_out is not None:
            p_out[r] = p
            low, high = p[:h], p[ys - h :]
            send_a[r] = jnp.where(odd, low, high)
            send_b[r] = jnp.where(odd, high, low)
        sums(r, out, p)

    return emit


def fold(acc, moment, index):
    value = acc[index]
    total = value[:8]
    for k in range(1, value.shape[0] // 8):
        total = total + value[8 * k : 8 * k + 8]
    lanes = total[:, :LANES]
    for t in range(1, total.shape[1] // LANES):
        lanes = lanes + total[:, t * LANES : (t + 1) * LANES]
    moment[index] = lanes


def first_kernel(n, sizes, *refs):
    full, ya, yb, xa, xb, flags = refs[:6]
    v_own, *rest = refs[6:]
    v_others, rest = rest[: n - 1], rest[n - 1 :]
    p_out, send_a, send_b, moment, kx, ky, kz, w = rest[:8]
    force, eta, line, b, one_buf, two_buf, acc = rest[8:]
    fields, rows, ys, lanes = full.shape
    h = HALO
    odd_y = lax.rem(lax.axis_index("gy"), 2) == 1
    place = lax.axis_index("gx") * lax.axis_size("gz") + lax.axis_index("gz")
    odd_x = lax.rem(place, 2) == 1
    slots = ys + 2 * h
    total = rows + 2 * h

    def set_row(ref, index, row, a, b_):
        ref[(*index, slice(0, ys), slice(None))] = row
        ref[(*index, slice(ys, ys + h), slice(None))] = jnp.where(odd_y, b_, a)
        ref[(*index, slice(ys + h, slots), slice(None))] = jnp.where(odd_y, a, b_)

    for c in range(fields):

        def one(r, c=c):
            row, a, b_ = full[c, r], ya[c * rows + r], yb[c * rows + r]
            if c < 3:
                set_row(force, (c, r + h), row, a, b_)
            else:
                set_row(eta, (r + h + 1,), row, a, b_)

        rows_loop(0, rows, one, 4)
        for k in range(h):
            t = 3 * (c * h + k)
            for q in range(3):
                a, b_ = xa[t + q], xb[t + q]
                lower, upper = jnp.where(odd_x, a, b_), jnp.where(odd_x, b_, a)
                where = slice(8 * q, 8 * q + 8)
                if c < 3:
                    force[c, k, where, :] = lower
                    force[c, h + rows + k, where, :] = upper
                else:
                    eta[1 + k, where, :] = lower
                    eta[1 + h + rows + k, where, :] = upper
    t = 3 * fields * h
    for q in range(3):
        eta[0, 8 * q : 8 * q + 8, :] = jnp.where(odd_x, xa[t + q], xb[t + q])
    lower = jnp.where(odd_x, xa[t + 3], xb[t + 3])
    upper = jnp.where(odd_x, xb[t + 3], xa[t + 3])
    for k in range(h):
        line[k] = lower[k : k + 1]
        line[h + rows + k] = upper[k : k + 1]
    for q in range(rows // 4):
        block = jnp.where(odd_y, ya[fields * rows + q], yb[fields * rows + q])
        for k in range(4):
            line[h + 4 * q + k] = block[k : k + 1]

    first_x = place * rows - h
    first_y = lax.axis_index("gy") * ys
    slot = lax.broadcasted_iota(jnp.int32, (slots, lanes), 0)
    at_y = first_y + slot - jnp.where(slot >= ys + h, slots, 0)
    at_z = lax.broadcasted_iota(jnp.int32, (slots, lanes), 1)
    in_y = (at_y >= 0) & (at_y < sizes[1])
    y_up, y_low = at_y + 1 < sizes[1], at_y >= 1
    z_up, z_low = at_z + 1 < sizes[2], at_z >= 1
    wall = [jnp.where(flags[k] == 0, 1.0, 0.0).astype(F32) for k in range(6)]

    def coefs(r):
        mid, before, after = eta[r + 1], eta[r], eta[jnp.minimum(r + 2, total)]
        at_x = first_x + r
        x_up = jnp.full(mid.shape, at_x + 1, jnp.int32) < sizes[0]
        x_low = jnp.full(mid.shape, at_x, jnp.int32) >= 1
        inside = in_y & jnp.broadcast_to((at_x >= 0) & (at_x < sizes[0]), mid.shape)
        y_before = jnp.where(slot == ys + h, line[r], down_y(mid))
        sides = (
            (x_up, after, x_low, before),
            (y_up, up_y(mid), y_low, y_before),
            (z_up, up_z(mid), z_low, down_z(mid)),
        )
        diag = [jnp.zeros_like(mid) for _ in range(3)]
        for axis, (up_in, up, low_in, low) in enumerate(sides):
            up, low = 0.5 * (mid + up), 0.5 * (mid + low)
            (kx, ky, kz)[axis][r] = jnp.where(up_in, up, 0.0)
            for c in range(3):
                low_wall = 1.0 if c == axis else wall[2 * axis]
                up_wall = 1.0 if c == axis else wall[2 * axis + 1]
                diag[c] = diag[c] + jnp.where(up_in, up, up_wall * mid)
                diag[c] = diag[c] + jnp.where(low_in, low, low_wall * mid)
        for c in range(3):
            weight = jnp.where(inside, OMEGA / diag[c], 0.0)
            w[c, r] = weight
            b[c, r] = weight * force[c, r]

    rows_loop(0, total, coefs, 1)
    acc[...] = jnp.zeros_like(acc)

    def sums(r, v, p):
        acc[0] = acc[0] + v * p
        acc[1] = acc[1] + v * v

    emit = emit_result(v_own, v_others, p_out, send_a, send_b, lambda r: full[3, r], sums)
    solve_and_diverge(b, one_buf, two_buf, w, kx, ky, kz, emit)
    for k in range(2):
        fold(acc, moment, k)


def next_kernel(n, step, *refs):
    p_in, ya, yb, xa, xb, full, kx, ky, kz, w = refs[:10]
    refs = refs[10:]
    earlier = [refs[k * n : (k + 1) * n] for k in range(step if step < ITERS else 0)]
    refs = refs[len(earlier) * n :]
    v_own, v_others, refs = refs[0], refs[1:n], refs[n:]
    if step < ITERS:
        p_out, send_a, send_b, refs = refs[0], refs[1], refs[2], refs[3:]
    else:
        p_out = send_a = send_b = None
    moment, p, b, one_buf, two_buf, acc = refs
    rows, ys, lanes = p_in.shape
    h = HALO
    core = lax.axis_index("gz")
    odd_y = lax.rem(lax.axis_index("gy"), 2) == 1
    place = lax.axis_index("gx") * lax.axis_size("gz") + lax.axis_index("gz")
    odd_x = lax.rem(place, 2) == 1
    total = rows + 2 * h
    slots = ys + 2 * h

    def fill(r):
        a, b_ = ya[r], yb[r]
        p[r + h, :ys, :] = p_in[r]
        p[r + h, ys : ys + h, :] = jnp.where(odd_y, b_, a)
        p[r + h, ys + h :, :] = jnp.where(odd_y, a, b_)

    rows_loop(0, rows, fill, 4)
    for k in range(h):
        a, b_ = xa[k], xb[k]
        p[k] = jnp.where(odd_x, a, b_)
        p[h + rows + k] = jnp.where(odd_x, b_, a)

    def grads(r):
        mid = p[r]
        lane = lax.broadcasted_iota(jnp.int32, mid.shape, 1)
        b[0, r] = w[0, r] * (p[r + 1] - mid)
        b[1, r] = w[1, r] * (up_y(mid) - mid)
        b[2, r] = w[2, r] * (jnp.where(lane == lanes - 1, 0.0, up_z(mid)) - mid)

    rows_loop(0, total - 1, grads, 2)
    acc[...] = jnp.zeros_like(acc)

    def sums(r, v, pv):
        acc[0] = acc[0] + v * p_in[r]
        if step < ITERS:
            acc[1] = acc[1] + v * pv
            acc[2] = acc[2] + v * v
            for k, parts in enumerate(earlier):
                acc[3 + k] = acc[3 + k] + v * join_own([q[r] for q in parts], core)

    emit = emit_result(v_own, v_others, p_out, send_a, send_b, lambda r: full[3, r], sums)
    solve_and_diverge(b, one_buf, two_buf, w, kx, ky, kz, emit)
    for k in range(acc.shape[0]):
        fold(acc, moment, k)


def two_sum(a, b):
    s = a + b
    t = s - a
    return s, (a - (s - t)) + (b - t)


def quick(a, b):
    s = a + b
    return s, b - (s - a)


def halves(a):
    t = 4097.0 * a
    high = t - (t - a)
    return high, a - high


def two_prod(a, b):
    p = a * b
    ah, al = halves(a)
    bh, bl = halves(b)
    return p, ((ah * bh - p) + ah * bl + al * bh) + al * bl


def add(a, b):
    s, e = two_sum(a[0], b[0])
    return quick(s, e + (a[1] + b[1]))


def mul(a, b):
    p, e = two_prod(a[0], b[0])
    return quick(p, e + (a[0] * b[1] + a[1] * b[0]))


def neg(a):
    return -a[0], -a[1]


def div(a, b):
    q = a[0] / b[0]
    r = add(a, neg(mul((q, jnp.zeros_like(q)), b)))
    q2 = r[0] / b[0]
    return quick(q, q2)


def twice(a):
    return 2.0 * a[0], 2.0 * a[1]


def last_kernel(n, cells, sums, eta, *refs):
    own = refs[: 4 * n]
    pressure, residual, norms = refs[4 * n :]
    core = lax.axis_index("gz")
    pair = (sums[0], sums[1])
    for shift in (64, 32, 16, 8, 4, 2, 1):
        pair = add(pair, tuple(pltpu.roll(x, shift, 1) for x in pair))
    item = [(pair[0][k : k + 1], pair[1][k : k + 1]) for k in range(12)]
    m0, n00, m1, m2, n11, n01, m3, m4, n22, n02, n12, m5 = item
    one = (jnp.ones_like(m0[0]), jnp.zeros_like(m0[0]))
    a0 = div(m0, m1)
    c11 = neg(a0)
    g1 = mul(c11, add(m1, mul(c11, m2)))
    b0 = div(g1, m0)
    d10, d11 = add(one, b0), c11
    a1 = div(g1, mul(d11, add(mul(d10, m2), mul(d11, m3))))
    c21 = add(c11, neg(mul(a1, d10)))
    c22 = neg(mul(a1, d11))
    g2 = mul(c22, add(m2, add(mul(c21, m3), mul(c22, m4))))
    b1 = div(g2, g1)
    d20 = add(one, mul(b1, d10))
    d21 = add(c21, mul(b1, d11))
    d22 = c22
    a2 = div(g2, mul(d22, add(mul(d20, m3), add(mul(d21, m4), mul(d22, m5)))))
    p0 = add(a0, add(mul(a1, d10), mul(a2, d20)))[0]
    p1 = add(mul(a1, d11), mul(a2, d21))[0]
    p2 = mul(a2, d22)[0]
    r1 = add(c21, neg(mul(a2, d20)))[0]
    r2 = add(c22, neg(mul(a2, d21)))[0]
    r3 = -p2
    norm1 = add(n00, mul(c11, add(twice(n01), mul(c11, n11))))
    norm2 = add(n00, mul(c21, add(twice(n01), mul(c21, n11))))
    norm2 = add(norm2, mul(c22, add(twice(n02), add(mul(twice(c21), n12), mul(c22, n22)))))
    row = lax.broadcasted_iota(jnp.int32, norms.shape, 0)
    value = jnp.where(row == 0, n00[0], jnp.where(row == 1, norm1[0], norm2[0]))
    norms[...] = value / cells
    rows = own[0].shape[0]
    for j in range(n):
        base = lax.rem(core - j + n, n) * rows
        v0, v1, v2, v3 = (own[k * n + j] for k in range(4))

        def one_row(r, base=base, v0=v0, v1=v1, v2=v2, v3=v3):
            x0, x1, x2, x3 = v0[r], v1[r], v2[r], v3[r]
            pressure[base + r] = eta[base + r] * (p0 * x0 + p1 * x1 + p2 * x2)
            residual[base + r] = (x0 + r1 * x1) + (r2 * x2 + r3 * x3)

        rows_loop(0, rows, one_row, 4)


def sums_kernel(m0, m1, m2, m3, out):
    at = 0
    for ref in (m0, m1, m2, m3):
        for k in range(ref.shape[0]):
            out[at : at + 1, :] = jnp.sum(ref[k], 0, keepdims=True)
            at += 1
    out[at:, :] = jnp.zeros_like(out[at:, :])


def reduce_all(value, counts):
    pair = jnp.stack([value, jnp.zeros_like(value)])
    for axis, n in counts:
        step = 1
        while step < n:
            other = lax.ppermute(pair, axis, [(i, i ^ step) for i in range(n)])
            s, e = two_sum(pair[0], other[0])
            pair = jnp.stack([s, e + (pair[1] + other[1])])
            step *= 2
    return pair


def per_device(nx, ny, nz, force, phase, table, flags):
    h = HALO
    wide, ys, lanes = phase.shape
    rows = wide // nz
    zs = lanes * nz
    sizes = (wide * nx, ys * ny, zs)
    slots, total = ys + 2 * h, rows + 2 * h
    cells = float(sizes[0] * sizes[1] * sizes[2])
    chain = nx * nz

    parts = call(
        functools.partial(prep_kernel, nz),
        [sds(4, rows, ys, lanes)] * nz + [sds(*phase.shape)],
        (force, phase, table),
        [VMEM, VMEM, SMEM],
        name="prep",
    )
    eta = parts[-1]
    parts = [parts[0]] + [core_shift(parts[j], nz, j) for j in range(1, nz)]
    edge = sds(4 * rows + rows // 4, h, zs)
    full, ya, yb = call(
        functools.partial(gather_kernel, nz),
        [sds(4, rows, ys, zs), edge, edge],
        parts,
        name="gather",
    )
    ya, yb = exchange("gy", ny, ya, yb)
    edge = sds(3 * 4 * h + 4, 8, zs)
    xa, xb = call(force_edges_kernel, [edge, edge], (full, ya, yb), name="force_edges")
    xa, xb = exchange(("gx", "gz"), chain, xa, xb)

    v_shape = [sds(rows, ys, lanes)] * nz
    sent = [sds(rows, ys, zs), sds(rows, h, zs), sds(rows, h, zs)]
    field = pltpu.VMEM((3, total, slots, zs), F32)
    coefs = [sds(total, slots, zs)] * 3 + [sds(3, total, slots, zs)]
    outs = call(
        functools.partial(first_kernel, nz, sizes),
        v_shape + sent + [sds(2, 8, LANES)] + coefs,
        (full, ya, yb, xa, xb, flags),
        [VMEM] * 5 + [SMEM],
        [
            field,
            pltpu.VMEM((total + 1, slots, zs), F32),
            pltpu.VMEM((total, 1, zs), F32),
            field,
            field,
            field,
            pltpu.VMEM((2, ys, zs), F32),
        ],
        name="first",
    )
    vs = [list(outs[:nz])]
    p, ya, yb, moment = outs[nz : nz + 4]
    coefs = outs[nz + 4 :]
    moments = [moment]
    for step in range(1, ITERS + 1):
        ya, yb = exchange("gy", ny, ya, yb)
        edge = sds(h, slots, zs)
        xa, xb = call(edges_kernel, [edge, edge], (p, ya, yb), name="edges")
        xa, xb = exchange(("gx", "gz"), chain, xa, xb)
        more = step < ITERS
        earlier = [q for v in vs for q in v] if more else []
        count = 3 + step if more else 1
        outs = call(
            functools.partial(next_kernel, nz, step),
            v_shape + (sent if more else []) + [sds(count, 8, LANES)],
            (p, ya, yb, xa, xb, full, *coefs, *earlier),
            None,
            [
                pltpu.VMEM((total, slots, zs), F32),
                field,
                field,
                field,
                pltpu.VMEM((count, ys, zs), F32),
            ],
            name="next",
        )
        vs.append(list(outs[:nz]))
        if more:
            p, ya, yb = outs[nz : nz + 3]
        moments.append(outs[-1])

    placed = [[v[0]] + [core_shift(v[j], nz, j) for j in range(1, nz)] for v in vs]
    flat = call(sums_kernel, sds(16, LANES), moments, name="sums")
    pair = reduce_all(flat, (("gz", nz), ("gx", nx), ("gy", ny)))
    pressure, residual, norms = call(
        functools.partial(last_kernel, nz, cells),
        [sds(*phase.shape), sds(*phase.shape), sds(8, LANES)],
        (pair, eta, *[q for v in placed for q in v]),
        name="last",
    )
    return pressure, residual, norms[:ITERS, 0]


def solution(mesh):
    placed = (P(None, "gx", "gy", "gz"), P("gx", "gy", "gz"), P(), P())
    return jax.shard_map(
        functools.partial(per_device, mesh.shape["gx"], mesh.shape["gy"], mesh.shape["gz"]),
        mesh=mesh,
        in_specs=placed,
        out_specs=(P("gx", "gy", "gz"), P("gx", "gy", "gz"), P()),
        check_vma=False,
    )
```

```python
import functools

import jax
import jax.numpy as jnp
from jax import lax
from jax.experimental import pallas as pl
from jax.experimental.pallas import tpu as pltpu
from jax.sharding import PartitionSpec as P

ITERS = 3
SWEEPS = 4
OMEGA = 0.8
HALO = 4
LANES = 128
F32 = jnp.float32

VMEM = pl.BlockSpec(memory_space=pltpu.VMEM)
SMEM = pl.BlockSpec(memory_space=pltpu.SMEM)


def sds(*shape):
    return jax.ShapeDtypeStruct(shape, F32)


def call(kernel, outs, ins, specs=None, scratch=(), flops=10**6, name=None):
    return pl.pallas_call(
        kernel,
        out_shape=outs,
        in_specs=specs or [VMEM] * len(ins),
        out_specs=jax.tree.map(lambda _: VMEM, outs),
        scratch_shapes=list(scratch),
        compiler_params=pltpu.CompilerParams(vmem_limit_bytes=24 * 2**20),
        cost_estimate=pl.CostEstimate(flops=flops, bytes_accessed=2**20, transcendentals=0),
        name=name,
    )(*ins)


def pick(items, index):
    value = items[0]
    for k in range(1, len(items)):
        value = jnp.where(index == k, items[k], value)
    return value


def split_z(value, core, n):
    blocks = [value[..., t * LANES : (t + 1) * LANES] for t in range(n)]
    return [pick(blocks, lax.rem(core + j, n)) for j in range(n)]


def join_own(parts, core):
    n = len(parts)
    return jnp.concatenate([pick(parts, lax.rem(t - core + n, n)) for t in range(n)], -1)


def join_received(parts, core):
    n = len(parts)
    return jnp.concatenate([pick(parts, lax.rem(core - t + n, n)) for t in range(n)], -1)


def up_y(row):
    return pltpu.roll(row, row.shape[0] - 1, 0)


def down_y(row):
    return pltpu.roll(row, 1, 0)


def up_z(row):
    return pltpu.roll(row, row.shape[1] - 1, 1)


def down_z(row):
    return pltpu.roll(row, 1, 1)


def rows_loop(start, stop, body, step=3):
    count = stop - start
    whole = count // step

    def chunk(i, carry):
        for k in range(step):
            body(start + i * step + k)
        return carry

    if whole > 1:
        lax.fori_loop(0, whole, chunk, 0)
        rest = start + whole * step
    else:
        rest = start
    for r in range(rest, stop):
        body(r)


def pair_perm(n, first):
    pairs = []
    for i in range(first, n - 1, 2):
        pairs += [(i, i + 1), (i + 1, i)]
    return pairs


def exchange(axis, n, a, b):
    return (
        lax.ppermute(a, axis, pair_perm(n, 0)),
        lax.ppermute(b, axis, pair_perm(n, 1)),
    )


def core_shift(value, n, j):
    return lax.ppermute(value, "gz", [(i, (i + j) % n) for i in range(n)])


def prep_kernel(n, force, phase, table, *outs):
    core = lax.axis_index("gz")
    rows = outs[0].shape[1]
    eta_out = outs[n]
    levels = table.shape[0]

    def one(r):
        ids = phase[r]
        eta = jnp.zeros(ids.shape, F32)
        for level in range(levels):
            eta = jnp.where(ids == level, table[level], eta)
        eta_out[r] = eta

    rows_loop(0, phase.shape[0], one, 4)
    for j in range(n):
        base = lax.rem(core + j, n) * rows

        def two(r, j=j, base=base):
            for c in range(3):
                outs[j][c, r] = force[c, base + r]
            outs[j][3, r] = eta_out[base + r]

        rows_loop(0, rows, two, 4)


def gather_kernel(n, *refs):
    parts = refs[:n]
    full, send_a, send_b = refs[n:]
    core = lax.axis_index("gz")
    odd = lax.rem(lax.axis_index("gy"), 2) == 1
    fields, rows, ys, _ = full.shape
    h = HALO

    for c in range(fields):

        def one(r, c=c):
            row = join_received([p[c, r] for p in parts], core)
            full[c, r] = row
            low, high = row[:h], row[ys - h :]
            send_a[c * rows + r] = jnp.where(odd, low, high)
            send_b[c * rows + r] = jnp.where(odd, high, low)

        rows_loop(0, rows, one, 4)
    for r in range(rows):
        line = full[3, r, ys - h - 1 : ys - h, :]
        send_a[fields * rows + r // 4, r % 4 : r % 4 + 1, :] = line
        send_b[fields * rows + r // 4, r % 4 : r % 4 + 1, :] = line


def force_edges_kernel(full, got_a, got_b, send_a, send_b):
    odd_y = lax.rem(lax.axis_index("gy"), 2) == 1
    place = lax.axis_index("gx") * lax.axis_size("gz") + lax.axis_index("gz")
    odd_x = lax.rem(place, 2) == 1
    fields, rows, ys, _ = full.shape
    h = HALO
    for send, first in ((send_a, odd_x), (send_b, jnp.logical_not(odd_x))):
        start = jnp.where(first, 0, rows - h)
        for c in range(fields):
            for k in range(h):
                r = start + k
                t = 3 * (c * h + k)
                row = full[c, r]
                a, b = got_a[c * rows + r], got_b[c * rows + r]
                send[t] = row[:8]
                send[t + 1] = row[8:]
                send[t + 2, :4, :] = jnp.where(odd_y, b, a)
                send[t + 2, 4:, :] = jnp.where(odd_y, a, b)
        t = 3 * fields * h
        r = jnp.where(first, h, rows - h - 1)
        row = full[3, r]
        a, b = got_a[3 * rows + r], got_b[3 * rows + r]
        send[t] = row[:8]
        send[t + 1] = row[8:]
        send[t + 2, :4, :] = jnp.where(odd_y, b, a)
        send[t + 2, 4:, :] = jnp.where(odd_y, a, b)
        line = fields * rows + start // 4
        send[t + 3, :4, :] = jnp.where(odd_y, got_a[line], got_b[line])
        send[t + 3, 4:, :] = jnp.zeros_like(send[t + 3, 4:, :])


def edges_kernel(p, got_a, got_b, send_a, send_b):
    odd_y = lax.rem(lax.axis_index("gy"), 2) == 1
    place = lax.axis_index("gx") * lax.axis_size("gz") + lax.axis_index("gz")
    odd_x = lax.rem(place, 2) == 1
    rows, ys, _ = p.shape
    h = HALO
    for send, first in ((send_a, odd_x), (send_b, jnp.logical_not(odd_x))):
        start = jnp.where(first, 0, rows - h)
        for k in range(h):
            r = start + k
            a, b = got_a[r], got_b[r]
            send[k, :ys, :] = p[r]
            send[k, ys : ys + h, :] = jnp.where(odd_y, b, a)
            send[k, ys + h :, :] = jnp.where(odd_y, a, b)


class Rows:
    def __init__(self, early, late, first, end):
        self.early, self.late, self.first, self.end = early, late, first, end

    def __getitem__(self, index):
        r = index[-1] if isinstance(index, tuple) else index
        mine = not isinstance(r, int) or not self.first <= r < self.end
        return (self.late if mine else self.early)[index]


def spans(lo, hi, total):
    full = [(s, total - 1 - s) for s in range(SWEEPS)] + [(HALO, total - HALO)]
    inner = [(lo + s, hi - s) for s in range(SWEEPS)] + [(lo + SWEEPS, hi - SWEEPS + 1)]
    inner = [i if i[0] < i[1] else (f[0], f[0]) for f, i in zip(full, inner)]
    return full, inner


def outside(full, inner):
    return list(range(full[0], inner[0])) + list(range(inner[1], full[1]))


def update(source, b, w, kx, ky, kz, target, r):
    keep = 1.0 - OMEGA
    here_x, past_x, here_y, here_z = kx[r], kx[r - 1], ky[r], kz[r]
    for c in range(3):
        u = source[c, r]
        near = here_x * source[c, r + 1] + past_x * source[c, r - 1]
        near = near + here_y * up_y(u) + down_y(here_y * u)
        near = near + here_z * up_z(u) + down_z(here_z * u)
        target[c, r] = keep * u + (b[c, r] + w[c, r] * near)


def diverge(v, r):
    vy, vz = v[1, r], v[2, r]
    lane = lax.broadcasted_iota(jnp.int32, vz.shape, 1)
    out = v[0, r - 1] - v[0, r]
    out = out + (down_y(vy) - vy)
    return out + (jnp.where(lane == 0, 0.0, down_z(vz)) - vz)


def inner_solve(b, levels, out, inner, w, kx, ky, kz):
    source = b
    for s in range(1, SWEEPS):
        target = levels[s - 1]

        def one(r, source=source, target=target):
            update(source, b, w, kx, ky, kz, target, r)

        rows_loop(*inner[s], one)
        source = target

    def last(r):
        out[r - HALO] = diverge(source, r)

    rows_loop(*inner[SWEEPS], last, 2)


def outer_solve(b, levels, buffers, inner, full, w, kx, ky, kz, emit):
    source = b
    for s in range(1, SWEEPS):
        target = buffers[s - 1]
        for r in outside(full[s], inner[s]):
            update(source, b, w, kx, ky, kz, target, r)
        source = Rows(levels[s - 1], target, *inner[s])
    for r in outside(full[SWEEPS], inner[SWEEPS]):
        emit(r - HALO, diverge(source, r))


def emit_result(v_own, v_others, p_out, send_a, send_b, eta_at, sums=None):
    n = 1 + len(v_others)
    core = lax.axis_index("gz")
    odd = lax.rem(lax.axis_index("gy"), 2) == 1
    h = HALO

    def emit(r, out):
        ys = v_own.shape[1]
        out = out[:ys]
        parts = split_z(out, core, n)
        v_own[r] = parts[0]
        for ref, part in zip(v_others, parts[1:]):
            ref[r] = part
        if p_out is not None:
            p = eta_at(r) * out
            p_out[r] = p
            low, high = p[:h], p[ys - h :]
            send_a[r] = jnp.where(odd, low, high)
            send_b[r] = jnp.where(odd, high, low)
        if sums is not None:
            sums(r, out)

    return emit


def fold(value):
    total = value[:8]
    for k in range(1, value.shape[0] // 8):
        total = total + value[8 * k : 8 * k + 8]
    lanes = total[:, :LANES]
    for t in range(1, total.shape[1] // LANES):
        lanes = lanes + total[:, t * LANES : (t + 1) * LANES]
    return lanes


def odd_places():
    place = lax.axis_index("gx") * lax.axis_size("gz") + lax.axis_index("gz")
    return lax.rem(lax.axis_index("gy"), 2) == 1, lax.rem(place, 2) == 1, place


def set_row(ref, index, row, a, b, odd_y):
    ys, h = row.shape[0], a.shape[0]
    ref[(*index, slice(0, ys), slice(None))] = row
    ref[(*index, slice(ys, ys + h), slice(None))] = jnp.where(odd_y, b, a)
    ref[(*index, slice(ys + h, ys + 2 * h), slice(None))] = jnp.where(odd_y, a, b)


def coefs_at(sizes, place, slots, lanes, rows, ys, flags):
    h = HALO
    slot = lax.broadcasted_iota(jnp.int32, (slots, lanes), 0)
    at_y = lax.axis_index("gy") * ys + slot - jnp.where(slot >= ys + h, slots, 0)
    at_z = lax.broadcasted_iota(jnp.int32, (slots, lanes), 1)
    in_y = (at_y >= 0) & (at_y < sizes[1])
    y_up, y_low = at_y + 1 < sizes[1], at_y >= 1
    z_up, z_low = at_z + 1 < sizes[2], at_z >= 1
    wall = [jnp.where(flags[k] == 0, 1.0, 0.0).astype(F32) for k in range(6)]

    def coefs(r, mid, before, after, line, force_at, kx, ky, kz, w, b):
        at_x = place * rows - h + r
        x_up = jnp.full(mid.shape, at_x + 1, jnp.int32) < sizes[0]
        x_low = jnp.full(mid.shape, at_x, jnp.int32) >= 1
        inside = in_y & jnp.broadcast_to((at_x >= 0) & (at_x < sizes[0]), mid.shape)
        y_before = jnp.where(slot == ys + h, line, down_y(mid))
        sides = (
            (x_up, after, x_low, before),
            (y_up, up_y(mid), y_low, y_before),
            (z_up, up_z(mid), z_low, down_z(mid)),
        )
        diag = [jnp.zeros_like(mid) for _ in range(3)]
        for axis, (up_in, up, low_in, low) in enumerate(sides):
            up, low = 0.5 * (mid + up), 0.5 * (mid + low)
            (kx, ky, kz)[axis][r] = jnp.where(up_in, up, 0.0)
            for c in range(3):
                low_wall = 1.0 if c == axis else wall[2 * axis]
                up_wall = 1.0 if c == axis else wall[2 * axis + 1]
                diag[c] = diag[c] + jnp.where(up_in, up, up_wall * mid)
                diag[c] = diag[c] + jnp.where(low_in, low, low_wall * mid)
        for c in range(3):
            weight = jnp.where(inside, OMEGA / diag[c], 0.0)
            w[c, r] = weight
            b[c, r] = weight * force_at(c)

    return coefs


def first_inner(sizes, full, ya, yb, flags, kx, ky, kz, w, b, *rest):
    levels, (out, force, eta, line) = rest[: SWEEPS - 1], rest[SWEEPS - 1 :]
    fields, rows, ys, lanes = full.shape
    h = HALO
    odd_y, _, place = odd_places()
    slots, total = ys + 2 * h, rows + 2 * h
    for c in range(fields):

        def one(r, c=c):
            row, a, b_ = full[c, r], ya[c * rows + r], yb[c * rows + r]
            if c < 3:
                set_row(force, (c, r + h), row, a, b_, odd_y)
            else:
                set_row(eta, (r + h,), row, a, b_, odd_y)

        rows_loop(0, rows, one, 4)
    for q in range(rows // 4):
        block = jnp.where(odd_y, ya[fields * rows + q], yb[fields * rows + q])
        for k in range(4):
            line[h + 4 * q + k] = block[k : k + 1]
    coefs = coefs_at(sizes, place, slots, lanes, rows, ys, flags)

    def at(r):
        coefs(r, eta[r], eta[r - 1], eta[r + 1], line[r], lambda c: force[c, r], kx, ky, kz, w, b)

    _, inner = spans(h + 1, h + rows - 1, total)
    rows_loop(*inner[0], at, 1)
    inner_solve(b, levels, out, inner, w, kx, ky, kz)


def first_outer(n, sizes, *refs):
    full, ya, yb, xa, xb, flags, *early = refs[: 11 + SWEEPS]
    kx0, ky0, kz0, w0, b0, *levels, out0 = early
    refs = refs[11 + SWEEPS :]
    v_own, v_others, refs = refs[0], refs[1:n], refs[n:]
    p_out, send_a, send_b, kx, ky, kz, w = refs[:7]
    force, eta, line, b, *buffers = refs[7:]
    fields, rows, ys, lanes = full.shape
    h = HALO
    odd_y, odd_x, place = odd_places()
    slots, total = ys + 2 * h, rows + 2 * h
    ranges, inner = spans(h + 1, h + rows - 1, total)
    todo = outside((0, total), inner[0])
    for r in sorted({min(max(q + d, h), h + rows - 1) for q in todo for d in (-1, 0, 1)}):
        k = r - h
        for c in range(3):
            set_row(force, (c, r), full[c, k], ya[c * rows + k], yb[c * rows + k], odd_y)
        set_row(eta, (r + 1,), full[3, k], ya[3 * rows + k], yb[3 * rows + k], odd_y)
        block = fields * rows + k // 4
        line[r] = jnp.where(odd_y, ya[block], yb[block])[k % 4 : k % 4 + 1]
    for c in range(fields):
        for k in range(h):
            t = 3 * (c * h + k)
            for q in range(3):
                a, b_ = xa[t + q], xb[t + q]
                lower, upper = jnp.where(odd_x, a, b_), jnp.where(odd_x, b_, a)
                where = slice(8 * q, 8 * q + 8)
                if c < 3:
                    force[c, k, where, :] = lower
                    force[c, h + rows + k, where, :] = upper
                else:
                    eta[1 + k, where, :] = lower
                    eta[1 + h + rows + k, where, :] = upper
    t = 3 * fields * h
    for q in range(3):
        eta[0, 8 * q : 8 * q + 8, :] = jnp.where(odd_x, xa[t + q], xb[t + q])
    lower = jnp.where(odd_x, xa[t + 3], xb[t + 3])
    upper = jnp.where(odd_x, xb[t + 3], xa[t + 3])
    for k in range(h):
        line[k] = lower[k : k + 1]
        line[h + rows + k] = upper[k : k + 1]
    coefs = coefs_at(sizes, place, slots, lanes, rows, ys, flags)
    for r in todo:
        after = eta[min(r + 2, total)]
        coefs(r, eta[r + 1], eta[r], after, line[r], lambda c: force[c, r], kx, ky, kz, w, b)

    def carry(r):
        kx[r], ky[r], kz[r] = kx0[r], ky0[r], kz0[r]
        for c in range(3):
            w[c, r] = w0[c, r]

    rows_loop(*inner[0], carry, 2)
    b = Rows(b0, b, *inner[0])
    emit = emit_result(v_own, v_others, p_out, send_a, send_b, lambda r: full[3, r])
    outer_solve(b, levels, buffers, inner, ranges, w, kx, ky, kz, emit)
    rows_loop(inner[SWEEPS][0] - h, inner[SWEEPS][1] - h, lambda r: emit(r, out0[r]), 4)


def next_inner(p_in, ya, yb, kx, ky, kz, w, p, b, *rest):
    levels, out = rest[: SWEEPS - 1], rest[SWEEPS - 1]
    rows = p_in.shape[0]
    h = HALO
    odd_y, _, _ = odd_places()

    def fill(r):
        set_row(p, (r + h,), p_in[r], ya[r], yb[r], odd_y)

    rows_loop(0, rows, fill, 4)
    _, inner = spans(h, h + rows - 1, rows + 2 * h)
    rows_loop(*inner[0], lambda r: grads(p, w, b, r), 2)
    inner_solve(b, levels, out, inner, w, kx, ky, kz)


def grads(p, w, b, r):
    mid = p[r]
    lanes = mid.shape[1]
    lane = lax.broadcasted_iota(jnp.int32, mid.shape, 1)
    b[0, r] = w[0, r] * (p[r + 1] - mid)
    b[1, r] = w[1, r] * (up_y(mid) - mid)
    b[2, r] = w[2, r] * (jnp.where(lane == lanes - 1, 0.0, up_z(mid)) - mid)


def next_outer(n, last, p_in, xa, xb, full, kx, ky, kz, w, p0, b0, *refs):
    levels, out0, refs = refs[: SWEEPS - 1], refs[SWEEPS - 1], refs[SWEEPS:]
    v_own, v_others, refs = refs[0], refs[1:n], refs[n:]
    p_out = send_a = send_b = sums = None
    if last:
        moment, refs = refs[0], refs[1:]
        acc, refs = refs[-1], refs[:-1]
        acc[...] = jnp.zeros_like(acc)

        def sums(r, v):
            acc[...] = acc[...] + v * p_in[r]
    else:
        p_out, send_a, send_b, *refs = refs
    p, b, *buffers = refs
    rows = p_in.shape[0]
    h = HALO
    _, odd_x, _ = odd_places()
    for k in range(h):
        a, b_ = xa[k], xb[k]
        p[k] = jnp.where(odd_x, a, b_)
        p[h + rows + k] = jnp.where(odd_x, b_, a)
    ranges, inner = spans(h, h + rows - 1, rows + 2 * h)
    p = Rows(p0, p, h, h + rows)
    for r in outside(ranges[0], inner[0]):
        grads(p, w, b, r)
    b = Rows(b0, b, *inner[0])
    emit = emit_result(v_own, v_others, p_out, send_a, send_b, lambda r: full[3, r], sums)
    outer_solve(b, levels, buffers, inner, ranges, w, kx, ky, kz, emit)
    rows_loop(inner[SWEEPS][0] - h, inner[SWEEPS][1] - h, lambda r: emit(r, out0[r]), 4)
    if last:
        moment[0] = fold(acc[...])


def moments_kernel(n, step, *refs):
    moment, acc = refs[-2:]
    p, refs = refs[0], refs[1:-2]
    before, refs = (refs[0], refs[1:]) if step else (None, refs)
    groups = [refs[k * n : (k + 1) * n] for k in range(step + 1)]
    core = lax.axis_index("gz")
    acc[...] = jnp.zeros_like(acc)

    def one(r):
        v = join_own([q[r] for q in groups[-1]], core)
        others = ([before[r]] if step else []) + [p[r], v]
        others += [join_own([q[r] for q in group], core) for group in groups[:-1]]
        for k, other in enumerate(others):
            acc[k] = acc[k] + v * other

    rows_loop(0, p.shape[0], one, 4)
    for k in range(acc.shape[0]):
        moment[k] = fold(acc[k])


def two_sum(a, b):
    s = a + b
    t = s - a
    return s, (a - (s - t)) + (b - t)


def quick(a, b):
    s = a + b
    return s, b - (s - a)


def halves(a):
    t = 4097.0 * a
    high = t - (t - a)
    return high, a - high


def two_prod(a, b):
    p = a * b
    ah, al = halves(a)
    bh, bl = halves(b)
    return p, ((ah * bh - p) + ah * bl + al * bh) + al * bl


def add(a, b):
    s, e = two_sum(a[0], b[0])
    return quick(s, e + (a[1] + b[1]))


def mul(a, b):
    p, e = two_prod(a[0], b[0])
    return quick(p, e + (a[0] * b[1] + a[1] * b[0]))


def neg(a):
    return -a[0], -a[1]


def div(a, b):
    q = a[0] / b[0]
    r = add(a, neg(mul((q, jnp.zeros_like(q)), b)))
    q2 = r[0] / b[0]
    return quick(q, q2)


def twice(a):
    return 2.0 * a[0], 2.0 * a[1]


def last_kernel(n, cells, sums, eta, *refs):
    own = refs[: 4 * n]
    pressure, residual, norms = refs[4 * n :]
    core = lax.axis_index("gz")
    pair = (sums[0], sums[1])
    for shift in (64, 32, 16, 8, 4, 2, 1):
        pair = add(pair, tuple(pltpu.roll(x, shift, 1) for x in pair))
    item = [(pair[0][k : k + 1], pair[1][k : k + 1]) for k in range(12)]
    m0, n00, m1, m2, n11, n01, m3, m4, n22, n02, n12, m5 = item
    one = (jnp.ones_like(m0[0]), jnp.zeros_like(m0[0]))
    a0 = div(m0, m1)
    c11 = neg(a0)
    g1 = mul(c11, add(m1, mul(c11, m2)))
    b0 = div(g1, m0)
    d10, d11 = add(one, b0), c11
    a1 = div(g1, mul(d11, add(mul(d10, m2), mul(d11, m3))))
    c21 = add(c11, neg(mul(a1, d10)))
    c22 = neg(mul(a1, d11))
    g2 = mul(c22, add(m2, add(mul(c21, m3), mul(c22, m4))))
    b1 = div(g2, g1)
    d20 = add(one, mul(b1, d10))
    d21 = add(c21, mul(b1, d11))
    d22 = c22
    a2 = div(g2, mul(d22, add(mul(d20, m3), add(mul(d21, m4), mul(d22, m5)))))
    p0 = add(a0, add(mul(a1, d10), mul(a2, d20)))[0]
    p1 = add(mul(a1, d11), mul(a2, d21))[0]
    p2 = mul(a2, d22)[0]
    r1 = add(c21, neg(mul(a2, d20)))[0]
    r2 = add(c22, neg(mul(a2, d21)))[0]
    r3 = -p2
    norm1 = add(n00, mul(c11, add(twice(n01), mul(c11, n11))))
    norm2 = add(n00, mul(c21, add(twice(n01), mul(c21, n11))))
    norm2 = add(norm2, mul(c22, add(twice(n02), add(mul(twice(c21), n12), mul(c22, n22)))))
    row = lax.broadcasted_iota(jnp.int32, norms.shape, 0)
    value = jnp.where(row == 0, n00[0], jnp.where(row == 1, norm1[0], norm2[0]))
    norms[...] = value / cells
    rows = own[0].shape[0]
    for j in range(n):
        base = lax.rem(core - j + n, n) * rows
        v0, v1, v2, v3 = (own[k * n + j] for k in range(4))

        def one_row(r, base=base, v0=v0, v1=v1, v2=v2, v3=v3):
            x0, x1, x2, x3 = v0[r], v1[r], v2[r], v3[r]
            pressure[base + r] = eta[base + r] * (p0 * x0 + p1 * x1 + p2 * x2)
            residual[base + r] = (x0 + r1 * x1) + (r2 * x2 + r3 * x3)

        rows_loop(0, rows, one_row, 4)


def sums_kernel(m0, m1, m2, m3, out):
    at = 0
    for ref in (m0, m1, m2, m3):
        for k in range(ref.shape[0]):
            out[at : at + 1, :] = jnp.sum(ref[k], 0, keepdims=True)
            at += 1
    out[at:, :] = jnp.zeros_like(out[at:, :])


def reduce_all(value, counts):
    pair = jnp.stack([value, jnp.zeros_like(value)])
    for axis, n in counts:
        step = 1
        while step < n:
            other = lax.ppermute(pair, axis, [(i, i ^ step) for i in range(n)])
            s, e = two_sum(pair[0], other[0])
            pair = jnp.stack([s, e + (pair[1] + other[1])])
            step *= 2
    return pair


def per_device(nx, ny, nz, force, phase, table, flags):
    h = HALO
    wide, ys, lanes = phase.shape
    rows = wide // nz
    zs = lanes * nz
    sizes = (wide * nx, ys * ny, zs)
    slots, total = ys + 2 * h, rows + 2 * h
    cells = float(sizes[0] * sizes[1] * sizes[2])
    chain = nx * nz

    parts = call(
        functools.partial(prep_kernel, nz),
        [sds(4, rows, ys, lanes)] * nz + [sds(*phase.shape)],
        (force, phase, table),
        [VMEM, VMEM, SMEM],
        name="prep",
    )
    eta = parts[-1]
    parts = [parts[0]] + [core_shift(parts[j], nz, j) for j in range(1, nz)]
    edge = sds(4 * rows + rows // 4, h, zs)
    full, ya, yb = call(
        functools.partial(gather_kernel, nz),
        [sds(4, rows, ys, zs), edge, edge],
        parts,
        name="gather",
    )
    ya, yb = exchange("gy", ny, ya, yb)
    edge = sds(3 * 4 * h + 4, 8, zs)
    xa, xb = call(force_edges_kernel, [edge, edge], (full, ya, yb), name="force_edges")
    xa, xb = exchange(("gx", "gz"), chain, xa, xb)

    v_shape = [sds(rows, ys, lanes)] * nz
    sent = [sds(rows, ys, zs), sds(rows, h, zs), sds(rows, h, zs)]
    scalar, vector = sds(total, slots, zs), sds(3, total, slots, zs)
    field = pltpu.VMEM((3, total, slots, zs), F32)
    line = pltpu.VMEM((total, 1, zs), F32)
    heavy = 4 * 10**7
    early = call(
        functools.partial(first_inner, sizes),
        [scalar] * 3 + [vector] * (1 + SWEEPS) + [sds(rows, slots, zs)],
        (full, ya, yb, flags),
        [VMEM] * 3 + [SMEM],
        [field, pltpu.VMEM((total, slots, zs), F32), line],
        heavy,
        "first_inner",
    )
    outs = call(
        functools.partial(first_outer, nz, sizes),
        v_shape + sent + [scalar] * 3 + [vector],
        (full, ya, yb, xa, xb, flags, *early),
        [VMEM] * 5 + [SMEM] + [VMEM] * len(early),
        [field, pltpu.VMEM((total + 1, slots, zs), F32), line] + [field] * SWEEPS,
        heavy,
        "first",
    )
    vs, ps, moments = [list(outs[:nz])], [outs[nz]], []
    ya, yb = outs[nz + 1 : nz + 3]
    coefs = outs[nz + 3 :]
    for step in range(1, ITERS + 1):
        last = step == ITERS
        p = ps[-1]
        count = 2 if step == 1 else 2 + step
        moments.append(
            call(
                functools.partial(moments_kernel, nz, step - 1),
                [sds(count, 8, LANES)],
                (p, *ps[:-1][-1:], *[q for v in vs for q in v]),
                None,
                [pltpu.VMEM((count, ys, zs), F32)],
                name="moments",
            )[0]
        )
        ya, yb = exchange("gy", ny, ya, yb)
        edge = sds(h, slots, zs)
        xa, xb = call(edges_kernel, [edge, edge], (p, ya, yb), name="edges")
        xa, xb = exchange(("gx", "gz"), chain, xa, xb)
        early = call(
            next_inner,
            [scalar] + [vector] * SWEEPS + [sds(rows, slots, zs)],
            (p, ya, yb, *coefs),
            None,
            (),
            heavy,
            "next_inner",
        )
        outs = call(
            functools.partial(next_outer, nz, last),
            v_shape + ([sds(1, 8, LANES)] if last else sent),
            (p, xa, xb, full, *coefs, *early),
            None,
            [pltpu.VMEM((total, slots, zs), F32)]
            + [field] * SWEEPS
            + ([pltpu.VMEM((ys, zs), F32)] if last else []),
            heavy,
            "next",
        )
        vs.append(list(outs[:nz]))
        if last:
            moments.append(outs[nz])
        else:
            ps.append(outs[nz])
            ya, yb = outs[nz + 1 : nz + 3]

    placed = [[v[0]] + [core_shift(v[j], nz, j) for j in range(1, nz)] for v in vs]
    flat = call(sums_kernel, sds(16, LANES), moments, name="sums")
    pair = reduce_all(flat, (("gz", nz), ("gx", nx), ("gy", ny)))
    pressure, residual, norms = call(
        functools.partial(last_kernel, nz, cells),
        [sds(*phase.shape), sds(*phase.shape), sds(8, LANES)],
        (pair, eta, *[q for v in placed for q in v]),
        name="last",
    )
    return pressure, residual, norms[:ITERS, 0]


def solution(mesh):
    placed = (P(None, "gx", "gy", "gz"), P("gx", "gy", "gz"), P(), P())
    return jax.shard_map(
        functools.partial(per_device, mesh.shape["gx"], mesh.shape["gy"], mesh.shape["gz"]),
        mesh=mesh,
        in_specs=placed,
        out_specs=(P("gx", "gy", "gz"), P("gx", "gy", "gz"), P()),
        check_vma=False,
    )
```

```python
import functools

import jax
import jax.numpy as jnp
from jax import lax
from jax.experimental import pallas as pl
from jax.experimental.pallas import tpu as pltpu
from jax.sharding import PartitionSpec as P

ITERS = 3
SWEEPS = 4
OMEGA = 0.8
HALO = 4
LANES = 128
F32 = jnp.float32

VMEM = pl.BlockSpec(memory_space=pltpu.VMEM)
SMEM = pl.BlockSpec(memory_space=pltpu.SMEM)
HBM = pl.BlockSpec(memory_space=pltpu.HBM)


def sds(*shape):
    return jax.ShapeDtypeStruct(shape, F32)


def call(kernel, outs, ins, specs=None, scratch=(), flops=10**6, name=None, out_specs=None):
    return pl.pallas_call(
        kernel,
        out_shape=outs,
        in_specs=specs or [VMEM] * len(ins),
        out_specs=out_specs or jax.tree.map(lambda _: VMEM, outs),
        scratch_shapes=list(scratch),
        compiler_params=pltpu.CompilerParams(vmem_limit_bytes=24 * 2**20),
        cost_estimate=pl.CostEstimate(flops=flops, bytes_accessed=2**20, transcendentals=0),
        name=name,
    )(*ins)


def pick(items, index):
    value = items[0]
    for k in range(1, len(items)):
        value = jnp.where(index == k, items[k], value)
    return value


def split_z(value, core, n):
    blocks = [value[..., t * LANES : (t + 1) * LANES] for t in range(n)]
    return [pick(blocks, lax.rem(core + j, n)) for j in range(n)]


def join_own(parts, core):
    n = len(parts)
    return jnp.concatenate([pick(parts, lax.rem(t - core + n, n)) for t in range(n)], -1)


def join_received(parts, core):
    n = len(parts)
    return jnp.concatenate([pick(parts, lax.rem(core - t + n, n)) for t in range(n)], -1)


def up_y(row):
    return pltpu.roll(row, row.shape[0] - 1, 0)


def down_y(row):
    return pltpu.roll(row, 1, 0)


def up_z(row):
    return pltpu.roll(row, row.shape[1] - 1, 1)


def down_z(row):
    return pltpu.roll(row, 1, 1)


def rows_loop(start, stop, body, step=3):
    count = stop - start
    whole = count // step

    def chunk(i, carry):
        for k in range(step):
            body(start + i * step + k)
        return carry

    if whole > 1:
        lax.fori_loop(0, whole, chunk, 0)
        rest = start + whole * step
    else:
        rest = start
    for r in range(rest, stop):
        body(r)


def pair_perm(n, first):
    pairs = []
    for i in range(first, n - 1, 2):
        pairs += [(i, i + 1), (i + 1, i)]
    return pairs


def exchange(axis, n, a, b):
    return (
        lax.ppermute(a, axis, pair_perm(n, 0)),
        lax.ppermute(b, axis, pair_perm(n, 1)),
    )


def core_shift(value, n, j):
    return lax.ppermute(value, "gz", [(i, (i + j) % n) for i in range(n)])


def prep_kernel(n, force, phase, table, *refs):
    parts, eta_out, ids_buf, sems = refs[:n], refs[n], refs[n + 1], refs[n + 2]
    core = lax.axis_index("gz")
    rows = parts[0].shape[1]
    levels = table.shape[0]
    fetch = pltpu.make_async_copy(phase, ids_buf, sems.at[3 * n])
    fetch.start()
    copies = []
    for j in range(n):
        base = lax.rem(core + j, n) * rows
        for c in range(3):
            source = force.at[c, pl.ds(base, rows)]
            copies.append(pltpu.make_async_copy(source, parts[j].at[c], sems.at[3 * j + c]))
            copies[-1].start()
    fetch.wait()

    def one(r):
        ids = ids_buf[r]
        eta = jnp.zeros(ids.shape, F32)
        for level in range(levels):
            eta = jnp.where(ids == level, table[level], eta)
        eta_out[r] = eta

    rows_loop(0, phase.shape[0], one, 4)
    for j in range(n):
        base = lax.rem(core + j, n) * rows

        def two(r, j=j, base=base):
            parts[j][3, r] = eta_out[base + r]

        rows_loop(0, rows, two, 4)
    for copy in copies:
        copy.wait()


def gather_kernel(n, *refs):
    parts = refs[:n]
    full, send_a, send_b = refs[n:]
    core = lax.axis_index("gz")
    odd = lax.rem(lax.axis_index("gy"), 2) == 1
    fields, rows, ys, _ = full.shape
    h = HALO

    for c in range(fields):

        def one(r, c=c):
            row = join_received([p[c, r] for p in parts], core)
            full[c, r] = row
            low, high = row[:h], row[ys - h :]
            send_a[c * rows + r] = jnp.where(odd, low, high)
            send_b[c * rows + r] = jnp.where(odd, high, low)

        rows_loop(0, rows, one, 4)
    for r in range(rows):
        line = full[3, r, ys - h - 1 : ys - h, :]
        send_a[fields * rows + r // 4, r % 4 : r % 4 + 1, :] = line
        send_b[fields * rows + r // 4, r % 4 : r % 4 + 1, :] = line


def edge_list(h):
    tiles = []
    for c in range(4):
        for k in range(h):
            if c in (1, 2) and k == 0:
                continue
            for q in range(2 if c == 0 and k == 0 else 3):
                tiles.append((c, k, q))
    return tiles + [(3, -1, 0), (3, -1, 1)]


def force_edges_kernel(full, got_a, got_b, send_a, send_b):
    odd_y, odd_x, _ = odd_places()
    _, rows, ys, _ = full.shape
    h = HALO
    for send, first in ((send_a, odd_x), (send_b, jnp.logical_not(odd_x))):
        for t, (c, k, q) in enumerate(edge_list(h)):
            r = jnp.where(first, h - 1 - k, rows - h + k)
            if q < 2:
                send[t] = full[c, r, 8 * q : 8 * q + 8, :]
            else:
                a, b = got_a[c * rows + r], got_b[c * rows + r]
                send[t, :h, :] = jnp.where(odd_y, b, a)
                send[t, h:, :] = jnp.where(odd_y, a, b)


def edges_kernel(p, got_a, got_b, *rest):
    send_a, send_b = rest[-2:]
    odd_y = lax.rem(lax.axis_index("gy"), 2) == 1
    place = lax.axis_index("gx") * lax.axis_size("gz") + lax.axis_index("gz")
    odd_x = lax.rem(place, 2) == 1
    rows, ys, _ = p.shape
    h = HALO
    for send, first in ((send_a, odd_x), (send_b, jnp.logical_not(odd_x))):
        start = jnp.where(first, 0, rows - h)
        for k in range(h):
            r = start + k
            a, b = got_a[r], got_b[r]
            send[k, :ys, :] = p[r]
            send[k, ys : ys + h, :] = jnp.where(odd_y, b, a)
            send[k, ys + h :, :] = jnp.where(odd_y, a, b)


class Rows:
    def __init__(self, early, late, first, end):
        self.early, self.late, self.first, self.end = early, late, first, end

    def __getitem__(self, index):
        r = index[-1] if isinstance(index, tuple) else index
        mine = not isinstance(r, int) or not self.first <= r < self.end
        return (self.late if mine else self.early)[index]


def spans(lo, hi, total):
    full = [(s, total - 1 - s) for s in range(SWEEPS)] + [(HALO, total - HALO)]
    inner = [(lo + s, hi - s) for s in range(SWEEPS)] + [(lo + SWEEPS, hi - SWEEPS + 1)]
    inner = [i if i[0] < i[1] else (f[0], f[0]) for f, i in zip(full, inner)]
    return full, inner


def outside(full, inner):
    return list(range(full[0], inner[0])) + list(range(inner[1], full[1]))


def update(source, b, w, kx, ky, kz, target, r):
    keep = 1.0 - OMEGA
    here_x, past_x, here_y, here_z = kx[r], kx[r - 1], ky[r], kz[r]
    for c in range(3):
        u = source[c, r]
        near = here_x * source[c, r + 1] + past_x * source[c, r - 1]
        near = near + here_y * up_y(u) + down_y(here_y * u)
        near = near + here_z * up_z(u) + down_z(here_z * u)
        target[c, r] = keep * u + (b[c, r] + w[c, r] * near)


def diverge(v, r):
    vy, vz = v[1, r], v[2, r]
    lane = lax.broadcasted_iota(jnp.int32, vz.shape, 1)
    out = v[0, r - 1] - v[0, r]
    out = out + (down_y(vy) - vy)
    return out + (jnp.where(lane == 0, 0.0, down_z(vz)) - vz)


def inner_solve(b, levels, out, inner, w, kx, ky, kz):
    source = b
    for s in range(1, SWEEPS):
        target = levels[s - 1]

        def one(r, source=source, target=target):
            update(source, b, w, kx, ky, kz, target, r)

        rows_loop(*inner[s], one)
        source = target

    def last(r):
        out[r - HALO] = diverge(source, r)

    rows_loop(*inner[SWEEPS], last, 2)


def outer_solve(b, levels, buffers, inner, full, w, kx, ky, kz, emit):
    source = b
    for s in range(1, SWEEPS):
        target = buffers[s - 1]
        for r in outside(full[s], inner[s]):
            update(source, b, w, kx, ky, kz, target, r)
        source = Rows(levels[s - 1], target, *inner[s])
    for r in outside(full[SWEEPS], inner[SWEEPS]):
        emit(r - HALO, diverge(source, r))


def emit_result(v_own, v_others, p_out, send_a, send_b, eta_at, sums=None):
    n = 1 + len(v_others)
    core = lax.axis_index("gz")
    odd = lax.rem(lax.axis_index("gy"), 2) == 1
    h = HALO

    def emit(r, out):
        ys = v_own.shape[1]
        out = out[:ys]
        parts = split_z(out, core, n)
        v_own[r] = parts[0]
        for ref, part in zip(v_others, parts[1:]):
            ref[r] = part
        if p_out is not None:
            p = eta_at(r) * out
            p_out[r] = p
            low, high = p[:h], p[ys - h :]
            send_a[r] = jnp.where(odd, low, high)
            send_b[r] = jnp.where(odd, high, low)
        if sums is not None:
            sums(r, out)

    return emit


def fold(value):
    total = value[:8]
    for k in range(1, value.shape[0] // 8):
        total = total + value[8 * k : 8 * k + 8]
    lanes = total[:, :LANES]
    for t in range(1, total.shape[1] // LANES):
        lanes = lanes + total[:, t * LANES : (t + 1) * LANES]
    return lanes


def odd_places():
    place = lax.axis_index("gx") * lax.axis_size("gz") + lax.axis_index("gz")
    return lax.rem(lax.axis_index("gy"), 2) == 1, lax.rem(place, 2) == 1, place


def set_row(ref, index, row, a, b, odd_y):
    ys, h = row.shape[0], a.shape[0]
    ref[(*index, slice(0, ys), slice(None))] = row
    ref[(*index, slice(ys, ys + h), slice(None))] = jnp.where(odd_y, b, a)
    ref[(*index, slice(ys + h, ys + 2 * h), slice(None))] = jnp.where(odd_y, a, b)


def coefs_at(sizes, place, slots, lanes, rows, ys, flags):
    h = HALO
    slot = lax.broadcasted_iota(jnp.int32, (slots, lanes), 0)
    at_y = lax.axis_index("gy") * ys + slot - jnp.where(slot >= ys + h, slots, 0)
    at_z = lax.broadcasted_iota(jnp.int32, (slots, lanes), 1)
    in_y = (at_y >= 0) & (at_y < sizes[1])
    y_up, y_low = at_y + 1 < sizes[1], at_y >= 1
    z_up, z_low = at_z + 1 < sizes[2], at_z >= 1
    wall = [jnp.where(flags[k] == 0, 1.0, 0.0).astype(F32) for k in range(6)]

    def coefs(r, mid, before, after, line, force_at, kx, ky, kz, w, b):
        at_x = place * rows - h + r
        x_up = jnp.full(mid.shape, at_x + 1, jnp.int32) < sizes[0]
        x_low = jnp.full(mid.shape, at_x, jnp.int32) >= 1
        inside = in_y & jnp.broadcast_to((at_x >= 0) & (at_x < sizes[0]), mid.shape)
        y_before = jnp.where(slot == ys + h, line, down_y(mid))
        sides = (
            (x_up, after, x_low, before),
            (y_up, up_y(mid), y_low, y_before),
            (z_up, up_z(mid), z_low, down_z(mid)),
        )
        diag = [jnp.zeros_like(mid) for _ in range(3)]
        for axis, (up_in, up, low_in, low) in enumerate(sides):
            up, low = 0.5 * (mid + up), 0.5 * (mid + low)
            (kx, ky, kz)[axis][r] = jnp.where(up_in, up, 0.0)
            for c in range(3):
                low_wall = 1.0 if c == axis else wall[2 * axis]
                up_wall = 1.0 if c == axis else wall[2 * axis + 1]
                diag[c] = diag[c] + jnp.where(up_in, up, up_wall * mid)
                diag[c] = diag[c] + jnp.where(low_in, low, low_wall * mid)
        for c in range(3):
            weight = jnp.where(inside, OMEGA / diag[c], 0.0)
            w[c, r] = weight
            b[c, r] = weight * force_at(c)

    return coefs


def first_inner(sizes, full, ya, yb, flags, kx, ky, kz, w, b, *rest):
    levels, (out, force, eta, line) = rest[: SWEEPS - 1], rest[SWEEPS - 1 :]
    fields, rows, ys, lanes = full.shape
    h = HALO
    odd_y, _, place = odd_places()
    slots, total = ys + 2 * h, rows + 2 * h
    for c in range(fields):

        def one(r, c=c):
            row, a, b_ = full[c, r], ya[c * rows + r], yb[c * rows + r]
            if c < 3:
                set_row(force, (c, r + h), row, a, b_, odd_y)
            else:
                set_row(eta, (r + h,), row, a, b_, odd_y)

        rows_loop(0, rows, one, 4)
    for q in range(rows // 4):
        block = jnp.where(odd_y, ya[fields * rows + q], yb[fields * rows + q])
        for k in range(4):
            line[h + 4 * q + k] = block[k : k + 1]
    coefs = coefs_at(sizes, place, slots, lanes, rows, ys, flags)

    def at(r):
        coefs(r, eta[r], eta[r - 1], eta[r + 1], line[r], lambda c: force[c, r], kx, ky, kz, w, b)

    _, inner = spans(h + 1, h + rows - 1, total)
    rows_loop(*inner[0], at, 1)
    inner_solve(b, levels, out, inner, w, kx, ky, kz)


def first_outer(n, sizes, *refs):
    full, ya, yb, xa, xb, flags, *early = refs[: 11 + SWEEPS]
    kx0, ky0, kz0, w0, b0, *levels, out0 = early
    refs = refs[11 + SWEEPS :]
    v_own, v_others, refs = refs[0], refs[1:n], refs[n:]
    p_out, send_a, send_b, kx, ky, kz, w = refs[:7]
    force, eta, line, b, *buffers = refs[7:]
    fields, rows, ys, lanes = full.shape
    h = HALO
    odd_y, odd_x, place = odd_places()
    slots, total = ys + 2 * h, rows + 2 * h
    ranges, inner = spans(h + 1, h + rows - 1, total)
    todo = outside((0, total), inner[0])
    for r in sorted({min(max(q + d, h), h + rows - 1) for q in todo for d in (-1, 0, 1)}):
        k = r - h
        for c in range(3):
            set_row(force, (c, r), full[c, k], ya[c * rows + k], yb[c * rows + k], odd_y)
        set_row(eta, (r + 1,), full[3, k], ya[3 * rows + k], yb[3 * rows + k], odd_y)
        block = fields * rows + k // 4
        line[r] = jnp.where(odd_y, ya[block], yb[block])[k % 4 : k % 4 + 1]
    blank = jnp.zeros((slots, lanes), F32)
    line_blank = jnp.zeros((1, lanes), F32)
    for k in range(h):
        for r in (k, h + rows + k):
            line[r] = line_blank
    for c in range(3):
        force[c, 0] = blank
        force[c, total - 1] = blank
    eta[0] = blank
    for t, (c, k, q) in enumerate(edge_list(h)):
        lower, upper = jnp.where(odd_x, xa[t], xb[t]), jnp.where(odd_x, xb[t], xa[t])
        where = slice(8 * q, 8 * q + 8)
        if c < 3:
            force[c, k, where, :] = lower
            force[c, total - 1 - k, where, :] = upper
        else:
            eta[1 + k, where, :] = lower
            if k >= 0:
                eta[total - k, where, :] = upper
    coefs = coefs_at(sizes, place, slots, lanes, rows, ys, flags)
    for r in todo:
        after = eta[min(r + 2, total)]
        coefs(r, eta[r + 1], eta[r], after, line[r], lambda c: force[c, r], kx, ky, kz, w, b)

    def carry(r):
        kx[r], ky[r], kz[r] = kx0[r], ky0[r], kz0[r]
        for c in range(3):
            w[c, r] = w0[c, r]

    rows_loop(*inner[0], carry, 2)
    b = Rows(b0, b, *inner[0])
    emit = emit_result(v_own, v_others, p_out, send_a, send_b, lambda r: full[3, r])
    outer_solve(b, levels, buffers, inner, ranges, w, kx, ky, kz, emit)
    rows_loop(inner[SWEEPS][0] - h, inner[SWEEPS][1] - h, lambda r: emit(r, out0[r]), 4)


def next_inner(extra, p_in, ya, yb, kx, ky, kz, w, *rest):
    p, b, *rest = rest[extra:]
    levels, out = rest[: SWEEPS - 1], rest[SWEEPS - 1]
    rows = p_in.shape[0]
    h = HALO
    odd_y, _, _ = odd_places()

    def fill(r):
        set_row(p, (r + h,), p_in[r], ya[r], yb[r], odd_y)

    rows_loop(0, rows, fill, 4)
    _, inner = spans(h, h + rows - 1, rows + 2 * h)
    rows_loop(*inner[0], lambda r: grads(p, w, b, r), 2)
    inner_solve(b, levels, out, inner, w, kx, ky, kz)


def grads(p, w, b, r):
    mid = p[r]
    lanes = mid.shape[1]
    lane = lax.broadcasted_iota(jnp.int32, mid.shape, 1)
    b[0, r] = w[0, r] * (p[r + 1] - mid)
    b[1, r] = w[1, r] * (up_y(mid) - mid)
    b[2, r] = w[2, r] * (jnp.where(lane == lanes - 1, 0.0, up_z(mid)) - mid)


def next_outer(n, last, p_in, xa, xb, full, kx, ky, kz, w, p0, b0, *refs):
    levels, out0, refs = refs[: SWEEPS - 1], refs[SWEEPS - 1], refs[SWEEPS:]
    if last:
        partials, refs = refs[:ITERS], refs[ITERS:]
    v_own, v_others, refs = refs[0], refs[1:n], refs[n:]
    p_out = send_a = send_b = sums = None
    if last:
        moment, acc, refs = v_others[-1].at[p_in.shape[0]], refs[-1], refs[:-1]
        acc[...] = jnp.zeros_like(acc)

        def sums(r, v):
            acc[...] = acc[...] + v * p_in[r]
    else:
        p_out, send_a, send_b, *refs = refs
    p, b, *buffers = refs
    rows = p_in.shape[0]
    h = HALO
    _, odd_x, _ = odd_places()
    for k in range(h):
        a, b_ = xa[k], xb[k]
        p[k] = jnp.where(odd_x, a, b_)
        p[h + rows + k] = jnp.where(odd_x, b_, a)
    ranges, inner = spans(h, h + rows - 1, rows + 2 * h)
    p = Rows(p0, p, h, h + rows)
    for r in outside(ranges[0], inner[0]):
        grads(p, w, b, r)
    b = Rows(b0, b, *inner[0])
    emit = emit_result(v_own, v_others, p_out, send_a, send_b, lambda r: full[3, r], sums)
    outer_solve(b, levels, buffers, inner, ranges, w, kx, ky, kz, emit)
    rows_loop(inner[SWEEPS][0] - h, inner[SWEEPS][1] - h, lambda r: emit(r, out0[r]), 4)
    if last:
        moment[...] = jnp.zeros_like(moment)
        at = 0
        for ref in partials:
            for k in range(ref.shape[0]):
                moment[at : at + 1, :] = jnp.sum(ref[k], 0, keepdims=True)
                at += 1
        moment[at : at + 1, :] = jnp.sum(fold(acc[...]), 0, keepdims=True)


def moments_kernel(n, step, *refs):
    moment, acc = refs[-2:]
    p, refs = refs[0], refs[1:-2]
    before, refs = (refs[0], refs[1:]) if step else (None, refs)
    groups = [refs[k * n : (k + 1) * n] for k in range(step + 1)]
    core = lax.axis_index("gz")
    acc[...] = jnp.zeros_like(acc)

    def one(r):
        v = join_own([q[r] for q in groups[-1]], core)
        others = ([before[r]] if step else []) + [p[r], v]
        others += [join_own([q[r] for q in group], core) for group in groups[:-1]]
        for k, other in enumerate(others):
            acc[k] = acc[k] + v * other

    rows_loop(0, p.shape[0], one, 4)
    for k in range(acc.shape[0]):
        moment[k] = fold(acc[k])


def two_sum(a, b):
    s = a + b
    t = s - a
    return s, (a - (s - t)) + (b - t)


def quick(a, b):
    s = a + b
    return s, b - (s - a)


def halves(a):
    t = 4097.0 * a
    high = t - (t - a)
    return high, a - high


def two_prod(a, b):
    p = a * b
    ah, al = halves(a)
    bh, bl = halves(b)
    return p, ((ah * bh - p) + ah * bl + al * bh) + al * bl


def add(a, b):
    s, e = two_sum(a[0], b[0])
    return quick(s, e + (a[1] + b[1]))


def mul(a, b):
    p, e = two_prod(a[0], b[0])
    return quick(p, e + (a[0] * b[1] + a[1] * b[0]))


def neg(a):
    return -a[0], -a[1]


def div(a, b):
    q = a[0] / b[0]
    r = add(a, neg(mul((q, jnp.zeros_like(q)), b)))
    q2 = r[0] / b[0]
    return quick(q, q2)


def twice(a):
    return 2.0 * a[0], 2.0 * a[1]


def last_kernel(n, cells, sums, eta, *refs):
    own = refs[: 4 * n]
    pressure, residual, norms = refs[4 * n :]
    core = lax.axis_index("gz")
    pair = (sums[0], sums[1])
    for shift in (64, 32, 16, 8, 4, 2, 1):
        pair = add(pair, tuple(pltpu.roll(x, shift, 1) for x in pair))
    item = [(pair[0][k : k + 1], pair[1][k : k + 1]) for k in range(12)]
    m0, n00, m1, m2, n11, n01, m3, m4, n22, n02, n12, m5 = item
    one = (jnp.ones_like(m0[0]), jnp.zeros_like(m0[0]))
    a0 = div(m0, m1)
    c11 = neg(a0)
    g1 = mul(c11, add(m1, mul(c11, m2)))
    b0 = div(g1, m0)
    d10, d11 = add(one, b0), c11
    a1 = div(g1, mul(d11, add(mul(d10, m2), mul(d11, m3))))
    c21 = add(c11, neg(mul(a1, d10)))
    c22 = neg(mul(a1, d11))
    g2 = mul(c22, add(m2, add(mul(c21, m3), mul(c22, m4))))
    b1 = div(g2, g1)
    d20 = add(one, mul(b1, d10))
    d21 = add(c21, mul(b1, d11))
    d22 = c22
    a2 = div(g2, mul(d22, add(mul(d20, m3), add(mul(d21, m4), mul(d22, m5)))))
    p0 = add(a0, add(mul(a1, d10), mul(a2, d20)))[0]
    p1 = add(mul(a1, d11), mul(a2, d21))[0]
    p2 = mul(a2, d22)[0]
    r1 = add(c21, neg(mul(a2, d20)))[0]
    r2 = add(c22, neg(mul(a2, d21)))[0]
    r3 = -p2
    norm1 = add(n00, mul(c11, add(twice(n01), mul(c11, n11))))
    norm2 = add(n00, mul(c21, add(twice(n01), mul(c21, n11))))
    norm2 = add(norm2, mul(c22, add(twice(n02), add(mul(twice(c21), n12), mul(c22, n22)))))
    for k, value in enumerate((n00, norm1, norm2)):
        norms[k] = (value[0] / cells)[0, 0]
    rows = own[0].shape[0]
    for j in range(n):
        base = lax.rem(core - j + n, n) * rows
        v0, v1, v2, v3 = (own[k * n + j] for k in range(4))

        def one_row(r, base=base, v0=v0, v1=v1, v2=v2, v3=v3):
            x0, x1, x2, x3 = v0[r], v1[r], v2[r], v3[r]
            pressure[base + r] = eta[base + r] * (p0 * x0 + p1 * x1 + p2 * x2)
            residual[base + r] = (x0 + r1 * x1) + (r2 * x2 + r3 * x3)

        rows_loop(0, rows, one_row, 4)


def add_pairs(a, b):
    s, e = two_sum(a[0], b[0])
    return jnp.stack([s, e + (a[1] + b[1])])


def reduce_all(pair, nx, ny, nz):
    axes = ("gx", "gy", "gz")
    places = [(x, y, z) for x in range(nx) for y in range(ny) for z in range(nz)]
    number = {place: k for k, place in enumerate(places)}
    for axis, n, step in ((0, nx, 1), (1, ny, 1), (2, nz, 2)):
        while step < n:
            moves = []
            for place in places:
                other = list(place)
                other[axis] ^= step
                if place[2] % 2 == 1:
                    moves.append((number[place], number[tuple(other)]))
            pair = add_pairs(pair, lax.ppermute(pair, axes, moves))
            step *= 2
    handed = lax.ppermute(pair, "gz", [(k, k - 1) for k in range(1, nz, 2)])
    return jnp.where(lax.rem(lax.axis_index("gz"), 2) == 1, pair, handed)


def per_device(nx, ny, nz, force, phase, table, flags):
    h = HALO
    wide, ys, lanes = phase.shape
    rows = wide // nz
    zs = lanes * nz
    sizes = (wide * nx, ys * ny, zs)
    slots, total = ys + 2 * h, rows + 2 * h
    cells = float(sizes[0] * sizes[1] * sizes[2])
    chain = nx * nz

    parts = call(
        functools.partial(prep_kernel, nz),
        [sds(4, rows, ys, lanes)] * nz + [sds(*phase.shape)],
        (force, phase, table),
        [HBM, HBM, SMEM],
        [pltpu.VMEM(phase.shape, jnp.int32), pltpu.SemaphoreType.DMA((3 * nz + 1,))],
        name="prep",
    )
    eta = parts[-1]
    parts = [parts[0]] + [core_shift(parts[j], nz, j) for j in range(1, nz)]
    edge = sds(4 * rows + rows // 4, h, zs)
    full, ya, yb = call(
        functools.partial(gather_kernel, nz),
        [sds(4, rows, ys, zs), edge, edge],
        parts,
        name="gather",
    )
    ya, yb = exchange("gy", ny, ya, yb)
    edge = sds(len(edge_list(h)), 8, zs)
    xa, xb = call(force_edges_kernel, [edge, edge], (full, ya, yb), name="force_edges")
    xa, xb = exchange(("gx", "gz"), chain, xa, xb)

    v_shape = [sds(rows, ys, lanes)] * nz
    sent = [sds(rows, ys, zs), sds(rows, h, zs), sds(rows, h, zs)]
    scalar, vector = sds(total, slots, zs), sds(3, total, slots, zs)
    field = pltpu.VMEM((3, total, slots, zs), F32)
    line = pltpu.VMEM((total, 1, zs), F32)
    heavy = 4 * 10**7
    early = call(
        functools.partial(first_inner, sizes),
        [scalar] * 3 + [vector] * (1 + SWEEPS) + [sds(rows, slots, zs)],
        (full, ya, yb, flags),
        [VMEM] * 3 + [SMEM],
        [field, pltpu.VMEM((total, slots, zs), F32), line],
        heavy,
        "first_inner",
    )
    outs = call(
        functools.partial(first_outer, nz, sizes),
        v_shape + sent + [scalar] * 3 + [vector],
        (full, ya, yb, xa, xb, flags, *early),
        [VMEM] * 5 + [SMEM] + [VMEM] * len(early),
        [field, pltpu.VMEM((total + 1, slots, zs), F32), line] + [field] * SWEEPS,
        heavy,
        "first",
    )
    vs, ps, moments = [list(outs[:nz])], [outs[nz]], []
    ya, yb = outs[nz + 1 : nz + 3]
    coefs = outs[nz + 3 :]
    placed = []
    for step in range(1, ITERS + 1):
        last = step == ITERS
        p, v = ps[-1], vs[-1]
        placed.append([v[0]] + [core_shift(v[j], nz, j) for j in range(1, nz)])
        count = 2 if step == 1 else 2 + step
        moments.append(
            call(
                functools.partial(moments_kernel, nz, step - 1),
                [sds(count, 8, LANES)],
                (p, *ps[:-1][-1:], *[q for v in vs for q in v]),
                None,
                [pltpu.VMEM((count, ys, zs), F32)],
                name="moments",
            )[0]
        )
        ya, yb = exchange("gy", ny, ya, yb)
        edge = sds(h, slots, zs)
        xa, xb = call(edges_kernel, [edge, edge], (p, ya, yb, moments[-1]), name="edges")
        xa, xb = exchange(("gx", "gz"), chain, xa, xb)
        early = call(
            functools.partial(next_inner, nz - 1),
            [scalar] + [vector] * SWEEPS + [sds(rows, slots, zs)],
            (p, ya, yb, *coefs, *placed[-1][1:]),
            None,
            (),
            heavy,
            "next_inner",
        )
        joint = v_shape[:-1] + [sds(rows + 1, ys, lanes)]
        outs = call(
            functools.partial(next_outer, nz, last),
            joint if last else v_shape + sent,
            (p, xa, xb, full, *coefs, *early, *(moments if last else ())),
            None,
            [pltpu.VMEM((total, slots, zs), F32)]
            + [field] * SWEEPS
            + ([pltpu.VMEM((ys, zs), F32)] if last else []),
            heavy,
            "next",
        )
        vs.append(list(outs[:nz]))
        if not last:
            ps.append(outs[nz])
            ya, yb = outs[nz + 1 : nz + 3]

    v = vs[-1]
    moved = [v[0]] + [core_shift(v[j], nz, j) for j in range(1, nz)]
    placed.append(moved)
    mine, theirs = v[-1][rows], moved[-1][rows]
    if nz > 2:
        theirs = lax.ppermute(mine, "gz", [(k, k ^ 1) for k in range(nz)])
    pair = jnp.stack(two_sum(mine, theirs))
    pair = reduce_all(pair, nx, ny, nz)
    pressure, residual, norms = call(
        functools.partial(last_kernel, nz, cells),
        [sds(*phase.shape), sds(*phase.shape), sds(ITERS)],
        (pair, eta, *[q for v in placed for q in v]),
        name="last",
        out_specs=[VMEM, VMEM, SMEM],
    )
    return pressure, residual, norms


def solution(mesh):
    placed = (P(None, "gx", "gy", "gz"), P("gx", "gy", "gz"), P(), P())
    return jax.shard_map(
        functools.partial(per_device, mesh.shape["gx"], mesh.shape["gy"], mesh.shape["gz"]),
        mesh=mesh,
        in_specs=placed,
        out_specs=(P("gx", "gy", "gz"), P("gx", "gy", "gz"), P()),
        check_vma=False,
    )
```

```python
import functools

import jax
import jax.numpy as jnp
from jax import lax
from jax.experimental import pallas as pl
from jax.experimental.pallas import tpu as pltpu
from jax.sharding import PartitionSpec as P

ITERS = 3
SWEEPS = 4
OMEGA = 0.8
HALO = 4
LANES = 128
F32 = jnp.float32

VMEM = pl.BlockSpec(memory_space=pltpu.VMEM)
SMEM = pl.BlockSpec(memory_space=pltpu.SMEM)


def sds(*shape):
    return jax.ShapeDtypeStruct(shape, F32)


def call(kernel, outs, ins, specs=None, scratch=(), flops=10**6, name=None, out_specs=None):
    return pl.pallas_call(
        kernel,
        out_shape=outs,
        in_specs=specs or [VMEM] * len(ins),
        out_specs=out_specs or jax.tree.map(lambda _: VMEM, outs),
        scratch_shapes=list(scratch),
        compiler_params=pltpu.CompilerParams(vmem_limit_bytes=24 * 2**20),
        cost_estimate=pl.CostEstimate(flops=flops, bytes_accessed=2**20, transcendentals=0),
        name=name,
    )(*ins)


def pick(items, index):
    value = items[0]
    for k in range(1, len(items)):
        value = jnp.where(index == k, items[k], value)
    return value


def split_z(value, core, n):
    blocks = [value[..., t * LANES : (t + 1) * LANES] for t in range(n)]
    return [pick(blocks, lax.rem(core + j, n)) for j in range(n)]


def join_own(parts, core):
    n = len(parts)
    return jnp.concatenate([pick(parts, lax.rem(t - core + n, n)) for t in range(n)], -1)


def join_received(parts, core):
    n = len(parts)
    return jnp.concatenate([pick(parts, lax.rem(core - t + n, n)) for t in range(n)], -1)


def up_y(row):
    return pltpu.roll(row, row.shape[0] - 1, 0)


def down_y(row):
    return pltpu.roll(row, 1, 0)


def up_z(row):
    return pltpu.roll(row, row.shape[1] - 1, 1)


def down_z(row):
    return pltpu.roll(row, 1, 1)


def rows_loop(start, stop, body, step=3):
    count = stop - start
    whole = count // step

    def chunk(i, carry):
        for k in range(step):
            body(start + i * step + k)
        return carry

    if whole > 1:
        lax.fori_loop(0, whole, chunk, 0)
        rest = start + whole * step
    else:
        rest = start
    for r in range(rest, stop):
        body(r)


def exchange_y(up, low, n):
    from_below = lax.ppermute(up, "gy", [(i, (i + 1) % n) for i in range(n)])
    from_above = lax.ppermute(low, "gy", [(i, (i - 1) % n) for i in range(n)])
    return from_above, from_below


def exchange_x(a, b, n):
    even = [(i, i ^ 1) for i in range(n)]
    odd = [(i, (i + (1 if i % 2 else -1)) % n) for i in range(n)]
    return lax.ppermute(a, ("gx", "gz"), even), lax.ppermute(b, ("gx", "gz"), odd)


def core_shift(value, n, j):
    return lax.ppermute(value, "gz", [(i, (i + j) % n) for i in range(n)])


def prep_kernel(n, force, phase, table, *outs):
    core = lax.axis_index("gz")
    rows = outs[0].shape[1]
    eta_out = outs[n]
    levels = table.shape[0]

    def one(r):
        ids = phase[r]
        eta = jnp.zeros(ids.shape, F32)
        for level in range(levels):
            eta = jnp.where(ids == level, table[level], eta)
        eta_out[r] = eta

    rows_loop(0, phase.shape[0], one, 4)
    for j in range(n):
        base = lax.rem(core + j, n) * rows

        def two(r, j=j, base=base):
            for c in range(3):
                outs[j][c, r] = force[c, base + r]
            outs[j][3, r] = eta_out[base + r]

        rows_loop(0, rows, two, 4)


def gather_kernel(n, *refs):
    parts = refs[:n]
    full, send_up, send_low = refs[n:]
    core = lax.axis_index("gz")
    fields, rows, ys, _ = full.shape
    h = HALO

    for c in range(fields):

        def one(r, c=c):
            row = join_received([p[c, r] for p in parts], core)
            full[c, r] = row
            send_low[c * rows + r] = row[:h]
            send_up[c * rows + r] = row[ys - h :]

        rows_loop(0, rows, one, 4)
    for r in range(rows):
        line = full[3, r, ys - h - 1 : ys - h, :]
        send_up[fields * rows + r // 4, r % 4 : r % 4 + 1, :] = line


def edge_list(h):
    tiles = []
    for c in range(4):
        for k in range(h):
            if c in (1, 2) and k == 0:
                continue
            for q in range(2 if c == 0 and k == 0 else 3):
                tiles.append((c, k, q))
    return tiles + [(3, -1, 0), (3, -1, 1)]


def force_edges_kernel(full, up, low, send_a, send_b):
    odd_x = Place().odd
    _, rows, ys, _ = full.shape
    h = HALO
    for send, first in ((send_a, odd_x), (send_b, jnp.logical_not(odd_x))):
        for t, (c, k, q) in enumerate(edge_list(h)):
            r = jnp.where(first, h - 1 - k, rows - h + k)
            if q < 2:
                send[t] = full[c, r, 8 * q : 8 * q + 8, :]
            else:
                send[t, :h, :] = up[c * rows + r]
                send[t, h:, :] = low[c * rows + r]


def edges_kernel(p, up, low, *rest):
    send_a, send_b = rest[-2:]
    place = Place()
    rows = p.shape[0]
    h = HALO
    for send, first in ((send_a, place.odd), (send_b, jnp.logical_not(place.odd))):
        start = jnp.where(first, 0, rows - h)
        for k in range(h):
            set_row(send, (k,), p[start + k], up[start + k], low[start + k], place)


class Rows:
    def __init__(self, early, late, first, end):
        self.early, self.late, self.first, self.end = early, late, first, end

    def __getitem__(self, index):
        r = index[-1] if isinstance(index, tuple) else index
        mine = not isinstance(r, int) or not self.first <= r < self.end
        return (self.late if mine else self.early)[index]


def spans(lo, hi, total):
    full = [(s, total - 1 - s) for s in range(SWEEPS)] + [(HALO, total - HALO)]
    inner = [(lo + s, hi - s) for s in range(SWEEPS)] + [(lo + SWEEPS, hi - SWEEPS + 1)]
    inner = [i if i[0] < i[1] else (f[0], f[0]) for f, i in zip(full, inner)]
    return full, inner


def outside(full, inner):
    return list(range(full[0], inner[0])) + list(range(inner[1], full[1]))


def update(source, b, w, kx, ky, kz, target, r):
    keep = 1.0 - OMEGA
    here_x, past_x, here_y, here_z = kx[r], kx[r - 1], ky[r], kz[r]
    for c in range(3):
        u = source[c, r]
        near = here_x * source[c, r + 1] + past_x * source[c, r - 1]
        near = near + here_y * up_y(u) + down_y(here_y * u)
        near = near + here_z * up_z(u) + down_z(here_z * u)
        target[c, r] = keep * u + (b[c, r] + w[c, r] * near)


def diverge(v, r):
    vy, vz = v[1, r], v[2, r]
    lane = lax.broadcasted_iota(jnp.int32, vz.shape, 1)
    out = v[0, r - 1] - v[0, r]
    out = out + (down_y(vy) - vy)
    return out + (jnp.where(lane == 0, 0.0, down_z(vz)) - vz)


def inner_solve(b, levels, out, inner, w, kx, ky, kz):
    source = b
    for s in range(1, SWEEPS):
        target = levels[s - 1]

        def one(r, source=source, target=target):
            update(source, b, w, kx, ky, kz, target, r)

        rows_loop(*inner[s], one)
        source = target

    def last(r):
        out[r - HALO] = diverge(source, r)

    rows_loop(*inner[SWEEPS], last, 2)


def outer_solve(b, levels, buffers, inner, full, w, kx, ky, kz, emit):
    source = b
    for s in range(1, SWEEPS):
        target = buffers[s - 1]
        for r in outside(full[s], inner[s]):
            update(source, b, w, kx, ky, kz, target, r)
        source = Rows(levels[s - 1], target, *inner[s])
    for r in outside(full[SWEEPS], inner[SWEEPS]):
        emit(r - HALO, diverge(source, r))


def emit_result(v_own, v_others, p_out, send_up, send_low, eta_at, sums=None):
    n = 1 + len(v_others)
    core = lax.axis_index("gz")
    h = HALO

    def emit(r, out):
        ys = v_own.shape[1]
        out = out[:ys]
        parts = split_z(out, core, n)
        v_own[r] = parts[0]
        for ref, part in zip(v_others, parts[1:]):
            ref[r] = part
        if p_out is not None:
            p = eta_at(r) * out
            p_out[r] = p
            send_up[r] = p[ys - h :]
            send_low[r] = p[:h]
        if sums is not None:
            sums(r, out)

    return emit


def fold(value):
    total = value[:8]
    for k in range(1, value.shape[0] // 8):
        total = total + value[8 * k : 8 * k + 8]
    lanes = total[:, :LANES]
    for t in range(1, total.shape[1] // LANES):
        lanes = lanes + total[:, t * LANES : (t + 1) * LANES]
    return lanes


class Place:
    def __init__(self):
        chain = lax.axis_size("gx") * lax.axis_size("gz")
        self.x = lax.axis_index("gx") * lax.axis_size("gz") + lax.axis_index("gz")
        self.odd = lax.rem(self.x, 2) == 1
        self.below_x, self.above_x = self.x > 0, self.x < chain - 1
        y = lax.axis_index("gy")
        self.below_y, self.above_y = y > 0, y < lax.axis_size("gy") - 1


def set_row(ref, index, row, up, low, place=None):
    ys, h = row.shape[0], up.shape[0]
    if place is not None:
        up, low = jnp.where(place.above_y, up, 0.0), jnp.where(place.below_y, low, 0.0)
    ref[(*index, slice(0, ys), slice(None))] = row
    ref[(*index, slice(ys, ys + h), slice(None))] = up
    ref[(*index, slice(ys + h, ys + 2 * h), slice(None))] = low


def coefs_at(sizes, place, slots, lanes, rows, ys, flags):
    h = HALO
    slot = lax.broadcasted_iota(jnp.int32, (slots, lanes), 0)
    at_y = lax.axis_index("gy") * ys + slot - jnp.where(slot >= ys + h, slots, 0)
    at_z = lax.broadcasted_iota(jnp.int32, (slots, lanes), 1)
    in_y = (at_y >= 0) & (at_y < sizes[1])
    y_up, y_low = at_y + 1 < sizes[1], at_y >= 1
    z_up, z_low = at_z + 1 < sizes[2], at_z >= 1
    wall = [jnp.where(flags[k] == 0, 1.0, 0.0).astype(F32) for k in range(6)]

    def coefs(r, mid, before, after, line, force_at, kx, ky, kz, w, b):
        at_x = place * rows - h + r
        x_up = jnp.full(mid.shape, at_x + 1, jnp.int32) < sizes[0]
        x_low = jnp.full(mid.shape, at_x, jnp.int32) >= 1
        inside = in_y & jnp.broadcast_to((at_x >= 0) & (at_x < sizes[0]), mid.shape)
        y_before = jnp.where(slot == ys + h, line, down_y(mid))
        sides = (
            (x_up, after, x_low, before),
            (y_up, up_y(mid), y_low, y_before),
            (z_up, up_z(mid), z_low, down_z(mid)),
        )
        diag = [jnp.zeros_like(mid) for _ in range(3)]
        for axis, (up_in, up, low_in, low) in enumerate(sides):
            up, low = 0.5 * (mid + up), 0.5 * (mid + low)
            (kx, ky, kz)[axis][r] = jnp.where(up_in, up, 0.0)
            for c in range(3):
                low_wall = 1.0 if c == axis else wall[2 * axis]
                up_wall = 1.0 if c == axis else wall[2 * axis + 1]
                diag[c] = diag[c] + jnp.where(up_in, up, up_wall * mid)
                diag[c] = diag[c] + jnp.where(low_in, low, low_wall * mid)
        for c in range(3):
            weight = jnp.where(inside, OMEGA / diag[c], 0.0)
            w[c, r] = weight
            b[c, r] = weight * force_at(c)

    return coefs


def first_inner(sizes, full, up, low, flags, kx, ky, kz, w, b, *rest):
    levels, (out, force, eta, line) = rest[: SWEEPS - 1], rest[SWEEPS - 1 :]
    fields, rows, ys, lanes = full.shape
    h = HALO
    place = Place().x
    slots, total = ys + 2 * h, rows + 2 * h
    for c in range(fields):

        def one(r, c=c):
            to, index = (force, (c, r + h)) if c < 3 else (eta, (r + h,))
            set_row(to, index, full[c, r], up[c * rows + r], low[c * rows + r])

        rows_loop(0, rows, one, 4)
    for q in range(rows // 4):
        block = low[fields * rows + q]
        for k in range(4):
            line[h + 4 * q + k] = block[k : k + 1]
    coefs = coefs_at(sizes, place, slots, lanes, rows, ys, flags)

    def at(r):
        coefs(r, eta[r], eta[r - 1], eta[r + 1], line[r], lambda c: force[c, r], kx, ky, kz, w, b)

    _, inner = spans(h + 1, h + rows - 1, total)
    rows_loop(*inner[0], at, 1)
    inner_solve(b, levels, out, inner, w, kx, ky, kz)


def first_outer(n, sizes, *refs):
    full, up, low, xa, xb, flags, *early = refs[: 11 + SWEEPS]
    kx0, ky0, kz0, w0, b0, *levels, out0 = early
    refs = refs[11 + SWEEPS :]
    v_own, v_others, refs = refs[0], refs[1:n], refs[n:]
    p_out, send_up, send_low, kx, ky, kz, w = refs[:7]
    force, eta, line, b, *buffers = refs[7:]
    fields, rows, ys, lanes = full.shape
    h = HALO
    place, odd_x = Place().x, Place().odd
    slots, total = ys + 2 * h, rows + 2 * h
    ranges, inner = spans(h + 1, h + rows - 1, total)
    todo = outside((0, total), inner[0])
    for r in sorted({min(max(q + d, h), h + rows - 1) for q in todo for d in (-1, 0, 1)}):
        k = r - h
        for c in range(fields):
            to, index = (force, (c, r)) if c < 3 else (eta, (r + 1,))
            set_row(to, index, full[c, k], up[c * rows + k], low[c * rows + k])
        line[r] = low[fields * rows + k // 4, k % 4 : k % 4 + 1, :]
    blank = jnp.zeros((slots, lanes), F32)
    line_blank = jnp.zeros((1, lanes), F32)
    for k in range(h):
        for r in (k, h + rows + k):
            line[r] = line_blank
    for c in range(3):
        force[c, 0] = blank
        force[c, total - 1] = blank
    eta[0] = blank
    for t, (c, k, q) in enumerate(edge_list(h)):
        lower, upper = jnp.where(odd_x, xa[t], xb[t]), jnp.where(odd_x, xb[t], xa[t])
        where = slice(8 * q, 8 * q + 8)
        if c < 3:
            force[c, k, where, :] = lower
            force[c, total - 1 - k, where, :] = upper
        else:
            eta[1 + k, where, :] = lower
            if k >= 0:
                eta[total - k, where, :] = upper
    coefs = coefs_at(sizes, place, slots, lanes, rows, ys, flags)
    for r in todo:
        after = eta[min(r + 2, total)]
        coefs(r, eta[r + 1], eta[r], after, line[r], lambda c: force[c, r], kx, ky, kz, w, b)

    def carry(r):
        kx[r], ky[r], kz[r] = kx0[r], ky0[r], kz0[r]
        for c in range(3):
            w[c, r] = w0[c, r]

    rows_loop(*inner[0], carry, 2)
    b = Rows(b0, b, *inner[0])
    emit = emit_result(v_own, v_others, p_out, send_up, send_low, lambda r: full[3, r])
    outer_solve(b, levels, buffers, inner, ranges, w, kx, ky, kz, emit)
    rows_loop(inner[SWEEPS][0] - h, inner[SWEEPS][1] - h, lambda r: emit(r, out0[r]), 4)


def next_inner(extra, p_in, up, low, kx, ky, kz, w, *rest):
    p, b, *rest = rest[extra:]
    levels, out = rest[: SWEEPS - 1], rest[SWEEPS - 1]
    rows = p_in.shape[0]
    h = HALO
    place = Place()

    def fill(r):
        set_row(p, (r + h,), p_in[r], up[r], low[r], place)

    rows_loop(0, rows, fill, 4)
    _, inner = spans(h, h + rows - 1, rows + 2 * h)
    rows_loop(*inner[0], lambda r: grads(p, w, b, r), 2)
    inner_solve(b, levels, out, inner, w, kx, ky, kz)


def grads(p, w, b, r):
    mid = p[r]
    lanes = mid.shape[1]
    lane = lax.broadcasted_iota(jnp.int32, mid.shape, 1)
    b[0, r] = w[0, r] * (p[r + 1] - mid)
    b[1, r] = w[1, r] * (up_y(mid) - mid)
    b[2, r] = w[2, r] * (jnp.where(lane == lanes - 1, 0.0, up_z(mid)) - mid)


def next_outer(n, last, p_in, xa, xb, full, kx, ky, kz, w, p0, b0, *refs):
    levels, out0, refs = refs[: SWEEPS - 1], refs[SWEEPS - 1], refs[SWEEPS:]
    if last:
        partials, refs = refs[:ITERS], refs[ITERS:]
    v_own, v_others, refs = refs[0], refs[1:n], refs[n:]
    p_out = send_up = send_low = sums = None
    if last:
        moment, acc, refs = v_others[-1].at[p_in.shape[0]], refs[-1], refs[:-1]
        acc[...] = jnp.zeros_like(acc)

        def sums(r, v):
            acc[...] = acc[...] + v * p_in[r]
    else:
        p_out, send_up, send_low, *refs = refs
    p, b, *buffers = refs
    rows = p_in.shape[0]
    h = HALO
    place = Place()
    for k in range(h):
        lower, upper = jnp.where(place.odd, xa[k], xb[k]), jnp.where(place.odd, xb[k], xa[k])
        p[k] = jnp.where(place.below_x, lower, 0.0)
        p[h + rows + k] = jnp.where(place.above_x, upper, 0.0)
    ranges, inner = spans(h, h + rows - 1, rows + 2 * h)
    p = Rows(p0, p, h, h + rows)
    for r in outside(ranges[0], inner[0]):
        grads(p, w, b, r)
    b = Rows(b0, b, *inner[0])
    emit = emit_result(v_own, v_others, p_out, send_up, send_low, lambda r: full[3, r], sums)
    outer_solve(b, levels, buffers, inner, ranges, w, kx, ky, kz, emit)
    rows_loop(inner[SWEEPS][0] - h, inner[SWEEPS][1] - h, lambda r: emit(r, out0[r]), 4)
    if last:
        moment[...] = jnp.zeros_like(moment)
        at = 0
        for ref in partials:
            for k in range(ref.shape[0]):
                moment[at : at + 1, :] = jnp.sum(ref[k], 0, keepdims=True)
                at += 1
        moment[at : at + 1, :] = jnp.sum(fold(acc[...]), 0, keepdims=True)


def moments_kernel(n, step, *refs):
    moment, acc = refs[-2:]
    p, refs = refs[0], refs[1:-2]
    before, refs = (refs[0], refs[1:]) if step else (None, refs)
    groups = [refs[k * n : (k + 1) * n] for k in range(step + 1)]
    core = lax.axis_index("gz")
    acc[...] = jnp.zeros_like(acc)

    def one(r):
        v = join_own([q[r] for q in groups[-1]], core)
        others = ([before[r]] if step else []) + [p[r], v]
        others += [join_own([q[r] for q in group], core) for group in groups[:-1]]
        for k, other in enumerate(others):
            acc[k] = acc[k] + v * other

    rows_loop(0, p.shape[0], one, 4)
    for k in range(acc.shape[0]):
        moment[k] = fold(acc[k])


def two_sum(a, b):
    s = a + b
    t = s - a
    return s, (a - (s - t)) + (b - t)


def quick(a, b):
    s = a + b
    return s, b - (s - a)


def halves(a):
    t = 4097.0 * a
    high = t - (t - a)
    return high, a - high


def two_prod(a, b):
    p = a * b
    ah, al = halves(a)
    bh, bl = halves(b)
    return p, ((ah * bh - p) + ah * bl + al * bh) + al * bl


def add(a, b):
    s, e = two_sum(a[0], b[0])
    return quick(s, e + (a[1] + b[1]))


def mul(a, b):
    p, e = two_prod(a[0], b[0])
    return quick(p, e + (a[0] * b[1] + a[1] * b[0]))


def neg(a):
    return -a[0], -a[1]


def div(a, b):
    q = a[0] / b[0]
    r = add(a, neg(mul((q, jnp.zeros_like(q)), b)))
    q2 = r[0] / b[0]
    return quick(q, q2)


def twice(a):
    return 2.0 * a[0], 2.0 * a[1]


def last_kernel(n, cells, sums, eta, *refs):
    own = refs[: 4 * n]
    pressure, residual, norms = refs[4 * n :]
    core = lax.axis_index("gz")
    pair = (sums[0], sums[1])
    for shift in (64, 32, 16, 8, 4, 2, 1):
        pair = add(pair, tuple(pltpu.roll(x, shift, 1) for x in pair))
    item = [(pair[0][k : k + 1], pair[1][k : k + 1]) for k in range(12)]
    m0, n00, m1, m2, n11, n01, m3, m4, n22, n02, n12, m5 = item
    one = (jnp.ones_like(m0[0]), jnp.zeros_like(m0[0]))
    a0 = div(m0, m1)
    c11 = neg(a0)
    g1 = mul(c11, add(m1, mul(c11, m2)))
    b0 = div(g1, m0)
    d10, d11 = add(one, b0), c11
    a1 = div(g1, mul(d11, add(mul(d10, m2), mul(d11, m3))))
    c21 = add(c11, neg(mul(a1, d10)))
    c22 = neg(mul(a1, d11))
    g2 = mul(c22, add(m2, add(mul(c21, m3), mul(c22, m4))))
    b1 = div(g2, g1)
    d20 = add(one, mul(b1, d10))
    d21 = add(c21, mul(b1, d11))
    d22 = c22
    a2 = div(g2, mul(d22, add(mul(d20, m3), add(mul(d21, m4), mul(d22, m5)))))
    p0 = add(a0, add(mul(a1, d10), mul(a2, d20)))[0]
    p1 = add(mul(a1, d11), mul(a2, d21))[0]
    p2 = mul(a2, d22)[0]
    r1 = add(c21, neg(mul(a2, d20)))[0]
    r2 = add(c22, neg(mul(a2, d21)))[0]
    r3 = -p2
    norm1 = add(n00, mul(c11, add(twice(n01), mul(c11, n11))))
    norm2 = add(n00, mul(c21, add(twice(n01), mul(c21, n11))))
    norm2 = add(norm2, mul(c22, add(twice(n02), add(mul(twice(c21), n12), mul(c22, n22)))))
    for k, value in enumerate((n00, norm1, norm2)):
        norms[k] = (value[0] / cells)[0, 0]
    rows = own[0].shape[0]
    for j in range(n):
        base = lax.rem(core - j + n, n) * rows
        v0, v1, v2, v3 = (own[k * n + j] for k in range(4))

        def one_row(r, base=base, v0=v0, v1=v1, v2=v2, v3=v3):
            x0, x1, x2, x3 = v0[r], v1[r], v2[r], v3[r]
            pressure[base + r] = eta[base + r] * (p0 * x0 + p1 * x1 + p2 * x2)
            residual[base + r] = (x0 + r1 * x1) + (r2 * x2 + r3 * x3)

        rows_loop(0, rows, one_row, 4)


def add_pairs(a, b):
    s, e = two_sum(a[0], b[0])
    return jnp.stack([s, e + (a[1] + b[1])])


def sum_along(pair, axis, n, stride=1):
    count = n // stride
    if count < 2:
        return pair
    terms = [pair]
    for k in range(1, count):
        moves = [(i, (i + k * stride) % n) for i in range(n)]
        terms.append(lax.ppermute(pair, axis, moves))
    me = lax.axis_index(axis) // stride
    terms = [pick(terms, lax.rem(me - j + count, count)) for j in range(count)]
    while len(terms) > 1:
        rest = terms[len(terms) // 2 * 2 :]
        terms = [add_pairs(a, b) for a, b in zip(terms[::2], terms[1::2])] + rest
    return terms[0]


def per_device(nx, ny, nz, force, phase, table, flags):
    h = HALO
    wide, ys, lanes = phase.shape
    rows = wide // nz
    zs = lanes * nz
    sizes = (wide * nx, ys * ny, zs)
    slots, total = ys + 2 * h, rows + 2 * h
    cells = float(sizes[0] * sizes[1] * sizes[2])
    chain = nx * nz

    parts = call(
        functools.partial(prep_kernel, nz),
        [sds(4, rows, ys, lanes)] * nz + [sds(*phase.shape)],
        (force, phase, table),
        [VMEM, VMEM, SMEM],
        name="prep",
    )
    eta = parts[-1]
    parts = [parts[0]] + [core_shift(parts[j], nz, j) for j in range(1, nz)]
    full, ya, yb = call(
        functools.partial(gather_kernel, nz),
        [
            sds(4, rows, ys, zs),
            sds(4 * rows + rows // 4, h, zs),
            sds(4 * rows, h, zs),
        ],
        parts,
        name="gather",
    )
    ya, yb = exchange_y(ya, yb, ny)
    edge = sds(len(edge_list(h)), 8, zs)
    xa, xb = call(force_edges_kernel, [edge, edge], (full, ya, yb), name="force_edges")
    xa, xb = exchange_x(xa, xb, chain)

    v_shape = [sds(rows, ys, lanes)] * nz
    sent = [sds(rows, ys, zs), sds(rows, h, zs), sds(rows, h, zs)]
    scalar, vector = sds(total, slots, zs), sds(3, total, slots, zs)
    field = pltpu.VMEM((3, total, slots, zs), F32)
    line = pltpu.VMEM((total, 1, zs), F32)
    heavy = 4 * 10**7
    early = call(
        functools.partial(first_inner, sizes),
        [scalar] * 3 + [vector] * (1 + SWEEPS) + [sds(rows, slots, zs)],
        (full, ya, yb, flags),
        [VMEM] * 3 + [SMEM],
        [field, pltpu.VMEM((total, slots, zs), F32), line],
        heavy,
        "first_inner",
    )
    outs = call(
        functools.partial(first_outer, nz, sizes),
        v_shape + sent + [scalar] * 3 + [vector],
        (full, ya, yb, xa, xb, flags, *early),
        [VMEM] * 5 + [SMEM] + [VMEM] * len(early),
        [field, pltpu.VMEM((total + 1, slots, zs), F32), line] + [field] * SWEEPS,
        heavy,
        "first",
    )
    vs, ps, moments = [list(outs[:nz])], [outs[nz]], []
    ya, yb = outs[nz + 1 : nz + 3]
    coefs = outs[nz + 3 :]
    placed = []
    for step in range(1, ITERS + 1):
        last = step == ITERS
        p, v = ps[-1], vs[-1]
        placed.append([v[0]] + [core_shift(v[j], nz, j) for j in range(1, nz)])
        count = 2 if step == 1 else 2 + step
        moments.append(
            call(
                functools.partial(moments_kernel, nz, step - 1),
                [sds(count, 8, LANES)],
                (p, *ps[:-1][-1:], *[q for v in vs for q in v]),
                None,
                [pltpu.VMEM((count, ys, zs), F32)],
                name="moments",
            )[0]
        )
        ya, yb = exchange_y(ya, yb, ny)
        edge = sds(h, slots, zs)
        xa, xb = call(edges_kernel, [edge, edge], (p, ya, yb, moments[-1]), name="edges")
        xa, xb = exchange_x(xa, xb, chain)
        early = call(
            functools.partial(next_inner, nz - 1),
            [scalar] + [vector] * SWEEPS + [sds(rows, slots, zs)],
            (p, ya, yb, *coefs, *placed[-1][1:]),
            None,
            (),
            heavy,
            "next_inner",
        )
        joint = v_shape[:-1] + [sds(rows + 1, ys, lanes)]
        outs = call(
            functools.partial(next_outer, nz, last),
            joint if last else v_shape + sent,
            (p, xa, xb, full, *coefs, *early, *(moments if last else ())),
            None,
            [pltpu.VMEM((total, slots, zs), F32)]
            + [field] * SWEEPS
            + ([pltpu.VMEM((ys, zs), F32)] if last else []),
            heavy,
            "next",
        )
        vs.append(list(outs[:nz]))
        if not last:
            ps.append(outs[nz])
            ya, yb = outs[nz + 1 : nz + 3]

    v = vs[-1]
    moved = [v[0]] + [core_shift(v[j], nz, j) for j in range(1, nz)]
    placed.append(moved)
    mine, theirs = v[-1][rows], moved[-1][rows]
    if nz > 2:
        theirs = lax.ppermute(mine, "gz", [(k, k ^ 1) for k in range(nz)])
    pair = jnp.stack(two_sum(mine, theirs))
    pair = sum_along(pair, "gz", nz, 2)
    pair = sum_along(sum_along(pair, "gx", nx), "gy", ny)
    pressure, residual, norms = call(
        functools.partial(last_kernel, nz, cells),
        [sds(*phase.shape), sds(*phase.shape), sds(ITERS)],
        (pair, eta, *[q for v in placed for q in v]),
        name="last",
        out_specs=[VMEM, VMEM, SMEM],
    )
    return pressure, residual, norms


def solution(mesh):
    placed = (P(None, "gx", "gy", "gz"), P("gx", "gy", "gz"), P(), P())
    return jax.shard_map(
        functools.partial(per_device, mesh.shape["gx"], mesh.shape["gy"], mesh.shape["gz"]),
        mesh=mesh,
        in_specs=placed,
        out_specs=(P("gx", "gy", "gz"), P("gx", "gy", "gz"), P()),
        check_vma=False,
    )
```

```python
import functools

import jax
import jax.numpy as jnp
from jax import lax
from jax.experimental import pallas as pl
from jax.experimental.pallas import tpu as pltpu
from jax.sharding import PartitionSpec as P

ITERS = 3
SWEEPS = 4
OMEGA = 0.8
HALO = 4
LANES = 128
F32 = jnp.float32

VMEM = pl.BlockSpec(memory_space=pltpu.VMEM)
SMEM = pl.BlockSpec(memory_space=pltpu.SMEM)


def sds(*shape):
    return jax.ShapeDtypeStruct(shape, F32)


def call(kernel, outs, ins, specs=None, scratch=(), flops=10**6, name=None, out_specs=None):
    return pl.pallas_call(
        kernel,
        out_shape=outs,
        in_specs=specs or [VMEM] * len(ins),
        out_specs=out_specs or jax.tree.map(lambda _: VMEM, outs),
        scratch_shapes=list(scratch),
        compiler_params=pltpu.CompilerParams(vmem_limit_bytes=24 * 2**20),
        cost_estimate=pl.CostEstimate(flops=flops, bytes_accessed=2**20, transcendentals=0),
        name=name,
    )(*ins)


def pick(items, index):
    value = items[0]
    for k in range(1, len(items)):
        value = jnp.where(index == k, items[k], value)
    return value


def split_z(value, core, n):
    blocks = [value[..., t * LANES : (t + 1) * LANES] for t in range(n)]
    return [pick(blocks, lax.rem(core + j, n)) for j in range(n)]


def join_own(parts, core):
    n = len(parts)
    return jnp.concatenate([pick(parts, lax.rem(t - core + n, n)) for t in range(n)], -1)


def join_received(parts, core):
    n = len(parts)
    return jnp.concatenate([pick(parts, lax.rem(core - t + n, n)) for t in range(n)], -1)


def up_y(row):
    return pltpu.roll(row, row.shape[0] - 1, 0)


def down_y(row):
    return pltpu.roll(row, 1, 0)


def up_z(row):
    return pltpu.roll(row, row.shape[1] - 1, 1)


def down_z(row):
    return pltpu.roll(row, 1, 1)


def rows_loop(start, stop, body, step=3):
    count = stop - start
    whole = count // step

    def chunk(i, carry):
        for k in range(step):
            body(start + i * step + k)
        return carry

    if whole > 1:
        lax.fori_loop(0, whole, chunk, 0)
        rest = start + whole * step
    else:
        rest = start
    for r in range(rest, stop):
        body(r)


def exchange_y(a, b, n):
    even = [(i, i ^ 1) for i in range(n)]
    odd = [(i, i + (1 if i % 2 else -1)) for i in range(1, n - 1)]
    return lax.ppermute(a, "gy", even), lax.ppermute(b, "gy", odd)


def exchange_x(a, b, n):
    even = [(i, i ^ 1) for i in range(n)]
    odd = [(i, (i + (1 if i % 2 else -1)) % n) for i in range(n)]
    return lax.ppermute(a, ("gx", "gz"), even), lax.ppermute(b, ("gx", "gz"), odd)


def core_shift(value, n, j):
    return lax.ppermute(value, "gz", [(i, (i + j) % n) for i in range(n)])


def prep_kernel(n, force, phase, table, *outs):
    core = lax.axis_index("gz")
    rows = outs[0].shape[1]
    eta_out = outs[n]
    levels = table.shape[0]

    def one(r):
        ids = phase[r]
        eta = jnp.zeros(ids.shape, F32)
        for level in range(levels):
            eta = jnp.where(ids == level, table[level], eta)
        eta_out[r] = eta

    rows_loop(0, phase.shape[0], one, 4)
    for j in range(n):
        base = lax.rem(core + j, n) * rows

        def two(r, j=j, base=base):
            for c in range(3):
                outs[j][c, r] = force[c, base + r]
            outs[j][3, r] = eta_out[base + r]

        rows_loop(0, rows, two, 4)


def gather_kernel(n, *refs):
    parts = refs[:n]
    full, send_a, send_b = refs[n:]
    core = lax.axis_index("gz")
    odd = Place().odd_y
    fields, rows, ys, _ = full.shape
    h = HALO

    for c in range(fields):

        def one(r, c=c):
            row = join_received([p[c, r] for p in parts], core)
            full[c, r] = row
            send_a[c * rows + r] = jnp.where(odd, row[:h], row[ys - h :])
            send_b[c * rows + r] = jnp.where(odd, row[ys - h :], row[:h])

        rows_loop(0, rows, one, 4)
    for r in range(rows):
        line = full[3, r, ys - h - 1 : ys - h, :]
        send_a[fields * rows + r // 4, r % 4 : r % 4 + 1, :] = line
        send_b[fields * rows + r // 4, r % 4 : r % 4 + 1, :] = line


def edge_list(h):
    tiles = []
    for c in range(4):
        for k in range(h):
            if c in (1, 2) and k == 0:
                continue
            for q in range(2 if c == 0 and k == 0 else 3):
                tiles.append((c, k, q))
    return tiles + [(3, -1, 0), (3, -1, 1)]


def force_edges_kernel(full, ya, yb, send_a, send_b):
    place = Place()
    odd_x = place.odd
    _, rows, ys, _ = full.shape
    h = HALO
    for send, first in ((send_a, odd_x), (send_b, jnp.logical_not(odd_x))):
        for t, (c, k, q) in enumerate(edge_list(h)):
            r = jnp.where(first, h - 1 - k, rows - h + k)
            if q < 2:
                send[t] = full[c, r, 8 * q : 8 * q + 8, :]
            else:
                a, b = ya[c * rows + r], yb[c * rows + r]
                send[t, :h, :] = place.up(a, b)
                send[t, h:, :] = place.low(a, b)


def edges_kernel(p, ya, yb, *rest):
    send_a, send_b = rest[-2:]
    place = Place()
    rows = p.shape[0]
    h = HALO
    for send, first in ((send_a, place.odd), (send_b, jnp.logical_not(place.odd))):
        start = jnp.where(first, 0, rows - h)
        for k in range(h):
            set_row(send, (k,), p[start + k], ya[start + k], yb[start + k], place)


class Rows:
    def __init__(self, early, late, first, end):
        self.early, self.late, self.first, self.end = early, late, first, end

    def __getitem__(self, index):
        r = index[-1] if isinstance(index, tuple) else index
        mine = not isinstance(r, int) or not self.first <= r < self.end
        return (self.late if mine else self.early)[index]


def spans(lo, hi, total):
    full = [(s, total - 1 - s) for s in range(SWEEPS)] + [(HALO, total - HALO)]
    inner = [(lo + s, hi - s) for s in range(SWEEPS)] + [(lo + SWEEPS, hi - SWEEPS + 1)]
    inner = [i if i[0] < i[1] else (f[0], f[0]) for f, i in zip(full, inner)]
    return full, inner


def outside(full, inner):
    return list(range(full[0], inner[0])) + list(range(inner[1], full[1]))


def update(source, b, w, kx, ky, kz, target, r):
    keep = 1.0 - OMEGA
    here_x, past_x, here_y, here_z = kx[r], kx[r - 1], ky[r], kz[r]
    for c in range(3):
        u = source[c, r]
        near = here_x * source[c, r + 1] + past_x * source[c, r - 1]
        near = near + here_y * up_y(u) + down_y(here_y * u)
        near = near + here_z * up_z(u) + down_z(here_z * u)
        target[c, r] = keep * u + (b[c, r] + w[c, r] * near)


def diverge(v, r):
    vy, vz = v[1, r], v[2, r]
    lane = lax.broadcasted_iota(jnp.int32, vz.shape, 1)
    out = v[0, r - 1] - v[0, r]
    out = out + (down_y(vy) - vy)
    return out + (jnp.where(lane == 0, 0.0, down_z(vz)) - vz)


def inner_solve(b, levels, out, inner, w, kx, ky, kz):
    source = b
    for s in range(1, SWEEPS):
        target = levels[s - 1]

        def one(r, source=source, target=target):
            update(source, b, w, kx, ky, kz, target, r)

        rows_loop(*inner[s], one)
        source = target

    def last(r):
        out[r - HALO] = diverge(source, r)

    rows_loop(*inner[SWEEPS], last, 2)


def outer_solve(b, levels, buffers, inner, full, w, kx, ky, kz, emit):
    source = b
    for s in range(1, SWEEPS):
        target = buffers[s - 1]
        for r in outside(full[s], inner[s]):
            update(source, b, w, kx, ky, kz, target, r)
        source = Rows(levels[s - 1], target, *inner[s])
    for r in outside(full[SWEEPS], inner[SWEEPS]):
        emit(r - HALO, diverge(source, r))


def emit_result(v_own, v_others, p_out, send_a, send_b, eta_at, sums=None):
    n = 1 + len(v_others)
    core = lax.axis_index("gz")
    odd = Place().odd_y
    h = HALO

    def emit(r, out):
        ys = v_own.shape[1]
        out = out[:ys]
        parts = split_z(out, core, n)
        v_own[r] = parts[0]
        for ref, part in zip(v_others, parts[1:]):
            ref[r] = part
        if p_out is not None:
            p = eta_at(r) * out
            p_out[r] = p
            send_a[r] = jnp.where(odd, p[:h], p[ys - h :])
            send_b[r] = jnp.where(odd, p[ys - h :], p[:h])
        if sums is not None:
            sums(r, out)

    return emit


def fold(value):
    total = value[:8]
    for k in range(1, value.shape[0] // 8):
        total = total + value[8 * k : 8 * k + 8]
    lanes = total[:, :LANES]
    for t in range(1, total.shape[1] // LANES):
        lanes = lanes + total[:, t * LANES : (t + 1) * LANES]
    return lanes


class Place:
    def __init__(self):
        chain = lax.axis_size("gx") * lax.axis_size("gz")
        self.x = lax.axis_index("gx") * lax.axis_size("gz") + lax.axis_index("gz")
        self.odd = lax.rem(self.x, 2) == 1
        self.below_x, self.above_x = self.x > 0, self.x < chain - 1
        self.odd_y = lax.rem(lax.axis_index("gy"), 2) == 1

    def up(self, a, b):
        return jnp.where(self.odd_y, b, a)

    def low(self, a, b):
        return jnp.where(self.odd_y, a, b)


def set_row(ref, index, row, a, b, place):
    ys, h = row.shape[0], a.shape[0]
    ref[(*index, slice(0, ys), slice(None))] = row
    ref[(*index, slice(ys, ys + h), slice(None))] = place.up(a, b)
    ref[(*index, slice(ys + h, ys + 2 * h), slice(None))] = place.low(a, b)


def coefs_at(sizes, place, slots, lanes, rows, ys, flags):
    h = HALO
    slot = lax.broadcasted_iota(jnp.int32, (slots, lanes), 0)
    at_y = lax.axis_index("gy") * ys + slot - jnp.where(slot >= ys + h, slots, 0)
    at_z = lax.broadcasted_iota(jnp.int32, (slots, lanes), 1)
    in_y = (at_y >= 0) & (at_y < sizes[1])
    y_up, y_low = at_y + 1 < sizes[1], at_y >= 1
    z_up, z_low = at_z + 1 < sizes[2], at_z >= 1
    wall = [jnp.where(flags[k] == 0, 1.0, 0.0).astype(F32) for k in range(6)]

    def coefs(r, mid, before, after, line, force_at, kx, ky, kz, w, b):
        at_x = place * rows - h + r
        x_up = jnp.full(mid.shape, at_x + 1, jnp.int32) < sizes[0]
        x_low = jnp.full(mid.shape, at_x, jnp.int32) >= 1
        inside = in_y & jnp.broadcast_to((at_x >= 0) & (at_x < sizes[0]), mid.shape)
        y_before = jnp.where(slot == ys + h, line, down_y(mid))
        sides = (
            (x_up, after, x_low, before),
            (y_up, up_y(mid), y_low, y_before),
            (z_up, up_z(mid), z_low, down_z(mid)),
        )
        diag = [jnp.zeros_like(mid) for _ in range(3)]
        for axis, (up_in, up, low_in, low) in enumerate(sides):
            up, low = 0.5 * (mid + up), 0.5 * (mid + low)
            (kx, ky, kz)[axis][r] = jnp.where(up_in, up, 0.0)
            for c in range(3):
                low_wall = 1.0 if c == axis else wall[2 * axis]
                up_wall = 1.0 if c == axis else wall[2 * axis + 1]
                diag[c] = diag[c] + jnp.where(up_in, up, up_wall * mid)
                diag[c] = diag[c] + jnp.where(low_in, low, low_wall * mid)
        for c in range(3):
            weight = jnp.where(inside, OMEGA / diag[c], 0.0)
            w[c, r] = weight
            b[c, r] = weight * force_at(c)

    return coefs


def first_inner(sizes, full, ya, yb, flags, kx, ky, kz, w, b, *rest):
    levels, (out, force, eta, line) = rest[: SWEEPS - 1], rest[SWEEPS - 1 :]
    fields, rows, ys, lanes = full.shape
    h = HALO
    place = Place()
    slots, total = ys + 2 * h, rows + 2 * h
    for c in range(fields):

        def one(r, c=c):
            to, index = (force, (c, r + h)) if c < 3 else (eta, (r + h,))
            set_row(to, index, full[c, r], ya[c * rows + r], yb[c * rows + r], place)

        rows_loop(0, rows, one, 4)
    for q in range(rows // 4):
        block = place.low(ya[fields * rows + q], yb[fields * rows + q])
        for k in range(4):
            line[h + 4 * q + k] = block[k : k + 1]
    coefs = coefs_at(sizes, place.x, slots, lanes, rows, ys, flags)

    def at(r):
        coefs(r, eta[r], eta[r - 1], eta[r + 1], line[r], lambda c: force[c, r], kx, ky, kz, w, b)

    _, inner = spans(h + 1, h + rows - 1, total)
    rows_loop(*inner[0], at, 1)
    inner_solve(b, levels, out, inner, w, kx, ky, kz)


def first_outer(n, sizes, *refs):
    full, ya, yb, xa, xb, flags, *early = refs[: 11 + SWEEPS]
    kx0, ky0, kz0, w0, b0, *levels, out0 = early
    refs = refs[11 + SWEEPS :]
    v_own, v_others, refs = refs[0], refs[1:n], refs[n:]
    p_out, send_a, send_b, kx, ky, kz, w = refs[:7]
    force, eta, line, b, *buffers = refs[7:]
    fields, rows, ys, lanes = full.shape
    h = HALO
    place = Place()
    odd_x = place.odd
    slots, total = ys + 2 * h, rows + 2 * h
    ranges, inner = spans(h + 1, h + rows - 1, total)
    todo = outside((0, total), inner[0])
    for r in sorted({min(max(q + d, h), h + rows - 1) for q in todo for d in (-1, 0, 1)}):
        k = r - h
        for c in range(fields):
            to, index = (force, (c, r)) if c < 3 else (eta, (r + 1,))
            set_row(to, index, full[c, k], ya[c * rows + k], yb[c * rows + k], place)
        block = fields * rows + k // 4
        line[r] = place.low(ya[block], yb[block])[k % 4 : k % 4 + 1]
    blank = jnp.zeros((slots, lanes), F32)
    line_blank = jnp.zeros((1, lanes), F32)
    for k in range(h):
        for r in (k, h + rows + k):
            line[r] = line_blank
    for c in range(3):
        force[c, 0] = blank
        force[c, total - 1] = blank
    eta[0] = blank
    for t, (c, k, q) in enumerate(edge_list(h)):
        lower, upper = jnp.where(odd_x, xa[t], xb[t]), jnp.where(odd_x, xb[t], xa[t])
        where = slice(8 * q, 8 * q + 8)
        if c < 3:
            force[c, k, where, :] = lower
            force[c, total - 1 - k, where, :] = upper
        else:
            eta[1 + k, where, :] = lower
            if k >= 0:
                eta[total - k, where, :] = upper
    coefs = coefs_at(sizes, place.x, slots, lanes, rows, ys, flags)
    for r in todo:
        after = eta[min(r + 2, total)]
        coefs(r, eta[r + 1], eta[r], after, line[r], lambda c: force[c, r], kx, ky, kz, w, b)

    def carry(r):
        kx[r], ky[r], kz[r] = kx0[r], ky0[r], kz0[r]
        for c in range(3):
            w[c, r] = w0[c, r]

    rows_loop(*inner[0], carry, 2)
    b = Rows(b0, b, *inner[0])
    emit = emit_result(v_own, v_others, p_out, send_a, send_b, lambda r: full[3, r])
    outer_solve(b, levels, buffers, inner, ranges, w, kx, ky, kz, emit)
    rows_loop(inner[SWEEPS][0] - h, inner[SWEEPS][1] - h, lambda r: emit(r, out0[r]), 4)


def next_inner(extra, p_in, ya, yb, kx, ky, kz, w, *rest):
    p, b, *rest = rest[extra:]
    levels, out = rest[: SWEEPS - 1], rest[SWEEPS - 1]
    rows = p_in.shape[0]
    h = HALO
    place = Place()

    def fill(r):
        set_row(p, (r + h,), p_in[r], ya[r], yb[r], place)

    rows_loop(0, rows, fill, 4)
    _, inner = spans(h, h + rows - 1, rows + 2 * h)
    rows_loop(*inner[0], lambda r: grads(p, w, b, r), 2)
    inner_solve(b, levels, out, inner, w, kx, ky, kz)


def grads(p, w, b, r):
    mid = p[r]
    lanes = mid.shape[1]
    lane = lax.broadcasted_iota(jnp.int32, mid.shape, 1)
    b[0, r] = w[0, r] * (p[r + 1] - mid)
    b[1, r] = w[1, r] * (up_y(mid) - mid)
    b[2, r] = w[2, r] * (jnp.where(lane == lanes - 1, 0.0, up_z(mid)) - mid)


def next_outer(n, last, p_in, xa, xb, full, kx, ky, kz, w, p0, b0, *refs):
    levels, out0, refs = refs[: SWEEPS - 1], refs[SWEEPS - 1], refs[SWEEPS:]
    if last:
        partials, refs = refs[:ITERS], refs[ITERS:]
    v_own, v_others, refs = refs[0], refs[1:n], refs[n:]
    p_out = send_a = send_b = sums = None
    if last:
        moment, acc, refs = v_others[-1].at[p_in.shape[0]], refs[-1], refs[:-1]
        acc[...] = jnp.zeros_like(acc)

        def sums(r, v):
            acc[...] = acc[...] + v * p_in[r]
    else:
        p_out, send_a, send_b, *refs = refs
    p, b, *buffers = refs
    rows = p_in.shape[0]
    h = HALO
    place = Place()
    for k in range(h):
        lower, upper = jnp.where(place.odd, xa[k], xb[k]), jnp.where(place.odd, xb[k], xa[k])
        p[k] = jnp.where(place.below_x, lower, 0.0)
        p[h + rows + k] = jnp.where(place.above_x, upper, 0.0)
    ranges, inner = spans(h, h + rows - 1, rows + 2 * h)
    p = Rows(p0, p, h, h + rows)
    for r in outside(ranges[0], inner[0]):
        grads(p, w, b, r)
    b = Rows(b0, b, *inner[0])
    emit = emit_result(v_own, v_others, p_out, send_a, send_b, lambda r: full[3, r], sums)
    outer_solve(b, levels, buffers, inner, ranges, w, kx, ky, kz, emit)
    rows_loop(inner[SWEEPS][0] - h, inner[SWEEPS][1] - h, lambda r: emit(r, out0[r]), 4)
    if last:
        moment[...] = jnp.zeros_like(moment)
        at = 0
        for ref in partials:
            for k in range(ref.shape[0]):
                moment[at : at + 1, :] = jnp.sum(ref[k], 0, keepdims=True)
                at += 1
        moment[at : at + 1, :] = jnp.sum(fold(acc[...]), 0, keepdims=True)


def moments_kernel(n, step, *refs):
    moment, acc = refs[-2:]
    p, refs = refs[0], refs[1:-2]
    before, refs = (refs[0], refs[1:]) if step else (None, refs)
    groups = [refs[k * n : (k + 1) * n] for k in range(step + 1)]
    core = lax.axis_index("gz")
    acc[...] = jnp.zeros_like(acc)

    def one(r):
        v = join_own([q[r] for q in groups[-1]], core)
        others = ([before[r]] if step else []) + [p[r], v]
        others += [join_own([q[r] for q in group], core) for group in groups[:-1]]
        for k, other in enumerate(others):
            acc[k] = acc[k] + v * other

    rows_loop(0, p.shape[0], one, 4)
    for k in range(acc.shape[0]):
        moment[k] = fold(acc[k])


def two_sum(a, b):
    s = a + b
    t = s - a
    return s, (a - (s - t)) + (b - t)


def quick(a, b):
    s = a + b
    return s, b - (s - a)


def halves(a):
    t = 4097.0 * a
    high = t - (t - a)
    return high, a - high


def two_prod(a, b):
    p = a * b
    ah, al = halves(a)
    bh, bl = halves(b)
    return p, ((ah * bh - p) + ah * bl + al * bh) + al * bl


def add(a, b):
    s, e = two_sum(a[0], b[0])
    return quick(s, e + (a[1] + b[1]))


def mul(a, b):
    p, e = two_prod(a[0], b[0])
    return quick(p, e + (a[0] * b[1] + a[1] * b[0]))


def neg(a):
    return -a[0], -a[1]


def div(a, b):
    q = a[0] / b[0]
    r = add(a, neg(mul((q, jnp.zeros_like(q)), b)))
    q2 = r[0] / b[0]
    return quick(q, q2)


def twice(a):
    return 2.0 * a[0], 2.0 * a[1]


def last_kernel(n, cells, sums, eta, *refs):
    own = refs[: 4 * n]
    pressure, residual, norms = refs[4 * n :]
    core = lax.axis_index("gz")
    pair = (sums[0], sums[1])
    for shift in (64, 32, 16, 8, 4, 2, 1):
        pair = add(pair, tuple(pltpu.roll(x, shift, 1) for x in pair))
    item = [(pair[0][k : k + 1], pair[1][k : k + 1]) for k in range(12)]
    m0, n00, m1, m2, n11, n01, m3, m4, n22, n02, n12, m5 = item
    one = (jnp.ones_like(m0[0]), jnp.zeros_like(m0[0]))
    a0 = div(m0, m1)
    c11 = neg(a0)
    g1 = mul(c11, add(m1, mul(c11, m2)))
    b0 = div(g1, m0)
    d10, d11 = add(one, b0), c11
    a1 = div(g1, mul(d11, add(mul(d10, m2), mul(d11, m3))))
    c21 = add(c11, neg(mul(a1, d10)))
    c22 = neg(mul(a1, d11))
    g2 = mul(c22, add(m2, add(mul(c21, m3), mul(c22, m4))))
    b1 = div(g2, g1)
    d20 = add(one, mul(b1, d10))
    d21 = add(c21, mul(b1, d11))
    d22 = c22
    a2 = div(g2, mul(d22, add(mul(d20, m3), add(mul(d21, m4), mul(d22, m5)))))
    p0 = add(a0, add(mul(a1, d10), mul(a2, d20)))[0]
    p1 = add(mul(a1, d11), mul(a2, d21))[0]
    p2 = mul(a2, d22)[0]
    r1 = add(c21, neg(mul(a2, d20)))[0]
    r2 = add(c22, neg(mul(a2, d21)))[0]
    r3 = -p2
    norm1 = add(n00, mul(c11, add(twice(n01), mul(c11, n11))))
    norm2 = add(n00, mul(c21, add(twice(n01), mul(c21, n11))))
    norm2 = add(norm2, mul(c22, add(twice(n02), add(mul(twice(c21), n12), mul(c22, n22)))))
    for k, value in enumerate((n00, norm1, norm2)):
        norms[k] = (value[0] / cells)[0, 0]
    rows = own[0].shape[0]
    for j in range(n):
        base = lax.rem(core - j + n, n) * rows
        v0, v1, v2, v3 = (own[k * n + j] for k in range(4))

        def one_row(r, base=base, v0=v0, v1=v1, v2=v2, v3=v3):
            x0, x1, x2, x3 = v0[r], v1[r], v2[r], v3[r]
            pressure[base + r] = eta[base + r] * (p0 * x0 + p1 * x1 + p2 * x2)
            residual[base + r] = (x0 + r1 * x1) + (r2 * x2 + r3 * x3)

        rows_loop(0, rows, one_row, 4)


def add_pairs(a, b):
    s, e = two_sum(a[0], b[0])
    return jnp.stack([s, e + (a[1] + b[1])])


def sum_along(pair, axis, n, stride=1):
    count = n // stride
    if count < 2:
        return pair
    terms = [pair]
    for k in range(1, count):
        moves = [(i, (i + k * stride) % n) for i in range(n)]
        terms.append(lax.ppermute(pair, axis, moves))
    me = lax.axis_index(axis) // stride
    terms = [pick(terms, lax.rem(me - j + count, count)) for j in range(count)]
    while len(terms) > 1:
        rest = terms[len(terms) // 2 * 2 :]
        terms = [add_pairs(a, b) for a, b in zip(terms[::2], terms[1::2])] + rest
    return terms[0]


def per_device(nx, ny, nz, force, phase, table, flags):
    h = HALO
    wide, ys, lanes = phase.shape
    rows = wide // nz
    zs = lanes * nz
    sizes = (wide * nx, ys * ny, zs)
    slots, total = ys + 2 * h, rows + 2 * h
    cells = float(sizes[0] * sizes[1] * sizes[2])
    chain = nx * nz

    parts = call(
        functools.partial(prep_kernel, nz),
        [sds(4, rows, ys, lanes)] * nz + [sds(*phase.shape)],
        (force, phase, table),
        [VMEM, VMEM, SMEM],
        name="prep",
    )
    eta = parts[-1]
    parts = [parts[0]] + [core_shift(parts[j], nz, j) for j in range(1, nz)]
    full, ya, yb = call(
        functools.partial(gather_kernel, nz),
        [
            sds(4, rows, ys, zs),
            sds(4 * rows + rows // 4, h, zs),
            sds(4 * rows + rows // 4, h, zs),
        ],
        parts,
        name="gather",
    )
    ya, yb = exchange_y(ya, yb, ny)
    edge = sds(len(edge_list(h)), 8, zs)
    xa, xb = call(force_edges_kernel, [edge, edge], (full, ya, yb), name="force_edges")
    xa, xb = exchange_x(xa, xb, chain)

    v_shape = [sds(rows, ys, lanes)] * nz
    sent = [sds(rows, ys, zs), sds(rows, h, zs), sds(rows, h, zs)]
    scalar, vector = sds(total, slots, zs), sds(3, total, slots, zs)
    field = pltpu.VMEM((3, total, slots, zs), F32)
    line = pltpu.VMEM((total, 1, zs), F32)
    heavy = 4 * 10**7
    early = call(
        functools.partial(first_inner, sizes),
        [scalar] * 3 + [vector] * (1 + SWEEPS) + [sds(rows, slots, zs)],
        (full, ya, yb, flags),
        [VMEM] * 3 + [SMEM],
        [field, pltpu.VMEM((total, slots, zs), F32), line],
        heavy,
        "first_inner",
    )
    outs = call(
        functools.partial(first_outer, nz, sizes),
        v_shape + sent + [scalar] * 3 + [vector],
        (full, ya, yb, xa, xb, flags, *early),
        [VMEM] * 5 + [SMEM] + [VMEM] * len(early),
        [field, pltpu.VMEM((total + 1, slots, zs), F32), line] + [field] * SWEEPS,
        heavy,
        "first",
    )
    vs, ps, moments = [list(outs[:nz])], [outs[nz]], []
    ya, yb = outs[nz + 1 : nz + 3]
    coefs = outs[nz + 3 :]
    placed = []
    for step in range(1, ITERS + 1):
        last = step == ITERS
        p, v = ps[-1], vs[-1]
        placed.append([v[0]] + [core_shift(v[j], nz, j) for j in range(1, nz)])
        count = 2 if step == 1 else 2 + step
        moments.append(
            call(
                functools.partial(moments_kernel, nz, step - 1),
                [sds(count, 8, LANES)],
                (p, *ps[:-1][-1:], *[q for v in vs for q in v]),
                None,
                [pltpu.VMEM((count, ys, zs), F32)],
                name="moments",
            )[0]
        )
        ya, yb = exchange_y(ya, yb, ny)
        edge = sds(h, slots, zs)
        xa, xb = call(edges_kernel, [edge, edge], (p, ya, yb, moments[-1]), name="edges")
        xa, xb = exchange_x(xa, xb, chain)
        early = call(
            functools.partial(next_inner, nz - 1),
            [scalar] + [vector] * SWEEPS + [sds(rows, slots, zs)],
            (p, ya, yb, *coefs, *placed[-1][1:]),
            None,
            (),
            heavy,
            "next_inner",
        )
        joint = v_shape[:-1] + [sds(rows + 1, ys, lanes)]
        outs = call(
            functools.partial(next_outer, nz, last),
            joint if last else v_shape + sent,
            (p, xa, xb, full, *coefs, *early, *(moments if last else ())),
            None,
            [pltpu.VMEM((total, slots, zs), F32)]
            + [field] * SWEEPS
            + ([pltpu.VMEM((ys, zs), F32)] if last else []),
            heavy,
            "next",
        )
        vs.append(list(outs[:nz]))
        if not last:
            ps.append(outs[nz])
            ya, yb = outs[nz + 1 : nz + 3]

    v = vs[-1]
    moved = [v[0]] + [core_shift(v[j], nz, j) for j in range(1, nz)]
    placed.append(moved)
    mine, theirs = v[-1][rows], moved[-1][rows]
    if nz > 2:
        theirs = lax.ppermute(mine, "gz", [(k, k ^ 1) for k in range(nz)])
    pair = jnp.stack(two_sum(mine, theirs))
    pair = sum_along(pair, "gz", nz, 2)
    pair = sum_along(sum_along(pair, "gx", nx), "gy", ny)
    pressure, residual, norms = call(
        functools.partial(last_kernel, nz, cells),
        [sds(*phase.shape), sds(*phase.shape), sds(ITERS)],
        (pair, eta, *[q for v in placed for q in v]),
        name="last",
        out_specs=[VMEM, VMEM, SMEM],
    )
    return pressure, residual, norms


def solution(mesh):
    placed = (P(None, "gx", "gy", "gz"), P("gx", "gy", "gz"), P(), P())
    return jax.shard_map(
        functools.partial(per_device, mesh.shape["gx"], mesh.shape["gy"], mesh.shape["gz"]),
        mesh=mesh,
        in_specs=placed,
        out_specs=(P("gx", "gy", "gz"), P("gx", "gy", "gz"), P()),
        check_vma=False,
    )
```

```python
import functools

import jax
import jax.numpy as jnp
from jax import lax
from jax.experimental import pallas as pl
from jax.experimental.pallas import tpu as pltpu
from jax.sharding import PartitionSpec as P

ITERS = 3
SWEEPS = 4
OMEGA = 0.8
HALO = 4
LANES = 128
F32 = jnp.float32

VMEM = pl.BlockSpec(memory_space=pltpu.VMEM)
SMEM = pl.BlockSpec(memory_space=pltpu.SMEM)


def sds(*shape):
    return jax.ShapeDtypeStruct(shape, F32)


def call(kernel, outs, ins, specs=None, scratch=(), flops=10**6, name=None, out_specs=None):
    return pl.pallas_call(
        kernel,
        out_shape=outs,
        in_specs=specs or [VMEM] * len(ins),
        out_specs=out_specs or jax.tree.map(lambda _: VMEM, outs),
        scratch_shapes=list(scratch),
        compiler_params=pltpu.CompilerParams(vmem_limit_bytes=24 * 2**20),
        cost_estimate=pl.CostEstimate(flops=flops, bytes_accessed=2**20, transcendentals=0),
        name=name,
    )(*ins)


def pick(items, index):
    value = items[0]
    for k in range(1, len(items)):
        value = jnp.where(index == k, items[k], value)
    return value


def split_z(value, core, n):
    blocks = [value[..., t * LANES : (t + 1) * LANES] for t in range(n)]
    return [pick(blocks, lax.rem(core + j, n)) for j in range(n)]


def join_own(parts, core):
    n = len(parts)
    return jnp.concatenate([pick(parts, lax.rem(t - core + n, n)) for t in range(n)], -1)


def join_received(parts, core):
    n = len(parts)
    return jnp.concatenate([pick(parts, lax.rem(core - t + n, n)) for t in range(n)], -1)


def up_y(row):
    return pltpu.roll(row, row.shape[0] - 1, 0)


def down_y(row):
    return pltpu.roll(row, 1, 0)


def up_z(row):
    return pltpu.roll(row, row.shape[1] - 1, 1)


def down_z(row):
    return pltpu.roll(row, 1, 1)


def rows_loop(start, stop, body, step=3):
    count = stop - start
    whole = count // step

    def chunk(i, carry):
        for k in range(step):
            body(start + i * step + k)
        return carry

    if whole > 1:
        lax.fori_loop(0, whole, chunk, 0)
        rest = start + whole * step
    else:
        rest = start
    for r in range(rest, stop):
        body(r)


def exchange_y(a, b, ny, nz):
    even = [(i, i ^ 1) for i in range(ny)]
    odd = []
    for y in range(ny):
        for z in range(nz):
            other = (y + (1 if y % 2 else -1), z) if 0 < y < ny - 1 else (y, z ^ 1)
            odd.append((y * nz + z, other[0] * nz + other[1]))
    return lax.ppermute(a, "gy", even), lax.ppermute(b, ("gy", "gz"), odd)


def exchange_x(a, b, n):
    even = [(i, i ^ 1) for i in range(n)]
    odd = [(i, (i + (1 if i % 2 else -1)) % n) for i in range(n)]
    return lax.ppermute(a, ("gx", "gz"), even), lax.ppermute(b, ("gx", "gz"), odd)


def core_shift(value, n, j):
    return lax.ppermute(value, "gz", [(i, (i + j) % n) for i in range(n)])


def prep_kernel(n, force, phase, table, *outs):
    core = lax.axis_index("gz")
    rows = outs[0].shape[1]
    eta_out = outs[n]
    levels = table.shape[0]

    def one(r):
        ids = phase[r]
        eta = jnp.zeros(ids.shape, F32)
        for level in range(levels):
            eta = jnp.where(ids == level, table[level], eta)
        eta_out[r] = eta

    rows_loop(0, phase.shape[0], one, 4)
    for j in range(n):
        base = lax.rem(core + j, n) * rows

        def two(r, j=j, base=base):
            for c in range(3):
                outs[j][c, r] = force[c, base + r]
            outs[j][3, r] = eta_out[base + r]

        rows_loop(0, rows, two, 4)


def gather_kernel(n, *refs):
    parts = refs[:n]
    full, send_a, send_b = refs[n:]
    core = lax.axis_index("gz")
    odd = Place().odd_y
    fields, rows, ys, _ = full.shape
    h = HALO

    for c in range(fields):

        def one(r, c=c):
            row = join_received([p[c, r] for p in parts], core)
            full[c, r] = row
            send_a[c * rows + r] = jnp.where(odd, row[:h], row[ys - h :])
            send_b[c * rows + r] = jnp.where(odd, row[ys - h :], row[:h])

        rows_loop(0, rows, one, 4)
    for r in range(rows):
        line = full[3, r, ys - h - 1 : ys - h, :]
        send_a[fields * rows + r // 4, r % 4 : r % 4 + 1, :] = line
        send_b[fields * rows + r // 4, r % 4 : r % 4 + 1, :] = line


def edge_list(h):
    tiles = []
    for c in range(4):
        for k in range(h):
            if c in (1, 2) and k == 0:
                continue
            for q in range(2 if c == 0 and k == 0 else 3):
                tiles.append((c, k, q))
    return tiles + [(3, -1, 0), (3, -1, 1)]


def force_edges_kernel(full, ya, yb, send_a, send_b):
    place = Place()
    odd_x = place.odd
    _, rows, ys, _ = full.shape
    h = HALO
    for send, first in ((send_a, odd_x), (send_b, jnp.logical_not(odd_x))):
        for t, (c, k, q) in enumerate(edge_list(h)):
            r = jnp.where(first, h - 1 - k, rows - h + k)
            if q < 2:
                send[t] = full[c, r, 8 * q : 8 * q + 8, :]
            else:
                a, b = ya[c * rows + r], yb[c * rows + r]
                send[t, :h, :] = place.up(a, b)
                send[t, h:, :] = place.low(a, b)


def edges_kernel(p, ya, yb, *rest):
    send_a, send_b = rest[-2:]
    place = Place()
    rows = p.shape[0]
    h = HALO
    for send, first in ((send_a, place.odd), (send_b, jnp.logical_not(place.odd))):
        start = jnp.where(first, 0, rows - h)
        for k in range(h):
            set_row(send, (k,), p[start + k], ya[start + k], yb[start + k], place)


class Rows:
    def __init__(self, early, late, first, end):
        self.early, self.late, self.first, self.end = early, late, first, end

    def __getitem__(self, index):
        r = index[-1] if isinstance(index, tuple) else index
        mine = not isinstance(r, int) or not self.first <= r < self.end
        return (self.late if mine else self.early)[index]


def spans(lo, hi, total):
    full = [(s, total - 1 - s) for s in range(SWEEPS)] + [(HALO, total - HALO)]
    inner = [(lo + s, hi - s) for s in range(SWEEPS)] + [(lo + SWEEPS, hi - SWEEPS + 1)]
    inner = [i if i[0] < i[1] else (f[0], f[0]) for f, i in zip(full, inner)]
    return full, inner


def outside(full, inner):
    return list(range(full[0], inner[0])) + list(range(inner[1], full[1]))


def update(source, b, w, kx, ky, kz, target, r):
    keep = 1.0 - OMEGA
    here_x, past_x, here_y, here_z = kx[r], kx[r - 1], ky[r], kz[r]
    for c in range(3):
        u = source[c, r]
        near = here_x * source[c, r + 1] + past_x * source[c, r - 1]
        near = near + here_y * up_y(u) + down_y(here_y * u)
        near = near + here_z * up_z(u) + down_z(here_z * u)
        target[c, r] = keep * u + (b[c, r] + w[c, r] * near)


def diverge(v, r):
    vy, vz = v[1, r], v[2, r]
    lane = lax.broadcasted_iota(jnp.int32, vz.shape, 1)
    out = v[0, r - 1] - v[0, r]
    out = out + (down_y(vy) - vy)
    return out + (jnp.where(lane == 0, 0.0, down_z(vz)) - vz)


def inner_solve(b, levels, out, inner, w, kx, ky, kz):
    source = b
    for s in range(1, SWEEPS):
        target = levels[s - 1]

        def one(r, source=source, target=target):
            update(source, b, w, kx, ky, kz, target, r)

        rows_loop(*inner[s], one)
        source = target

    def last(r):
        out[r - HALO] = diverge(source, r)

    rows_loop(*inner[SWEEPS], last, 2)


def outer_solve(b, levels, buffers, inner, full, w, kx, ky, kz, emit):
    source = b
    for s in range(1, SWEEPS):
        target = buffers[s - 1]
        for r in outside(full[s], inner[s]):
            update(source, b, w, kx, ky, kz, target, r)
        source = Rows(levels[s - 1], target, *inner[s])
    for r in outside(full[SWEEPS], inner[SWEEPS]):
        emit(r - HALO, diverge(source, r))


def emit_result(v_own, v_others, p_out, send_a, send_b, eta_at, sums=None):
    n = 1 + len(v_others)
    core = lax.axis_index("gz")
    odd = Place().odd_y
    h = HALO

    def emit(r, out):
        ys = v_own.shape[1]
        out = out[:ys]
        parts = split_z(out, core, n)
        v_own[r] = parts[0]
        for ref, part in zip(v_others, parts[1:]):
            ref[r] = part
        if p_out is not None:
            p = eta_at(r) * out
            p_out[r] = p
            send_a[r] = jnp.where(odd, p[:h], p[ys - h :])
            send_b[r] = jnp.where(odd, p[ys - h :], p[:h])
        if sums is not None:
            sums(r, out)

    return emit


def fold(value):
    total = value[:8]
    for k in range(1, value.shape[0] // 8):
        total = total + value[8 * k : 8 * k + 8]
    lanes = total[:, :LANES]
    for t in range(1, total.shape[1] // LANES):
        lanes = lanes + total[:, t * LANES : (t + 1) * LANES]
    return lanes


class Place:
    def __init__(self):
        chain = lax.axis_size("gx") * lax.axis_size("gz")
        self.x = lax.axis_index("gx") * lax.axis_size("gz") + lax.axis_index("gz")
        self.odd = lax.rem(self.x, 2) == 1
        self.below_x, self.above_x = self.x > 0, self.x < chain - 1
        y = lax.axis_index("gy")
        self.odd_y = lax.rem(y, 2) == 1
        self.below_y, self.above_y = y > 0, y < lax.axis_size("gy") - 1

    def up(self, a, b):
        return jnp.where(self.above_y, jnp.where(self.odd_y, b, a), 0.0)

    def low(self, a, b):
        return jnp.where(self.below_y, jnp.where(self.odd_y, a, b), 0.0)


def set_row(ref, index, row, a, b, place):
    ys, h = row.shape[0], a.shape[0]
    ref[(*index, slice(0, ys), slice(None))] = row
    ref[(*index, slice(ys, ys + h), slice(None))] = place.up(a, b)
    ref[(*index, slice(ys + h, ys + 2 * h), slice(None))] = place.low(a, b)


def coefs_at(sizes, place, slots, lanes, rows, ys, flags):
    h = HALO
    slot = lax.broadcasted_iota(jnp.int32, (slots, lanes), 0)
    at_y = lax.axis_index("gy") * ys + slot - jnp.where(slot >= ys + h, slots, 0)
    at_z = lax.broadcasted_iota(jnp.int32, (slots, lanes), 1)
    in_y = (at_y >= 0) & (at_y < sizes[1])
    y_up, y_low = at_y + 1 < sizes[1], at_y >= 1
    z_up, z_low = at_z + 1 < sizes[2], at_z >= 1
    wall = [jnp.where(flags[k] == 0, 1.0, 0.0).astype(F32) for k in range(6)]

    def coefs(r, mid, before, after, line, force_at, kx, ky, kz, w, b):
        at_x = place * rows - h + r
        x_up = jnp.full(mid.shape, at_x + 1, jnp.int32) < sizes[0]
        x_low = jnp.full(mid.shape, at_x, jnp.int32) >= 1
        inside = in_y & jnp.broadcast_to((at_x >= 0) & (at_x < sizes[0]), mid.shape)
        y_before = jnp.where(slot == ys + h, line, down_y(mid))
        sides = (
            (x_up, after, x_low, before),
            (y_up, up_y(mid), y_low, y_before),
            (z_up, up_z(mid), z_low, down_z(mid)),
        )
        diag = [jnp.zeros_like(mid) for _ in range(3)]
        for axis, (up_in, up, low_in, low) in enumerate(sides):
            up, low = 0.5 * (mid + up), 0.5 * (mid + low)
            (kx, ky, kz)[axis][r] = jnp.where(up_in, up, 0.0)
            for c in range(3):
                low_wall = 1.0 if c == axis else wall[2 * axis]
                up_wall = 1.0 if c == axis else wall[2 * axis + 1]
                diag[c] = diag[c] + jnp.where(up_in, up, up_wall * mid)
                diag[c] = diag[c] + jnp.where(low_in, low, low_wall * mid)
        for c in range(3):
            weight = jnp.where(inside, OMEGA / diag[c], 0.0)
            w[c, r] = weight
            b[c, r] = weight * force_at(c)

    return coefs


def first_inner(sizes, full, ya, yb, flags, kx, ky, kz, w, b, *rest):
    levels, (out, force, eta, line) = rest[: SWEEPS - 1], rest[SWEEPS - 1 :]
    fields, rows, ys, lanes = full.shape
    h = HALO
    place = Place()
    slots, total = ys + 2 * h, rows + 2 * h
    for c in range(fields):

        def one(r, c=c):
            to, index = (force, (c, r + h)) if c < 3 else (eta, (r + h,))
            set_row(to, index, full[c, r], ya[c * rows + r], yb[c * rows + r], place)

        rows_loop(0, rows, one, 4)
    for q in range(rows // 4):
        block = place.low(ya[fields * rows + q], yb[fields * rows + q])
        for k in range(4):
            line[h + 4 * q + k] = block[k : k + 1]
    coefs = coefs_at(sizes, place.x, slots, lanes, rows, ys, flags)

    def at(r):
        coefs(r, eta[r], eta[r - 1], eta[r + 1], line[r], lambda c: force[c, r], kx, ky, kz, w, b)

    _, inner = spans(h + 1, h + rows - 1, total)
    rows_loop(*inner[0], at, 1)
    inner_solve(b, levels, out, inner, w, kx, ky, kz)


def first_outer(n, sizes, *refs):
    full, ya, yb, xa, xb, flags, *early = refs[: 11 + SWEEPS]
    kx0, ky0, kz0, w0, b0, *levels, out0 = early
    refs = refs[11 + SWEEPS :]
    v_own, v_others, refs = refs[0], refs[1:n], refs[n:]
    p_out, send_a, send_b, kx, ky, kz, w = refs[:7]
    force, eta, line, b, *buffers = refs[7:]
    fields, rows, ys, lanes = full.shape
    h = HALO
    place = Place()
    odd_x = place.odd
    slots, total = ys + 2 * h, rows + 2 * h
    ranges, inner = spans(h + 1, h + rows - 1, total)
    todo = outside((0, total), inner[0])
    for r in sorted({min(max(q + d, h), h + rows - 1) for q in todo for d in (-1, 0, 1)}):
        k = r - h
        for c in range(fields):
            to, index = (force, (c, r)) if c < 3 else (eta, (r + 1,))
            set_row(to, index, full[c, k], ya[c * rows + k], yb[c * rows + k], place)
        block = fields * rows + k // 4
        line[r] = place.low(ya[block], yb[block])[k % 4 : k % 4 + 1]
    blank = jnp.zeros((slots, lanes), F32)
    line_blank = jnp.zeros((1, lanes), F32)
    for k in range(h):
        for r in (k, h + rows + k):
            line[r] = line_blank
    for c in range(3):
        force[c, 0] = blank
        force[c, total - 1] = blank
    eta[0] = blank
    for t, (c, k, q) in enumerate(edge_list(h)):
        lower, upper = jnp.where(odd_x, xa[t], xb[t]), jnp.where(odd_x, xb[t], xa[t])
        where = slice(8 * q, 8 * q + 8)
        if c < 3:
            force[c, k, where, :] = lower
            force[c, total - 1 - k, where, :] = upper
        else:
            eta[1 + k, where, :] = lower
            if k >= 0:
                eta[total - k, where, :] = upper
    coefs = coefs_at(sizes, place.x, slots, lanes, rows, ys, flags)
    for r in todo:
        after = eta[min(r + 2, total)]
        coefs(r, eta[r + 1], eta[r], after, line[r], lambda c: force[c, r], kx, ky, kz, w, b)

    def carry(r):
        kx[r], ky[r], kz[r] = kx0[r], ky0[r], kz0[r]
        for c in range(3):
            w[c, r] = w0[c, r]

    rows_loop(*inner[0], carry, 2)
    b = Rows(b0, b, *inner[0])
    emit = emit_result(v_own, v_others, p_out, send_a, send_b, lambda r: full[3, r])
    outer_solve(b, levels, buffers, inner, ranges, w, kx, ky, kz, emit)
    rows_loop(inner[SWEEPS][0] - h, inner[SWEEPS][1] - h, lambda r: emit(r, out0[r]), 4)


def next_inner(extra, p_in, ya, yb, kx, ky, kz, w, *rest):
    p, b, *rest = rest[extra:]
    levels, out = rest[: SWEEPS - 1], rest[SWEEPS - 1]
    rows = p_in.shape[0]
    h = HALO
    place = Place()

    def fill(r):
        set_row(p, (r + h,), p_in[r], ya[r], yb[r], place)

    rows_loop(0, rows, fill, 4)
    _, inner = spans(h, h + rows - 1, rows + 2 * h)
    rows_loop(*inner[0], lambda r: grads(p, w, b, r), 2)
    inner_solve(b, levels, out, inner, w, kx, ky, kz)


def grads(p, w, b, r):
    mid = p[r]
    lanes = mid.shape[1]
    lane = lax.broadcasted_iota(jnp.int32, mid.shape, 1)
    b[0, r] = w[0, r] * (p[r + 1] - mid)
    b[1, r] = w[1, r] * (up_y(mid) - mid)
    b[2, r] = w[2, r] * (jnp.where(lane == lanes - 1, 0.0, up_z(mid)) - mid)


def next_outer(n, last, p_in, xa, xb, full, kx, ky, kz, w, p0, b0, *refs):
    levels, out0, refs = refs[: SWEEPS - 1], refs[SWEEPS - 1], refs[SWEEPS:]
    if last:
        partials, refs = refs[:ITERS], refs[ITERS:]
    v_own, v_others, refs = refs[0], refs[1:n], refs[n:]
    p_out = send_a = send_b = sums = None
    if last:
        moment, acc, refs = v_others[-1].at[p_in.shape[0]], refs[-1], refs[:-1]
        acc[...] = jnp.zeros_like(acc)

        def sums(r, v):
            acc[...] = acc[...] + v * p_in[r]
    else:
        p_out, send_a, send_b, *refs = refs
    p, b, *buffers = refs
    rows = p_in.shape[0]
    h = HALO
    place = Place()
    for k in range(h):
        lower, upper = jnp.where(place.odd, xa[k], xb[k]), jnp.where(place.odd, xb[k], xa[k])
        p[k] = jnp.where(place.below_x, lower, 0.0)
        p[h + rows + k] = jnp.where(place.above_x, upper, 0.0)
    ranges, inner = spans(h, h + rows - 1, rows + 2 * h)
    p = Rows(p0, p, h, h + rows)
    for r in outside(ranges[0], inner[0]):
        grads(p, w, b, r)
    b = Rows(b0, b, *inner[0])
    emit = emit_result(v_own, v_others, p_out, send_a, send_b, lambda r: full[3, r], sums)
    outer_solve(b, levels, buffers, inner, ranges, w, kx, ky, kz, emit)
    rows_loop(inner[SWEEPS][0] - h, inner[SWEEPS][1] - h, lambda r: emit(r, out0[r]), 4)
    if last:
        moment[...] = jnp.zeros_like(moment)
        at = 0
        for ref in partials:
            for k in range(ref.shape[0]):
                moment[at : at + 1, :] = jnp.sum(ref[k], 0, keepdims=True)
                at += 1
        moment[at : at + 1, :] = jnp.sum(fold(acc[...]), 0, keepdims=True)


def moments_kernel(n, step, *refs):
    moment, acc = refs[-2:]
    p, refs = refs[0], refs[1:-2]
    before, refs = (refs[0], refs[1:]) if step else (None, refs)
    groups = [refs[k * n : (k + 1) * n] for k in range(step + 1)]
    core = lax.axis_index("gz")
    acc[...] = jnp.zeros_like(acc)

    def one(r):
        v = join_own([q[r] for q in groups[-1]], core)
        others = ([before[r]] if step else []) + [p[r], v]
        others += [join_own([q[r] for q in group], core) for group in groups[:-1]]
        for k, other in enumerate(others):
            acc[k] = acc[k] + v * other

    rows_loop(0, p.shape[0], one, 4)
    for k in range(acc.shape[0]):
        moment[k] = fold(acc[k])


def two_sum(a, b):
    s = a + b
    t = s - a
    return s, (a - (s - t)) + (b - t)


def quick(a, b):
    s = a + b
    return s, b - (s - a)


def halves(a):
    t = 4097.0 * a
    high = t - (t - a)
    return high, a - high


def two_prod(a, b):
    p = a * b
    ah, al = halves(a)
    bh, bl = halves(b)
    return p, ((ah * bh - p) + ah * bl + al * bh) + al * bl


def add(a, b):
    s, e = two_sum(a[0], b[0])
    return quick(s, e + (a[1] + b[1]))


def mul(a, b):
    p, e = two_prod(a[0], b[0])
    return quick(p, e + (a[0] * b[1] + a[1] * b[0]))


def neg(a):
    return -a[0], -a[1]


def div(a, b):
    q = a[0] / b[0]
    r = add(a, neg(mul((q, jnp.zeros_like(q)), b)))
    q2 = r[0] / b[0]
    return quick(q, q2)


def twice(a):
    return 2.0 * a[0], 2.0 * a[1]


def last_kernel(n, cells, sums, eta, *refs):
    own = refs[: 4 * n]
    pressure, residual, norms = refs[4 * n :]
    core = lax.axis_index("gz")
    pair = (sums[0], sums[1])
    for shift in (64, 32, 16, 8, 4, 2, 1):
        pair = add(pair, tuple(pltpu.roll(x, shift, 1) for x in pair))
    item = [(pair[0][k : k + 1], pair[1][k : k + 1]) for k in range(12)]
    m0, n00, m1, m2, n11, n01, m3, m4, n22, n02, n12, m5 = item
    one = (jnp.ones_like(m0[0]), jnp.zeros_like(m0[0]))
    a0 = div(m0, m1)
    c11 = neg(a0)
    g1 = mul(c11, add(m1, mul(c11, m2)))
    b0 = div(g1, m0)
    d10, d11 = add(one, b0), c11
    a1 = div(g1, mul(d11, add(mul(d10, m2), mul(d11, m3))))
    c21 = add(c11, neg(mul(a1, d10)))
    c22 = neg(mul(a1, d11))
    g2 = mul(c22, add(m2, add(mul(c21, m3), mul(c22, m4))))
    b1 = div(g2, g1)
    d20 = add(one, mul(b1, d10))
    d21 = add(c21, mul(b1, d11))
    d22 = c22
    a2 = div(g2, mul(d22, add(mul(d20, m3), add(mul(d21, m4), mul(d22, m5)))))
    p0 = add(a0, add(mul(a1, d10), mul(a2, d20)))[0]
    p1 = add(mul(a1, d11), mul(a2, d21))[0]
    p2 = mul(a2, d22)[0]
    r1 = add(c21, neg(mul(a2, d20)))[0]
    r2 = add(c22, neg(mul(a2, d21)))[0]
    r3 = -p2
    norm1 = add(n00, mul(c11, add(twice(n01), mul(c11, n11))))
    norm2 = add(n00, mul(c21, add(twice(n01), mul(c21, n11))))
    norm2 = add(norm2, mul(c22, add(twice(n02), add(mul(twice(c21), n12), mul(c22, n22)))))
    for k, value in enumerate((n00, norm1, norm2)):
        norms[k] = (value[0] / cells)[0, 0]
    rows = own[0].shape[0]
    for j in range(n):
        base = lax.rem(core - j + n, n) * rows
        v0, v1, v2, v3 = (own[k * n + j] for k in range(4))

        def one_row(r, base=base, v0=v0, v1=v1, v2=v2, v3=v3):
            x0, x1, x2, x3 = v0[r], v1[r], v2[r], v3[r]
            pressure[base + r] = eta[base + r] * (p0 * x0 + p1 * x1 + p2 * x2)
            residual[base + r] = (x0 + r1 * x1) + (r2 * x2 + r3 * x3)

        rows_loop(0, rows, one_row, 4)


def add_pairs(a, b):
    s, e = two_sum(a[0], b[0])
    return jnp.stack([s, e + (a[1] + b[1])])


def sum_along(pair, axis, n, stride=1):
    count = n // stride
    if count < 2:
        return pair
    terms = [pair]
    for k in range(1, count):
        moves = [(i, (i + k * stride) % n) for i in range(n)]
        terms.append(lax.ppermute(pair, axis, moves))
    me = lax.axis_index(axis) // stride
    terms = [pick(terms, lax.rem(me - j + count, count)) for j in range(count)]
    while len(terms) > 1:
        rest = terms[len(terms) // 2 * 2 :]
        terms = [add_pairs(a, b) for a, b in zip(terms[::2], terms[1::2])] + rest
    return terms[0]


def per_device(nx, ny, nz, force, phase, table, flags):
    h = HALO
    wide, ys, lanes = phase.shape
    rows = wide // nz
    zs = lanes * nz
    sizes = (wide * nx, ys * ny, zs)
    slots, total = ys + 2 * h, rows + 2 * h
    cells = float(sizes[0] * sizes[1] * sizes[2])
    chain = nx * nz

    parts = call(
        functools.partial(prep_kernel, nz),
        [sds(4, rows, ys, lanes)] * nz + [sds(*phase.shape)],
        (force, phase, table),
        [VMEM, VMEM, SMEM],
        name="prep",
    )
    eta = parts[-1]
    parts = [parts[0]] + [core_shift(parts[j], nz, j) for j in range(1, nz)]
    full, ya, yb = call(
        functools.partial(gather_kernel, nz),
        [
            sds(4, rows, ys, zs),
            sds(4 * rows + rows // 4, h, zs),
            sds(4 * rows + rows // 4, h, zs),
        ],
        parts,
        name="gather",
    )
    ya, yb = exchange_y(ya, yb, ny, nz)
    edge = sds(len(edge_list(h)), 8, zs)
    xa, xb = call(force_edges_kernel, [edge, edge], (full, ya, yb), name="force_edges")
    xa, xb = exchange_x(xa, xb, chain)

    v_shape = [sds(rows, ys, lanes)] * nz
    sent = [sds(rows, ys, zs), sds(rows, h, zs), sds(rows, h, zs)]
    scalar, vector = sds(total, slots, zs), sds(3, total, slots, zs)
    field = pltpu.VMEM((3, total, slots, zs), F32)
    line = pltpu.VMEM((total, 1, zs), F32)
    heavy = 4 * 10**7
    early = call(
        functools.partial(first_inner, sizes),
        [scalar] * 3 + [vector] * (1 + SWEEPS) + [sds(rows, slots, zs)],
        (full, ya, yb, flags),
        [VMEM] * 3 + [SMEM],
        [field, pltpu.VMEM((total, slots, zs), F32), line],
        heavy,
        "first_inner",
    )
    outs = call(
        functools.partial(first_outer, nz, sizes),
        v_shape + sent + [scalar] * 3 + [vector],
        (full, ya, yb, xa, xb, flags, *early),
        [VMEM] * 5 + [SMEM] + [VMEM] * len(early),
        [field, pltpu.VMEM((total + 1, slots, zs), F32), line] + [field] * SWEEPS,
        heavy,
        "first",
    )
    vs, ps, moments = [list(outs[:nz])], [outs[nz]], []
    ya, yb = outs[nz + 1 : nz + 3]
    coefs = outs[nz + 3 :]
    placed = []
    for step in range(1, ITERS + 1):
        last = step == ITERS
        p, v = ps[-1], vs[-1]
        placed.append([v[0]] + [core_shift(v[j], nz, j) for j in range(1, nz)])
        count = 2 if step == 1 else 2 + step
        moments.append(
            call(
                functools.partial(moments_kernel, nz, step - 1),
                [sds(count, 8, LANES)],
                (p, *ps[:-1][-1:], *[q for v in vs for q in v]),
                None,
                [pltpu.VMEM((count, ys, zs), F32)],
                name="moments",
            )[0]
        )
        ya, yb = exchange_y(ya, yb, ny, nz)
        edge = sds(h, slots, zs)
        xa, xb = call(edges_kernel, [edge, edge], (p, ya, yb, moments[-1]), name="edges")
        xa, xb = exchange_x(xa, xb, chain)
        early = call(
            functools.partial(next_inner, nz - 1),
            [scalar] + [vector] * SWEEPS + [sds(rows, slots, zs)],
            (p, ya, yb, *coefs, *placed[-1][1:]),
            None,
            (),
            heavy,
            "next_inner",
        )
        joint = v_shape[:-1] + [sds(rows + 1, ys, lanes)]
        outs = call(
            functools.partial(next_outer, nz, last),
            joint if last else v_shape + sent,
            (p, xa, xb, full, *coefs, *early, *(moments if last else ())),
            None,
            [pltpu.VMEM((total, slots, zs), F32)]
            + [field] * SWEEPS
            + ([pltpu.VMEM((ys, zs), F32)] if last else []),
            heavy,
            "next",
        )
        vs.append(list(outs[:nz]))
        if not last:
            ps.append(outs[nz])
            ya, yb = outs[nz + 1 : nz + 3]

    v = vs[-1]
    moved = [v[0]] + [core_shift(v[j], nz, j) for j in range(1, nz)]
    placed.append(moved)
    mine, theirs = v[-1][rows], moved[-1][rows]
    if nz > 2:
        theirs = lax.ppermute(mine, "gz", [(k, k ^ 1) for k in range(nz)])
    pair = jnp.stack(two_sum(mine, theirs))
    pair = sum_along(pair, "gz", nz, 2)
    pair = sum_along(sum_along(pair, "gx", nx), "gy", ny)
    pressure, residual, norms = call(
        functools.partial(last_kernel, nz, cells),
        [sds(*phase.shape), sds(*phase.shape), sds(ITERS)],
        (pair, eta, *[q for v in placed for q in v]),
        name="last",
        out_specs=[VMEM, VMEM, SMEM],
    )
    return pressure, residual, norms


def solution(mesh):
    placed = (P(None, "gx", "gy", "gz"), P("gx", "gy", "gz"), P(), P())
    return jax.shard_map(
        functools.partial(per_device, mesh.shape["gx"], mesh.shape["gy"], mesh.shape["gz"]),
        mesh=mesh,
        in_specs=placed,
        out_specs=(P("gx", "gy", "gz"), P("gx", "gy", "gz"), P()),
        check_vma=False,
    )
```

```python
import functools

import jax
import jax.numpy as jnp
from jax import lax
from jax.experimental import pallas as pl
from jax.experimental.pallas import tpu as pltpu
from jax.sharding import PartitionSpec as P

ITERS = 3
SWEEPS = 4
OMEGA = 0.8
HALO = 4
LANES = 128
F32 = jnp.float32

VMEM = pl.BlockSpec(memory_space=pltpu.VMEM)
SMEM = pl.BlockSpec(memory_space=pltpu.SMEM)


def sds(*shape):
    return jax.ShapeDtypeStruct(shape, F32)


def call(kernel, outs, ins, specs=None, scratch=(), flops=10**6, name=None, out_specs=None):
    return pl.pallas_call(
        kernel,
        out_shape=outs,
        in_specs=specs or [VMEM] * len(ins),
        out_specs=out_specs or jax.tree.map(lambda _: VMEM, outs),
        scratch_shapes=list(scratch),
        compiler_params=pltpu.CompilerParams(vmem_limit_bytes=24 * 2**20),
        cost_estimate=pl.CostEstimate(flops=flops, bytes_accessed=2**20, transcendentals=0),
        name=name,
    )(*ins)


def pick(items, index):
    value = items[0]
    for k in range(1, len(items)):
        value = jnp.where(index == k, items[k], value)
    return value


def split_z(value, core, n):
    blocks = [value[..., t * LANES : (t + 1) * LANES] for t in range(n)]
    return [pick(blocks, lax.rem(core + j, n)) for j in range(n)]


def join_own(parts, core):
    n = len(parts)
    return jnp.concatenate([pick(parts, lax.rem(t - core + n, n)) for t in range(n)], -1)


def join_received(parts, core):
    n = len(parts)
    return jnp.concatenate([pick(parts, lax.rem(core - t + n, n)) for t in range(n)], -1)


def up_y(row):
    return pltpu.roll(row, row.shape[0] - 1, 0)


def down_y(row):
    return pltpu.roll(row, 1, 0)


def up_z(row):
    return pltpu.roll(row, row.shape[1] - 1, 1)


def down_z(row):
    return pltpu.roll(row, 1, 1)


def rows_loop(start, stop, body, step=3):
    count = stop - start
    whole = count // step

    def chunk(i, carry):
        for k in range(step):
            body(start + i * step + k)
        return carry

    if whole > 1:
        lax.fori_loop(0, whole, chunk, 0)
        rest = start + whole * step
    else:
        rest = start
    for r in range(rest, stop):
        body(r)


def exchange_y(a, b, ny, nz):
    even = [(i, i ^ 1) for i in range(ny)]
    odd = []
    for y in range(ny):
        for z in range(nz):
            other = (y + (1 if y % 2 else -1), z) if 0 < y < ny - 1 else (y, z ^ 1)
            odd.append((y * nz + z, other[0] * nz + other[1]))
    return lax.ppermute(a, "gy", even), lax.ppermute(b, ("gy", "gz"), odd)


def exchange_x(a, b, n):
    even = [(i, i ^ 1) for i in range(n)]
    odd = [(i, (i + (1 if i % 2 else -1)) % n) for i in range(n)]
    return lax.ppermute(a, ("gx", "gz"), even), lax.ppermute(b, ("gx", "gz"), odd)


def core_shift(value, n, j):
    return lax.ppermute(value, "gz", [(i, (i + j) % n) for i in range(n)])


def prep_kernel(n, force, phase, table, *outs):
    core = lax.axis_index("gz")
    rows = outs[0].shape[1]
    eta_out = outs[n]
    levels = table.shape[0]

    def one(r):
        ids = phase[r]
        eta = jnp.zeros(ids.shape, F32)
        for level in range(levels):
            eta = jnp.where(ids == level, table[level], eta)
        eta_out[r] = eta

    rows_loop(0, phase.shape[0], one, 4)
    for j in range(n):
        base = lax.rem(core + j, n) * rows

        def two(r, j=j, base=base):
            for c in range(3):
                outs[j][c, r] = force[c, base + r]
            outs[j][3, r] = eta_out[base + r]

        rows_loop(0, rows, two, 4)


def gather_kernel(n, *refs):
    parts = refs[:n]
    full, send_a, send_b = refs[n:]
    core = lax.axis_index("gz")
    odd = Place().odd_y
    fields, rows, ys, _ = full.shape
    h = HALO

    for c in range(fields):

        def one(r, c=c):
            row = join_received([p[c, r] for p in parts], core)
            full[c, r] = row
            send_a[c * rows + r] = jnp.where(odd, row[:h], row[ys - h :])
            send_b[c * rows + r] = jnp.where(odd, row[ys - h :], row[:h])

        rows_loop(0, rows, one, 4)
    for r in range(rows):
        line = full[3, r, ys - h - 1 : ys - h, :]
        send_a[fields * rows + r // 4, r % 4 : r % 4 + 1, :] = line
        send_b[fields * rows + r // 4, r % 4 : r % 4 + 1, :] = line


def edge_list(h):
    tiles = []
    for c in range(4):
        for k in range(h):
            if c in (1, 2) and k == 0:
                continue
            for q in range(2 if c == 0 and k == 0 else 3):
                tiles.append((c, k, q))
    return tiles + [(3, -1, 0), (3, -1, 1)]


def force_edges_kernel(full, ya, yb, send_a, send_b):
    place = Place()
    odd_x = place.odd
    _, rows, ys, _ = full.shape
    h = HALO
    for send, first in ((send_a, odd_x), (send_b, jnp.logical_not(odd_x))):
        for t, (c, k, q) in enumerate(edge_list(h)):
            r = jnp.where(first, h - 1 - k, rows - h + k)
            if q < 2:
                send[t] = full[c, r, 8 * q : 8 * q + 8, :]
            else:
                a, b = ya[c * rows + r], yb[c * rows + r]
                send[t, :h, :] = place.up(a, b)
                send[t, h:, :] = place.low(a, b)


def edges_kernel(p, ya, yb, *rest):
    send_a, send_b = rest[-2:]
    place = Place()
    rows = p.shape[0]
    h = HALO
    for send, first in ((send_a, place.odd), (send_b, jnp.logical_not(place.odd))):
        start = jnp.where(first, 0, rows - h)
        for k in range(h):
            set_row(send, (k,), p[start + k], ya[start + k], yb[start + k], place)


class Rows:
    def __init__(self, early, late, first, end):
        self.early, self.late, self.first, self.end = early, late, first, end

    def __getitem__(self, index):
        r = index[-1] if isinstance(index, tuple) else index
        mine = not isinstance(r, int) or not self.first <= r < self.end
        return (self.late if mine else self.early)[index]


def spans(lo, hi, total):
    full = [(s, total - 1 - s) for s in range(SWEEPS)] + [(HALO, total - HALO)]
    inner = [(lo + s, hi - s) for s in range(SWEEPS)] + [(lo + SWEEPS, hi - SWEEPS + 1)]
    inner = [i if i[0] < i[1] else (f[0], f[0]) for f, i in zip(full, inner)]
    return full, inner


def outside(full, inner, side):
    return range(full[0], inner[0]) if side == "low" else range(inner[1], full[1])


def on_side(near, body):
    odd = Place().odd
    pl.when(odd)(lambda: body("low" if near else "high"))
    pl.when(jnp.logical_not(odd))(lambda: body("high" if near else "low"))


def update(source, b, w, kx, ky, kz, target, r):
    keep = 1.0 - OMEGA
    here_x, past_x, here_y, here_z = kx[r], kx[r - 1], ky[r], kz[r]
    for c in range(3):
        u = source[c, r]
        near = here_x * source[c, r + 1] + past_x * source[c, r - 1]
        near = near + here_y * up_y(u) + down_y(here_y * u)
        near = near + here_z * up_z(u) + down_z(here_z * u)
        target[c, r] = keep * u + (b[c, r] + w[c, r] * near)


def diverge(v, r):
    vy, vz = v[1, r], v[2, r]
    lane = lax.broadcasted_iota(jnp.int32, vz.shape, 1)
    out = v[0, r - 1] - v[0, r]
    out = out + (down_y(vy) - vy)
    return out + (jnp.where(lane == 0, 0.0, down_z(vz)) - vz)


def emit_early(emit, near_side, full, inner, out_inner, out_near):
    for r in outside(full[SWEEPS], inner[SWEEPS], near_side):
        emit(r - HALO, out_near[r - HALO])
    rows_loop(inner[SWEEPS][0] - HALO, inner[SWEEPS][1] - HALO, lambda r: emit(r, out_inner[r]), 4)


def inner_solve(b, levels, out, inner, w, kx, ky, kz):
    source = b
    for s in range(1, SWEEPS):
        target = levels[s - 1]

        def one(r, source=source, target=target):
            update(source, b, w, kx, ky, kz, target, r)

        rows_loop(*inner[s], one)
        source = target

    def last(r):
        out[r - HALO] = diverge(source, r)

    rows_loop(*inner[SWEEPS], last, 2)


def outer_solve(side, b, levels, buffers, inner, full, w, kx, ky, kz, emit):
    source = b
    for s in range(1, SWEEPS):
        target = buffers[s - 1]
        for r in outside(full[s], inner[s], side):
            update(source, b, w, kx, ky, kz, target, r)
        source = Rows(levels[s - 1], target, *inner[s])
    for r in outside(full[SWEEPS], inner[SWEEPS], side):
        emit(r - HALO, diverge(source, r))


def emit_result(v_own, v_others, p_out, send_a, send_b, eta_at, sums=None):
    n = 1 + len(v_others)
    core = lax.axis_index("gz")
    odd = Place().odd_y
    h = HALO

    def emit(r, out):
        ys = v_own.shape[1]
        out = out[:ys]
        parts = split_z(out, core, n)
        v_own[r] = parts[0]
        for ref, part in zip(v_others, parts[1:]):
            ref[r] = part
        if p_out is not None:
            p = eta_at(r) * out
            p_out[r] = p
            send_a[r] = jnp.where(odd, p[:h], p[ys - h :])
            send_b[r] = jnp.where(odd, p[ys - h :], p[:h])
        if sums is not None:
            sums(r, out)

    return emit


def fold(value):
    total = value[:8]
    for k in range(1, value.shape[0] // 8):
        total = total + value[8 * k : 8 * k + 8]
    lanes = total[:, :LANES]
    for t in range(1, total.shape[1] // LANES):
        lanes = lanes + total[:, t * LANES : (t + 1) * LANES]
    return lanes


class Place:
    def __init__(self):
        chain = lax.axis_size("gx") * lax.axis_size("gz")
        self.x = lax.axis_index("gx") * lax.axis_size("gz") + lax.axis_index("gz")
        self.odd = lax.rem(self.x, 2) == 1
        self.below_x, self.above_x = self.x > 0, self.x < chain - 1
        y = lax.axis_index("gy")
        self.odd_y = lax.rem(y, 2) == 1
        self.below_y, self.above_y = y > 0, y < lax.axis_size("gy") - 1

    def up(self, a, b):
        return jnp.where(self.above_y, jnp.where(self.odd_y, b, a), 0.0)

    def low(self, a, b):
        return jnp.where(self.below_y, jnp.where(self.odd_y, a, b), 0.0)


def set_row(ref, index, row, a, b, place):
    ys, h = row.shape[0], a.shape[0]
    ref[(*index, slice(0, ys), slice(None))] = row
    ref[(*index, slice(ys, ys + h), slice(None))] = place.up(a, b)
    ref[(*index, slice(ys + h, ys + 2 * h), slice(None))] = place.low(a, b)


def coefs_at(sizes, place, slots, lanes, rows, ys, flags):
    h = HALO
    slot = lax.broadcasted_iota(jnp.int32, (slots, lanes), 0)
    at_y = lax.axis_index("gy") * ys + slot - jnp.where(slot >= ys + h, slots, 0)
    at_z = lax.broadcasted_iota(jnp.int32, (slots, lanes), 1)
    in_y = (at_y >= 0) & (at_y < sizes[1])
    y_up, y_low = at_y + 1 < sizes[1], at_y >= 1
    z_up, z_low = at_z + 1 < sizes[2], at_z >= 1
    wall = [jnp.where(flags[k] == 0, 1.0, 0.0).astype(F32) for k in range(6)]

    def coefs(r, mid, before, after, line, force_at, kx, ky, kz, w, b):
        at_x = place * rows - h + r
        x_up = jnp.full(mid.shape, at_x + 1, jnp.int32) < sizes[0]
        x_low = jnp.full(mid.shape, at_x, jnp.int32) >= 1
        inside = in_y & jnp.broadcast_to((at_x >= 0) & (at_x < sizes[0]), mid.shape)
        y_before = jnp.where(slot == ys + h, line, down_y(mid))
        sides = (
            (x_up, after, x_low, before),
            (y_up, up_y(mid), y_low, y_before),
            (z_up, up_z(mid), z_low, down_z(mid)),
        )
        diag = [jnp.zeros_like(mid) for _ in range(3)]
        for axis, (up_in, up, low_in, low) in enumerate(sides):
            up, low = 0.5 * (mid + up), 0.5 * (mid + low)
            (kx, ky, kz)[axis][r] = jnp.where(up_in, up, 0.0)
            for c in range(3):
                low_wall = 1.0 if c == axis else wall[2 * axis]
                up_wall = 1.0 if c == axis else wall[2 * axis + 1]
                diag[c] = diag[c] + jnp.where(up_in, up, up_wall * mid)
                diag[c] = diag[c] + jnp.where(low_in, low, low_wall * mid)
        for c in range(3):
            weight = jnp.where(inside, OMEGA / diag[c], 0.0)
            w[c, r] = weight
            b[c, r] = weight * force_at(c)

    return coefs


def first_inner(sizes, full, ya, yb, flags, kx, ky, kz, w, b, *rest):
    levels, (out, force, eta, line) = rest[: SWEEPS - 1], rest[SWEEPS - 1 :]
    fields, rows, ys, lanes = full.shape
    h = HALO
    place = Place()
    slots, total = ys + 2 * h, rows + 2 * h
    for c in range(fields):

        def one(r, c=c):
            to, index = (force, (c, r + h)) if c < 3 else (eta, (r + h,))
            set_row(to, index, full[c, r], ya[c * rows + r], yb[c * rows + r], place)

        rows_loop(0, rows, one, 4)
    for q in range(rows // 4):
        block = place.low(ya[fields * rows + q], yb[fields * rows + q])
        for k in range(4):
            line[h + 4 * q + k] = block[k : k + 1]
    coefs = coefs_at(sizes, place.x, slots, lanes, rows, ys, flags)

    def at(r):
        coefs(r, eta[r], eta[r - 1], eta[r + 1], line[r], lambda c: force[c, r], kx, ky, kz, w, b)

    _, inner = spans(h + 1, h + rows - 1, total)
    rows_loop(*inner[0], at, 1)
    inner_solve(b, levels, out, inner, w, kx, ky, kz)


def first_side(n, sizes, near, *refs):
    count = 10 + SWEEPS
    full, ya, yb, xs, flags, *early = refs[:count]
    kx0, ky0, kz0, w0, b0, *levels, out0 = early
    if near:
        kx, ky, kz, w, out, *scratch = refs[count:]
    else:
        out_near, refs = refs[count], refs[count + 1 :]
        v_own, v_others, refs = refs[0], refs[1:n], refs[n:]
        p_out, send_a, send_b, kx, ky, kz, w, *scratch = refs
    force, eta, line, b, *buffers = scratch
    fields, rows, ys, lanes = full.shape
    h = HALO
    place = Place()
    slots, total = ys + 2 * h, rows + 2 * h
    ranges, inner = spans(h + 1, h + rows - 1, total)
    coefs = coefs_at(sizes, place.x, slots, lanes, rows, ys, flags)

    def body(side):
        todo = outside((0, total), inner[0], side)
        for r in sorted({min(max(q + d, h), h + rows - 1) for q in todo for d in (-1, 0, 1)}):
            k = r - h
            for c in range(fields):
                to, index = (force, (c, r)) if c < 3 else (eta, (r + 1,))
                set_row(to, index, full[c, k], ya[c * rows + k], yb[c * rows + k], place)
            block = fields * rows + k // 4
            line[r] = place.low(ya[block], yb[block])[k % 4 : k % 4 + 1]
        low = side == "low"
        blank = jnp.zeros((slots, lanes), F32)
        for k in range(h):
            line[k if low else h + rows + k] = jnp.zeros((1, lanes), F32)
        for c in range(3):
            force[c, 0 if low else total - 1] = blank
        if low:
            eta[0] = blank
        for t, (c, k, q) in enumerate(edge_list(h)):
            where = slice(8 * q, 8 * q + 8)
            if c < 3:
                force[c, k if low else total - 1 - k, where, :] = xs[t]
            elif low or k >= 0:
                eta[1 + k if low else total - k, where, :] = xs[t]
        for r in todo:
            after = eta[min(r + 2, total)]
            coefs(r, eta[r + 1], eta[r], after, line[r], lambda c: force[c, r], kx, ky, kz, w, b)
        early_late = [(kx0, kx), (ky0, ky), (kz0, kz), (w0, w), (b0, b)]
        kxs, kys, kzs, ws, bs = (Rows(e, f, *inner[0]) for e, f in early_late)
        if near:

            def emit(r, value):
                out[r] = value

            outer_solve(side, bs, levels, buffers, inner, ranges, ws, kxs, kys, kzs, emit)
        else:
            emit = emit_result(v_own, v_others, p_out, send_a, send_b, lambda r: full[3, r])
            outer_solve(side, bs, levels, buffers, inner, ranges, ws, kxs, kys, kzs, emit)
            emit_early(emit, "high" if low else "low", ranges, inner, out0, out_near)

    on_side(near, body)


def join_kernel(total, rows, *refs):
    inner_refs, near_refs, far_refs, outs = (refs[4 * k : 4 * k + 4] for k in range(4))
    _, inner = spans(HALO + 1, HALO + rows - 1, total)

    def carry(source, r):
        for k in range(3):
            outs[k][r] = source[k][r]
        for c in range(3):
            outs[3][c, r] = source[3][c, r]

    rows_loop(*inner[0], lambda r: carry(inner_refs, r), 2)
    for near, source in ((True, near_refs), (False, far_refs)):

        def body(side, source=source):
            for r in outside((0, total), inner[0], side):
                carry(source, r)

        on_side(near, body)


def next_inner(extra, p_in, ya, yb, kx, ky, kz, w, *rest):
    p, b, *rest = rest[extra:]
    levels, out = rest[: SWEEPS - 1], rest[SWEEPS - 1]
    rows = p_in.shape[0]
    h = HALO
    place = Place()

    def fill(r):
        set_row(p, (r + h,), p_in[r], ya[r], yb[r], place)

    rows_loop(0, rows, fill, 4)
    _, inner = spans(h, h + rows - 1, rows + 2 * h)
    rows_loop(*inner[0], lambda r: grads(p, w, b, r), 2)
    inner_solve(b, levels, out, inner, w, kx, ky, kz)


def grads(p, w, b, r):
    mid = p[r]
    lanes = mid.shape[1]
    lane = lax.broadcasted_iota(jnp.int32, mid.shape, 1)
    b[0, r] = w[0, r] * (p[r + 1] - mid)
    b[1, r] = w[1, r] * (up_y(mid) - mid)
    b[2, r] = w[2, r] * (jnp.where(lane == lanes - 1, 0.0, up_z(mid)) - mid)


def next_side(n, near, last, p_in, xs, kx, ky, kz, w, p0, b0, *refs):
    levels, refs = refs[: SWEEPS - 1], refs[SWEEPS - 1 :]
    if near:
        out, *scratch = refs
    else:
        full, out0, out_near, refs = refs[0], refs[1], refs[2], refs[3:]
        sums = p_out = send_a = send_b = None
        if last:
            partials, refs = refs[:ITERS], refs[ITERS:]
        v_own, v_others, refs = refs[0], refs[1:n], refs[n:]
        if last:
            moment, acc, refs = v_others[-1].at[p_in.shape[0]], refs[-1], refs[:-1]
            acc[...] = jnp.zeros_like(acc)

            def sums(r, v):
                acc[...] = acc[...] + v * p_in[r]
        else:
            p_out, send_a, send_b, *refs = refs
        scratch = refs
    p, b, *buffers = scratch
    rows = p_in.shape[0]
    h = HALO
    place = Place()
    ranges, inner = spans(h, h + rows - 1, rows + 2 * h)

    def body(side):
        low = side == "low"
        for k in range(h):
            row = xs[k]
            if not near:
                row = jnp.where(place.below_x if low else place.above_x, row, 0.0)
            p[k if low else h + rows + k] = row
        ps = Rows(p0, p, h, h + rows)
        for r in outside(ranges[0], inner[0], side):
            grads(ps, w, b, r)
        bs = Rows(b0, b, *inner[0])
        if near:

            def emit(r, value):
                out[r] = value

            outer_solve(side, bs, levels, buffers, inner, ranges, w, kx, ky, kz, emit)
        else:
            emit = emit_result(v_own, v_others, p_out, send_a, send_b, lambda r: full[3, r], sums)
            outer_solve(side, bs, levels, buffers, inner, ranges, w, kx, ky, kz, emit)
            emit_early(emit, "high" if low else "low", ranges, inner, out0, out_near)

    on_side(near, body)
    if not near and last:
        moment[...] = jnp.zeros_like(moment)
        at = 0
        for ref in partials:
            for k in range(ref.shape[0]):
                moment[at : at + 1, :] = jnp.sum(ref[k], 0, keepdims=True)
                at += 1
        moment[at : at + 1, :] = jnp.sum(fold(acc[...]), 0, keepdims=True)


def moments_kernel(n, step, *refs):
    moment, acc = refs[-2:]
    p, refs = refs[0], refs[1:-2]
    before, refs = (refs[0], refs[1:]) if step else (None, refs)
    groups = [refs[k * n : (k + 1) * n] for k in range(step + 1)]
    core = lax.axis_index("gz")
    acc[...] = jnp.zeros_like(acc)

    def one(r):
        v = join_own([q[r] for q in groups[-1]], core)
        others = ([before[r]] if step else []) + [p[r], v]
        others += [join_own([q[r] for q in group], core) for group in groups[:-1]]
        for k, other in enumerate(others):
            acc[k] = acc[k] + v * other

    rows_loop(0, p.shape[0], one, 4)
    for k in range(acc.shape[0]):
        moment[k] = fold(acc[k])


def two_sum(a, b):
    s = a + b
    t = s - a
    return s, (a - (s - t)) + (b - t)


def quick(a, b):
    s = a + b
    return s, b - (s - a)


def halves(a):
    t = 4097.0 * a
    high = t - (t - a)
    return high, a - high


def two_prod(a, b):
    p = a * b
    ah, al = halves(a)
    bh, bl = halves(b)
    return p, ((ah * bh - p) + ah * bl + al * bh) + al * bl


def add(a, b):
    s, e = two_sum(a[0], b[0])
    return quick(s, e + (a[1] + b[1]))


def mul(a, b):
    p, e = two_prod(a[0], b[0])
    return quick(p, e + (a[0] * b[1] + a[1] * b[0]))


def neg(a):
    return -a[0], -a[1]


def div(a, b):
    q = a[0] / b[0]
    r = add(a, neg(mul((q, jnp.zeros_like(q)), b)))
    q2 = r[0] / b[0]
    return quick(q, q2)


def twice(a):
    return 2.0 * a[0], 2.0 * a[1]


def last_kernel(n, cells, sums, eta, *refs):
    own = refs[: 4 * n]
    pressure, residual, norms = refs[4 * n :]
    core = lax.axis_index("gz")
    pair = (sums[0], sums[1])
    for shift in (64, 32, 16, 8, 4, 2, 1):
        pair = add(pair, tuple(pltpu.roll(x, shift, 1) for x in pair))
    item = [(pair[0][k : k + 1], pair[1][k : k + 1]) for k in range(12)]
    m0, n00, m1, m2, n11, n01, m3, m4, n22, n02, n12, m5 = item
    one = (jnp.ones_like(m0[0]), jnp.zeros_like(m0[0]))
    a0 = div(m0, m1)
    c11 = neg(a0)
    g1 = mul(c11, add(m1, mul(c11, m2)))
    b0 = div(g1, m0)
    d10, d11 = add(one, b0), c11
    a1 = div(g1, mul(d11, add(mul(d10, m2), mul(d11, m3))))
    c21 = add(c11, neg(mul(a1, d10)))
    c22 = neg(mul(a1, d11))
    g2 = mul(c22, add(m2, add(mul(c21, m3), mul(c22, m4))))
    b1 = div(g2, g1)
    d20 = add(one, mul(b1, d10))
    d21 = add(c21, mul(b1, d11))
    d22 = c22
    a2 = div(g2, mul(d22, add(mul(d20, m3), add(mul(d21, m4), mul(d22, m5)))))
    p0 = add(a0, add(mul(a1, d10), mul(a2, d20)))[0]
    p1 = add(mul(a1, d11), mul(a2, d21))[0]
    p2 = mul(a2, d22)[0]
    r1 = add(c21, neg(mul(a2, d20)))[0]
    r2 = add(c22, neg(mul(a2, d21)))[0]
    r3 = -p2
    norm1 = add(n00, mul(c11, add(twice(n01), mul(c11, n11))))
    norm2 = add(n00, mul(c21, add(twice(n01), mul(c21, n11))))
    norm2 = add(norm2, mul(c22, add(twice(n02), add(mul(twice(c21), n12), mul(c22, n22)))))
    for k, value in enumerate((n00, norm1, norm2)):
        norms[k] = (value[0] / cells)[0, 0]
    rows = own[0].shape[0]
    for j in range(n):
        base = lax.rem(core - j + n, n) * rows
        v0, v1, v2, v3 = (own[k * n + j] for k in range(4))

        def one_row(r, base=base, v0=v0, v1=v1, v2=v2, v3=v3):
            x0, x1, x2, x3 = v0[r], v1[r], v2[r], v3[r]
            pressure[base + r] = eta[base + r] * (p0 * x0 + p1 * x1 + p2 * x2)
            residual[base + r] = (x0 + r1 * x1) + (r2 * x2 + r3 * x3)

        rows_loop(0, rows, one_row, 4)


def add_pairs(a, b):
    s, e = two_sum(a[0], b[0])
    return jnp.stack([s, e + (a[1] + b[1])])


def sum_along(pair, axis, n, stride=1):
    count = n // stride
    if count < 2:
        return pair
    terms = [pair]
    for k in range(1, count):
        moves = [(i, (i + k * stride) % n) for i in range(n)]
        terms.append(lax.ppermute(pair, axis, moves))
    me = lax.axis_index(axis) // stride
    terms = [pick(terms, lax.rem(me - j + count, count)) for j in range(count)]
    while len(terms) > 1:
        rest = terms[len(terms) // 2 * 2 :]
        terms = [add_pairs(a, b) for a, b in zip(terms[::2], terms[1::2])] + rest
    return terms[0]


def per_device(nx, ny, nz, force, phase, table, flags):
    h = HALO
    wide, ys, lanes = phase.shape
    rows = wide // nz
    zs = lanes * nz
    sizes = (wide * nx, ys * ny, zs)
    slots, total = ys + 2 * h, rows + 2 * h
    cells = float(sizes[0] * sizes[1] * sizes[2])
    chain = nx * nz

    parts = call(
        functools.partial(prep_kernel, nz),
        [sds(4, rows, ys, lanes)] * nz + [sds(*phase.shape)],
        (force, phase, table),
        [VMEM, VMEM, SMEM],
        name="prep",
    )
    eta = parts[-1]
    parts = [parts[0]] + [core_shift(parts[j], nz, j) for j in range(1, nz)]
    full, ya, yb = call(
        functools.partial(gather_kernel, nz),
        [
            sds(4, rows, ys, zs),
            sds(4 * rows + rows // 4, h, zs),
            sds(4 * rows + rows // 4, h, zs),
        ],
        parts,
        name="gather",
    )
    ya, yb = exchange_y(ya, yb, ny, nz)
    edge = sds(len(edge_list(h)), 8, zs)
    xa, xb = call(force_edges_kernel, [edge, edge], (full, ya, yb), name="force_edges")
    xa, xb = exchange_x(xa, xb, chain)

    v_shape = [sds(rows, ys, lanes)] * nz
    sent = [sds(rows, ys, zs), sds(rows, h, zs), sds(rows, h, zs)]
    scalar, vector = sds(total, slots, zs), sds(3, total, slots, zs)
    field = pltpu.VMEM((3, total, slots, zs), F32)
    line = pltpu.VMEM((total, 1, zs), F32)
    heavy = 4 * 10**7
    early = call(
        functools.partial(first_inner, sizes),
        [scalar] * 3 + [vector] * (1 + SWEEPS) + [sds(rows, slots, zs)],
        (full, ya, yb, flags),
        [VMEM] * 3 + [SMEM],
        [field, pltpu.VMEM((total, slots, zs), F32), line],
        heavy,
        "first_inner",
    )
    scratch = [field, pltpu.VMEM((total + 1, slots, zs), F32), line] + [field] * SWEEPS
    result = sds(rows, slots, zs)
    near = call(
        functools.partial(first_side, nz, sizes, True),
        [scalar] * 3 + [vector, result],
        (full, ya, yb, xa, flags, *early),
        [VMEM] * 4 + [SMEM] + [VMEM] * len(early),
        scratch,
        heavy // 2,
        "first_near",
    )
    outs = call(
        functools.partial(first_side, nz, sizes, False),
        v_shape + sent + [scalar] * 3 + [vector],
        (full, ya, yb, xb, flags, *early, near[-1]),
        [VMEM] * 4 + [SMEM] + [VMEM] * (len(early) + 1),
        scratch,
        heavy // 2,
        "first",
    )
    coefs = call(
        functools.partial(join_kernel, total, rows),
        [scalar] * 3 + [vector],
        (*early[:4], *near[:4], *outs[nz + 3 :]),
        name="join",
    )
    vs, ps, moments = [list(outs[:nz])], [outs[nz]], []
    ya, yb = outs[nz + 1 : nz + 3]
    placed = []
    for step in range(1, ITERS + 1):
        last = step == ITERS
        p, v = ps[-1], vs[-1]
        placed.append([v[0]] + [core_shift(v[j], nz, j) for j in range(1, nz)])
        count = 2 if step == 1 else 2 + step
        moments.append(
            call(
                functools.partial(moments_kernel, nz, step - 1),
                [sds(count, 8, LANES)],
                (p, *ps[:-1][-1:], *[q for v in vs for q in v]),
                None,
                [pltpu.VMEM((count, ys, zs), F32)],
                name="moments",
            )[0]
        )
        ya, yb = exchange_y(ya, yb, ny, nz)
        edge = sds(h, slots, zs)
        xa, xb = call(edges_kernel, [edge, edge], (p, ya, yb, moments[-1]), name="edges")
        xa, xb = exchange_x(xa, xb, chain)
        early = call(
            functools.partial(next_inner, nz - 1),
            [scalar] + [vector] * SWEEPS + [sds(rows, slots, zs)],
            (p, ya, yb, *coefs, *placed[-1][1:]),
            None,
            (),
            heavy,
            "next_inner",
        )
        scratch = [pltpu.VMEM((total, slots, zs), F32)] + [field] * SWEEPS
        near = call(
            functools.partial(next_side, nz, True, last),
            [result],
            (p, xa, *coefs, *early[:-1]),
            None,
            scratch,
            heavy // 4,
            "next_near",
        )
        joint = v_shape[:-1] + [sds(rows + 1, ys, lanes)]
        outs = call(
            functools.partial(next_side, nz, False, last),
            joint if last else v_shape + sent,
            (p, xb, *coefs, *early[:-1], full, early[-1], *near, *(moments if last else ())),
            None,
            scratch + ([pltpu.VMEM((ys, zs), F32)] if last else []),
            heavy // 4,
            "next",
        )
        vs.append(list(outs[:nz]))
        if not last:
            ps.append(outs[nz])
            ya, yb = outs[nz + 1 : nz + 3]

    v = vs[-1]
    moved = [v[0]] + [core_shift(v[j], nz, j) for j in range(1, nz)]
    placed.append(moved)
    mine, theirs = v[-1][rows], moved[-1][rows]
    if nz > 2:
        theirs = lax.ppermute(mine, "gz", [(k, k ^ 1) for k in range(nz)])
    pair = jnp.stack(two_sum(mine, theirs))
    pair = sum_along(pair, "gz", nz, 2)
    pair = sum_along(sum_along(pair, "gx", nx), "gy", ny)
    pressure, residual, norms = call(
        functools.partial(last_kernel, nz, cells),
        [sds(*phase.shape), sds(*phase.shape), sds(ITERS)],
        (pair, eta, *[q for v in placed for q in v]),
        name="last",
        out_specs=[VMEM, VMEM, SMEM],
    )
    return pressure, residual, norms


def solution(mesh):
    placed = (P(None, "gx", "gy", "gz"), P("gx", "gy", "gz"), P(), P())
    return jax.shard_map(
        functools.partial(per_device, mesh.shape["gx"], mesh.shape["gy"], mesh.shape["gz"]),
        mesh=mesh,
        in_specs=placed,
        out_specs=(P("gx", "gy", "gz"), P("gx", "gy", "gz"), P()),
        check_vma=False,
    )
```

```python
import functools

import jax
import jax.numpy as jnp
from jax import lax
from jax.experimental import pallas as pl
from jax.experimental.pallas import tpu as pltpu
from jax.sharding import PartitionSpec as P

ITERS = 3
SWEEPS = 4
OMEGA = 0.8
HALO = 4
LANES = 128
F32 = jnp.float32

VMEM = pl.BlockSpec(memory_space=pltpu.VMEM)
SMEM = pl.BlockSpec(memory_space=pltpu.SMEM)


def sds(*shape):
    return jax.ShapeDtypeStruct(shape, F32)


def call(kernel, outs, ins, specs=None, scratch=(), flops=10**6, name=None, out_specs=None):
    return pl.pallas_call(
        kernel,
        out_shape=outs,
        in_specs=specs or [VMEM] * len(ins),
        out_specs=out_specs or jax.tree.map(lambda _: VMEM, outs),
        scratch_shapes=list(scratch),
        compiler_params=pltpu.CompilerParams(vmem_limit_bytes=24 * 2**20),
        cost_estimate=pl.CostEstimate(flops=flops, bytes_accessed=2**20, transcendentals=0),
        name=name,
    )(*ins)


def pick(items, index):
    value = items[0]
    for k in range(1, len(items)):
        value = jnp.where(index == k, items[k], value)
    return value


def split_z(value, core, n):
    blocks = [value[..., t * LANES : (t + 1) * LANES] for t in range(n)]
    return [pick(blocks, lax.rem(core + j, n)) for j in range(n)]


def join_own(parts, core):
    n = len(parts)
    return jnp.concatenate([pick(parts, lax.rem(t - core + n, n)) for t in range(n)], -1)


def join_received(parts, core):
    n = len(parts)
    return jnp.concatenate([pick(parts, lax.rem(core - t + n, n)) for t in range(n)], -1)


def up_y(row):
    return pltpu.roll(row, row.shape[0] - 1, 0)


def down_y(row):
    return pltpu.roll(row, 1, 0)


def up_z(row):
    return pltpu.roll(row, row.shape[1] - 1, 1)


def down_z(row):
    return pltpu.roll(row, 1, 1)


def rows_loop(start, stop, body, step=3):
    count = stop - start
    whole = count // step

    def chunk(i, carry):
        for k in range(step):
            body(start + i * step + k)
        return carry

    if whole > 1:
        lax.fori_loop(0, whole, chunk, 0)
        rest = start + whole * step
    else:
        rest = start
    for r in range(rest, stop):
        body(r)


def exchange_y(a, b, ny, nz):
    even = [(i, i ^ 1) for i in range(ny)]
    odd = []
    for y in range(ny):
        for z in range(nz):
            other = (y + (1 if y % 2 else -1), z) if 0 < y < ny - 1 else (y, z ^ 1)
            odd.append((y * nz + z, other[0] * nz + other[1]))
    return lax.ppermute(a, "gy", even), lax.ppermute(b, ("gy", "gz"), odd)


def exchange_x(a, b, n):
    even = [(i, i ^ 1) for i in range(n)]
    odd = [(i, (i + (1 if i % 2 else -1)) % n) for i in range(n)]
    return lax.ppermute(a, ("gx", "gz"), even), lax.ppermute(b, ("gx", "gz"), odd)


def core_shift(value, n, j):
    return lax.ppermute(value, "gz", [(i, (i + j) % n) for i in range(n)])


def lookup(ids, table):
    eta = jnp.zeros(ids.shape, F32)
    for level in range(table.shape[0]):
        eta = jnp.where(ids == level, table[level], eta)
    return eta


def gather_kernel(n, *refs):
    forces, etas = refs[:n], refs[n : 2 * n]
    full, send_a, send_b = refs[2 * n :]
    core = lax.axis_index("gz")
    odd = Place().odd_y
    fields, rows, ys, _ = full.shape
    h = HALO

    for c in range(fields):

        def one(r, c=c):
            parts = [q[c, r] for q in forces] if c < 3 else [q[r] for q in etas]
            row = join_received(parts, core)
            full[c, r] = row
            send_a[c * rows + r] = jnp.where(odd, row[:h], row[ys - h :])
            send_b[c * rows + r] = jnp.where(odd, row[ys - h :], row[:h])

        rows_loop(0, rows, one, 4)
    for r in range(rows):
        line = full[3, r, ys - h - 1 : ys - h, :]
        send_a[fields * rows + r // 4, r % 4 : r % 4 + 1, :] = line
        send_b[fields * rows + r // 4, r % 4 : r % 4 + 1, :] = line


def edge_list(h):
    tiles = []
    for c in range(4):
        for k in range(h):
            if c in (1, 2) and k == 0:
                continue
            for q in range(2 if c == 0 and k == 0 else 3):
                tiles.append((c, k, q))
    return tiles + [(3, -1, 0), (3, -1, 1)]


def force_edges_kernel(full, ya, yb, send_a, send_b):
    place = Place()
    odd_x = place.odd
    _, rows, ys, _ = full.shape
    h = HALO
    for send, first in ((send_a, odd_x), (send_b, jnp.logical_not(odd_x))):
        for t, (c, k, q) in enumerate(edge_list(h)):
            r = jnp.where(first, h - 1 - k, rows - h + k)
            if q < 2:
                send[t] = full[c, r, 8 * q : 8 * q + 8, :]
            else:
                a, b = ya[c * rows + r], yb[c * rows + r]
                send[t, :h, :] = place.up(a, b)
                send[t, h:, :] = place.low(a, b)


def edges_kernel(p, ya, yb, *rest):
    send_a, send_b = rest[-2:]
    place = Place()
    rows = p.shape[0]
    h = HALO
    for send, first in ((send_a, place.odd), (send_b, jnp.logical_not(place.odd))):
        start = jnp.where(first, 0, rows - h)
        for k in range(h):
            set_row(send, (k,), p[start + k], ya[start + k], yb[start + k], place)


class Rows:
    def __init__(self, early, late, first, end):
        self.early, self.late, self.first, self.end = early, late, first, end

    def __getitem__(self, index):
        r = index[-1] if isinstance(index, tuple) else index
        mine = not isinstance(r, int) or not self.first <= r < self.end
        return (self.late if mine else self.early)[index]


def spans(lo, hi, total):
    full = [(s, total - 1 - s) for s in range(SWEEPS)] + [(HALO, total - HALO)]
    inner = [(lo + s, hi - s) for s in range(SWEEPS)] + [(lo + SWEEPS, hi - SWEEPS + 1)]
    inner = [i if i[0] < i[1] else (f[0], f[0]) for f, i in zip(full, inner)]
    return full, inner


def outside(full, inner, side):
    return range(full[0], inner[0]) if side == "low" else range(inner[1], full[1])


def on_side(near, body):
    odd = Place().odd
    pl.when(odd)(lambda: body("low" if near else "high"))
    pl.when(jnp.logical_not(odd))(lambda: body("high" if near else "low"))


def update(source, b, w, kx, ky, kz, target, r):
    keep = 1.0 - OMEGA
    here_x, past_x, here_y, here_z = kx[r], kx[r - 1], ky[r], kz[r]
    for c in range(3):
        u = source[c, r]
        near = here_x * source[c, r + 1] + past_x * source[c, r - 1]
        near = near + here_y * up_y(u) + down_y(here_y * u)
        near = near + here_z * up_z(u) + down_z(here_z * u)
        target[c, r] = keep * u + (b[c, r] + w[c, r] * near)


def diverge(v, r):
    vy, vz = v[1, r], v[2, r]
    lane = lax.broadcasted_iota(jnp.int32, vz.shape, 1)
    out = v[0, r - 1] - v[0, r]
    out = out + (down_y(vy) - vy)
    return out + (jnp.where(lane == 0, 0.0, down_z(vz)) - vz)


def emit_early(emit, near_side, full, inner, out_inner, out_near):
    for r in outside(full[SWEEPS], inner[SWEEPS], near_side):
        emit(r - HALO, out_near[r - HALO])
    rows_loop(inner[SWEEPS][0] - HALO, inner[SWEEPS][1] - HALO, lambda r: emit(r, out_inner[r]), 4)


def inner_solve(b, levels, out, inner, w, kx, ky, kz, step):
    source = b
    for s in range(1, SWEEPS):
        target = levels[s - 1]

        def one(r, source=source, target=target):
            update(source, b, w, kx, ky, kz, target, r)

        rows_loop(*inner[s], one, step)
        source = target

    def last(r):
        out[r - HALO] = diverge(source, r)

    rows_loop(*inner[SWEEPS], last, 2)


def outer_solve(side, b, levels, buffers, inner, full, w, kx, ky, kz, emit):
    source = b
    for s in range(1, SWEEPS):
        target = buffers[s - 1]
        for r in outside(full[s], inner[s], side):
            update(source, b, w, kx, ky, kz, target, r)
        source = Rows(levels[s - 1], target, *inner[s])
    for r in outside(full[SWEEPS], inner[SWEEPS], side):
        emit(r - HALO, diverge(source, r))


def emit_result(v_own, v_others, p_out, send_a, send_b, eta_at, sums=None):
    n = 1 + len(v_others)
    core = lax.axis_index("gz")
    odd = Place().odd_y
    h = HALO

    def emit(r, out):
        ys = v_own.shape[1]
        out = out[:ys]
        parts = split_z(out, core, n)
        v_own[r] = parts[0]
        for ref, part in zip(v_others, parts[1:]):
            ref[r] = part
        if p_out is not None:
            p = eta_at(r) * out
            p_out[r] = p
            send_a[r] = jnp.where(odd, p[:h], p[ys - h :])
            send_b[r] = jnp.where(odd, p[ys - h :], p[:h])
        if sums is not None:
            sums(r, out)

    return emit


def fold(value):
    total = value[:8]
    for k in range(1, value.shape[0] // 8):
        total = total + value[8 * k : 8 * k + 8]
    lanes = total[:, :LANES]
    for t in range(1, total.shape[1] // LANES):
        lanes = lanes + total[:, t * LANES : (t + 1) * LANES]
    return lanes


class Place:
    def __init__(self):
        chain = lax.axis_size("gx") * lax.axis_size("gz")
        self.x = lax.axis_index("gx") * lax.axis_size("gz") + lax.axis_index("gz")
        self.odd = lax.rem(self.x, 2) == 1
        self.below_x, self.above_x = self.x > 0, self.x < chain - 1
        y = lax.axis_index("gy")
        self.odd_y = lax.rem(y, 2) == 1
        self.below_y, self.above_y = y > 0, y < lax.axis_size("gy") - 1

    def up(self, a, b):
        return jnp.where(self.above_y, jnp.where(self.odd_y, b, a), 0.0)

    def low(self, a, b):
        return jnp.where(self.below_y, jnp.where(self.odd_y, a, b), 0.0)


def set_row(ref, index, row, a, b, place):
    ys, h = row.shape[0], a.shape[0]
    ref[(*index, slice(0, ys), slice(None))] = row
    ref[(*index, slice(ys, ys + h), slice(None))] = place.up(a, b)
    ref[(*index, slice(ys + h, ys + 2 * h), slice(None))] = place.low(a, b)


def coefs_at(sizes, place, slots, lanes, rows, ys, flags):
    h = HALO
    slot = lax.broadcasted_iota(jnp.int32, (slots, lanes), 0)
    at_y = lax.axis_index("gy") * ys + slot - jnp.where(slot >= ys + h, slots, 0)
    at_z = lax.broadcasted_iota(jnp.int32, (slots, lanes), 1)
    in_y = (at_y >= 0) & (at_y < sizes[1])
    y_up, y_low = at_y + 1 < sizes[1], at_y >= 1
    z_up, z_low = at_z + 1 < sizes[2], at_z >= 1
    wall = [jnp.where(flags[k] == 0, 1.0, 0.0).astype(F32) for k in range(6)]

    def coefs(r, mid, before, after, line, force_at, kx, ky, kz, w, b):
        at_x = place * rows - h + r
        x_up = jnp.full(mid.shape, at_x + 1, jnp.int32) < sizes[0]
        x_low = jnp.full(mid.shape, at_x, jnp.int32) >= 1
        inside = in_y & jnp.broadcast_to((at_x >= 0) & (at_x < sizes[0]), mid.shape)
        y_before = jnp.where(slot == ys + h, line, down_y(mid))
        sides = (
            (x_up, after, x_low, before),
            (y_up, up_y(mid), y_low, y_before),
            (z_up, up_z(mid), z_low, down_z(mid)),
        )
        diag = [jnp.zeros_like(mid) for _ in range(3)]
        for axis, (up_in, up, low_in, low) in enumerate(sides):
            up, low = 0.5 * (mid + up), 0.5 * (mid + low)
            (kx, ky, kz)[axis][r] = jnp.where(up_in, up, 0.0)
            for c in range(3):
                low_wall = 1.0 if c == axis else wall[2 * axis]
                up_wall = 1.0 if c == axis else wall[2 * axis + 1]
                diag[c] = diag[c] + jnp.where(up_in, up, up_wall * mid)
                diag[c] = diag[c] + jnp.where(low_in, low, low_wall * mid)
        for c in range(3):
            weight = jnp.where(inside, OMEGA / diag[c], 0.0)
            w[c, r] = weight
            b[c, r] = weight * force_at(c)

    return coefs


def first_inner(sizes, full, ya, yb, flags, kx, ky, kz, w, b, *rest):
    levels, (out, force, eta, line) = rest[: SWEEPS - 1], rest[SWEEPS - 1 :]
    fields, rows, ys, lanes = full.shape
    h = HALO
    place = Place()
    slots, total = ys + 2 * h, rows + 2 * h
    for c in range(fields):

        def one(r, c=c):
            to, index = (force, (c, r + h)) if c < 3 else (eta, (r + h,))
            set_row(to, index, full[c, r], ya[c * rows + r], yb[c * rows + r], place)

        rows_loop(0, rows, one, 4)
    for q in range(rows // 4):
        block = place.low(ya[fields * rows + q], yb[fields * rows + q])
        for k in range(4):
            line[h + 4 * q + k] = block[k : k + 1]
    coefs = coefs_at(sizes, place.x, slots, lanes, rows, ys, flags)

    def at(r):
        coefs(r, eta[r], eta[r - 1], eta[r + 1], line[r], lambda c: force[c, r], kx, ky, kz, w, b)

    _, inner = spans(h + 1, h + rows - 1, total)
    rows_loop(*inner[0], at, 1)
    inner_solve(b, levels, out, inner, w, kx, ky, kz, 3)


def first_side(n, sizes, near, *refs):
    count = 10 + SWEEPS
    full, ya, yb, xs, flags, *early = refs[:count]
    kx0, ky0, kz0, w0, b0, *levels, out0 = early
    if near:
        kx, ky, kz, w, out, *scratch = refs[count:]
    else:
        out_near, refs = refs[count], refs[count + 1 :]
        v_own, v_others, refs = refs[0], refs[1:n], refs[n:]
        p_out, send_a, send_b, kx, ky, kz, w, *scratch = refs
    force, eta, line, b, *buffers = scratch
    fields, rows, ys, lanes = full.shape
    h = HALO
    place = Place()
    slots, total = ys + 2 * h, rows + 2 * h
    ranges, inner = spans(h + 1, h + rows - 1, total)
    coefs = coefs_at(sizes, place.x, slots, lanes, rows, ys, flags)

    def body(side):
        todo = outside((0, total), inner[0], side)
        for r in sorted({min(max(q + d, h), h + rows - 1) for q in todo for d in (-1, 0, 1)}):
            k = r - h
            for c in range(fields):
                to, index = (force, (c, r)) if c < 3 else (eta, (r + 1,))
                set_row(to, index, full[c, k], ya[c * rows + k], yb[c * rows + k], place)
            block = fields * rows + k // 4
            line[r] = place.low(ya[block], yb[block])[k % 4 : k % 4 + 1]
        low = side == "low"
        blank = jnp.zeros((slots, lanes), F32)
        for k in range(h):
            line[k if low else h + rows + k] = jnp.zeros((1, lanes), F32)
        for c in range(3):
            force[c, 0 if low else total - 1] = blank
        if low:
            eta[0] = blank
        for t, (c, k, q) in enumerate(edge_list(h)):
            where = slice(8 * q, 8 * q + 8)
            if c < 3:
                force[c, k if low else total - 1 - k, where, :] = xs[t]
            elif low or k >= 0:
                eta[1 + k if low else total - k, where, :] = xs[t]
        for r in todo:
            after = eta[min(r + 2, total)]
            coefs(r, eta[r + 1], eta[r], after, line[r], lambda c: force[c, r], kx, ky, kz, w, b)
        early_late = [(kx0, kx), (ky0, ky), (kz0, kz), (w0, w), (b0, b)]
        kxs, kys, kzs, ws, bs = (Rows(e, f, *inner[0]) for e, f in early_late)
        if near:

            def emit(r, value):
                out[r] = value

            outer_solve(side, bs, levels, buffers, inner, ranges, ws, kxs, kys, kzs, emit)
        else:
            emit = emit_result(v_own, v_others, p_out, send_a, send_b, lambda r: full[3, r])
            outer_solve(side, bs, levels, buffers, inner, ranges, ws, kxs, kys, kzs, emit)
            emit_early(emit, "high" if low else "low", ranges, inner, out0, out_near)

    on_side(near, body)


def join_kernel(total, rows, *refs):
    inner_refs, near_refs, far_refs, outs = (refs[4 * k : 4 * k + 4] for k in range(4))
    _, inner = spans(HALO + 1, HALO + rows - 1, total)

    def carry(source, r):
        for k in range(3):
            outs[k][r] = source[k][r]
        for c in range(3):
            outs[3][c, r] = source[3][c, r]

    rows_loop(*inner[0], lambda r: carry(inner_refs, r), 2)
    for near, source in ((True, near_refs), (False, far_refs)):

        def body(side, source=source):
            for r in outside((0, total), inner[0], side):
                carry(source, r)

        on_side(near, body)


def next_inner(extra, p_in, ya, yb, kx, ky, kz, w, *rest):
    p, b, *rest = rest[extra:]
    levels, out = rest[: SWEEPS - 1], rest[SWEEPS - 1]
    rows = p_in.shape[0]
    h = HALO
    place = Place()

    def fill(r):
        set_row(p, (r + h,), p_in[r], ya[r], yb[r], place)

    rows_loop(0, rows, fill, 4)
    _, inner = spans(h, h + rows - 1, rows + 2 * h)
    rows_loop(*inner[0], lambda r: grads(p, w, b, r), 16)
    inner_solve(b, levels, out, inner, w, kx, ky, kz, 16)


def grads(p, w, b, r):
    mid = p[r]
    lanes = mid.shape[1]
    lane = lax.broadcasted_iota(jnp.int32, mid.shape, 1)
    b[0, r] = w[0, r] * (p[r + 1] - mid)
    b[1, r] = w[1, r] * (up_y(mid) - mid)
    b[2, r] = w[2, r] * (jnp.where(lane == lanes - 1, 0.0, up_z(mid)) - mid)


def next_side(n, near, last, p_in, xs, kx, ky, kz, w, p0, b0, *refs):
    levels, refs = refs[: SWEEPS - 1], refs[SWEEPS - 1 :]
    if near:
        out, *scratch = refs
    else:
        full, out0, out_near, refs = refs[0], refs[1], refs[2], refs[3:]
        sums = p_out = send_a = send_b = None
        if last:
            partials, refs = refs[:ITERS], refs[ITERS:]
        v_own, v_others, refs = refs[0], refs[1:n], refs[n:]
        if last:
            moment, acc, refs = v_others[-1].at[p_in.shape[0]], refs[-1], refs[:-1]
            acc[...] = jnp.zeros_like(acc)

            def sums(r, v):
                acc[...] = acc[...] + v * p_in[r]
        else:
            p_out, send_a, send_b, *refs = refs
        scratch = refs
    p, b, *buffers = scratch
    rows = p_in.shape[0]
    h = HALO
    place = Place()
    ranges, inner = spans(h, h + rows - 1, rows + 2 * h)

    def body(side):
        low = side == "low"
        for k in range(h):
            row = xs[k]
            if not near:
                row = jnp.where(place.below_x if low else place.above_x, row, 0.0)
            p[k if low else h + rows + k] = row
        ps = Rows(p0, p, h, h + rows)
        for r in outside(ranges[0], inner[0], side):
            grads(ps, w, b, r)
        bs = Rows(b0, b, *inner[0])
        if near:

            def emit(r, value):
                out[r] = value

            outer_solve(side, bs, levels, buffers, inner, ranges, w, kx, ky, kz, emit)
        else:
            emit = emit_result(v_own, v_others, p_out, send_a, send_b, lambda r: full[3, r], sums)
            outer_solve(side, bs, levels, buffers, inner, ranges, w, kx, ky, kz, emit)
            emit_early(emit, "high" if low else "low", ranges, inner, out0, out_near)

    on_side(near, body)
    if not near and last:
        moment[...] = jnp.zeros_like(moment)
        at = 0
        for ref in partials:
            for k in range(ref.shape[0]):
                moment[at : at + 1, :] = jnp.sum(ref[k], 0, keepdims=True)
                at += 1
        moment[at : at + 1, :] = jnp.sum(fold(acc[...]), 0, keepdims=True)


def moments_kernel(n, step, *refs):
    moment, acc = refs[-2:]
    p, refs = refs[0], refs[1:-2]
    before, refs = (refs[0], refs[1:]) if step else (None, refs)
    groups = [refs[k * n : (k + 1) * n] for k in range(step + 1)]
    core = lax.axis_index("gz")
    acc[...] = jnp.zeros_like(acc)

    def one(r):
        v = join_own([q[r] for q in groups[-1]], core)
        others = ([before[r]] if step else []) + [p[r], v]
        others += [join_own([q[r] for q in group], core) for group in groups[:-1]]
        for k, other in enumerate(others):
            acc[k] = acc[k] + v * other

    rows_loop(0, p.shape[0], one, 4)
    for k in range(acc.shape[0]):
        moment[k] = fold(acc[k])


def two_sum(a, b):
    s = a + b
    t = s - a
    return s, (a - (s - t)) + (b - t)


def quick(a, b):
    s = a + b
    return s, b - (s - a)


def halves(a):
    t = 4097.0 * a
    high = t - (t - a)
    return high, a - high


def two_prod(a, b):
    p = a * b
    ah, al = halves(a)
    bh, bl = halves(b)
    return p, ((ah * bh - p) + ah * bl + al * bh) + al * bl


def add(a, b):
    s, e = two_sum(a[0], b[0])
    return quick(s, e + (a[1] + b[1]))


def mul(a, b):
    p, e = two_prod(a[0], b[0])
    return quick(p, e + (a[0] * b[1] + a[1] * b[0]))


def neg(a):
    return -a[0], -a[1]


def div(a, b):
    q = a[0] / b[0]
    r = add(a, neg(mul((q, jnp.zeros_like(q)), b)))
    q2 = r[0] / b[0]
    return quick(q, q2)


def twice(a):
    return 2.0 * a[0], 2.0 * a[1]


def last_kernel(n, cells, sums, eta, *refs):
    own = refs[: 4 * n]
    pressure, residual, norms = refs[4 * n :]
    core = lax.axis_index("gz")
    pair = (sums[0], sums[1])
    for shift in (64, 32, 16, 8, 4, 2, 1):
        pair = add(pair, tuple(pltpu.roll(x, shift, 1) for x in pair))
    item = [(pair[0][k : k + 1], pair[1][k : k + 1]) for k in range(12)]
    m0, n00, m1, m2, n11, n01, m3, m4, n22, n02, n12, m5 = item
    one = (jnp.ones_like(m0[0]), jnp.zeros_like(m0[0]))
    a0 = div(m0, m1)
    c11 = neg(a0)
    g1 = mul(c11, add(m1, mul(c11, m2)))
    b0 = div(g1, m0)
    d10, d11 = add(one, b0), c11
    a1 = div(g1, mul(d11, add(mul(d10, m2), mul(d11, m3))))
    c21 = add(c11, neg(mul(a1, d10)))
    c22 = neg(mul(a1, d11))
    g2 = mul(c22, add(m2, add(mul(c21, m3), mul(c22, m4))))
    b1 = div(g2, g1)
    d20 = add(one, mul(b1, d10))
    d21 = add(c21, mul(b1, d11))
    d22 = c22
    a2 = div(g2, mul(d22, add(mul(d20, m3), add(mul(d21, m4), mul(d22, m5)))))
    p0 = add(a0, add(mul(a1, d10), mul(a2, d20)))[0]
    p1 = add(mul(a1, d11), mul(a2, d21))[0]
    p2 = mul(a2, d22)[0]
    r1 = add(c21, neg(mul(a2, d20)))[0]
    r2 = add(c22, neg(mul(a2, d21)))[0]
    r3 = -p2
    norm1 = add(n00, mul(c11, add(twice(n01), mul(c11, n11))))
    norm2 = add(n00, mul(c21, add(twice(n01), mul(c21, n11))))
    norm2 = add(norm2, mul(c22, add(twice(n02), add(mul(twice(c21), n12), mul(c22, n22)))))
    for k, value in enumerate((n00, norm1, norm2)):
        norms[k] = (value[0] / cells)[0, 0]
    rows = own[0].shape[0]
    for j in range(n):
        base = lax.rem(core - j + n, n) * rows
        v0, v1, v2, v3 = (own[k * n + j] for k in range(4))

        def one_row(r, base=base, v0=v0, v1=v1, v2=v2, v3=v3):
            x0, x1, x2, x3 = v0[r], v1[r], v2[r], v3[r]
            pressure[base + r] = eta[base + r] * (p0 * x0 + p1 * x1 + p2 * x2)
            residual[base + r] = (x0 + r1 * x1) + (r2 * x2 + r3 * x3)

        rows_loop(0, rows, one_row, 4)


def add_pairs(a, b):
    s, e = two_sum(a[0], b[0])
    return jnp.stack([s, e + (a[1] + b[1])])


def sum_along(pair, axis, n, stride=1):
    count = n // stride
    if count < 2:
        return pair
    terms = [pair]
    for k in range(1, count):
        moves = [(i, (i + k * stride) % n) for i in range(n)]
        terms.append(lax.ppermute(pair, axis, moves))
    me = lax.axis_index(axis) // stride
    terms = [pick(terms, lax.rem(me - j + count, count)) for j in range(count)]
    while len(terms) > 1:
        rest = terms[len(terms) // 2 * 2 :]
        terms = [add_pairs(a, b) for a, b in zip(terms[::2], terms[1::2])] + rest
    return terms[0]


def per_device(nx, ny, nz, force, phase, table, flags):
    h = HALO
    wide, ys, lanes = phase.shape
    rows = wide // nz
    zs = lanes * nz
    sizes = (wide * nx, ys * ny, zs)
    slots, total = ys + 2 * h, rows + 2 * h
    cells = float(sizes[0] * sizes[1] * sizes[2])
    chain = nx * nz

    core = lax.axis_index("gz")
    eta = lookup(phase, table)
    forces, etas = [], []
    for j in range(nz):
        start = lax.rem(core + j, nz) * rows
        forces.append(lax.dynamic_slice_in_dim(force, start, rows, 1))
        etas.append(lax.dynamic_slice_in_dim(eta, start, rows, 0))
    forces = forces[:1] + [core_shift(forces[j], nz, j) for j in range(1, nz)]
    etas = etas[:1] + [core_shift(etas[j], nz, j) for j in range(1, nz)]
    full, ya, yb = call(
        functools.partial(gather_kernel, nz),
        [
            sds(4, rows, ys, zs),
            sds(4 * rows + rows // 4, h, zs),
            sds(4 * rows + rows // 4, h, zs),
        ],
        (*forces, *etas),
        name="gather",
    )
    ya, yb = exchange_y(ya, yb, ny, nz)
    edge = sds(len(edge_list(h)), 8, zs)
    xa, xb = call(force_edges_kernel, [edge, edge], (full, ya, yb), name="force_edges")
    xa, xb = exchange_x(xa, xb, chain)

    v_shape = [sds(rows, ys, lanes)] * nz
    sent = [sds(rows, ys, zs), sds(rows, h, zs), sds(rows, h, zs)]
    scalar, vector = sds(total, slots, zs), sds(3, total, slots, zs)
    field = pltpu.VMEM((3, total, slots, zs), F32)
    line = pltpu.VMEM((total, 1, zs), F32)
    heavy = 4 * 10**7
    early = call(
        functools.partial(first_inner, sizes),
        [scalar] * 3 + [vector] * (1 + SWEEPS) + [sds(rows, slots, zs)],
        (full, ya, yb, flags),
        [VMEM] * 3 + [SMEM],
        [field, pltpu.VMEM((total, slots, zs), F32), line],
        heavy,
        "first_inner",
    )
    scratch = [field, pltpu.VMEM((total + 1, slots, zs), F32), line] + [field] * SWEEPS
    result = sds(rows, slots, zs)
    near = call(
        functools.partial(first_side, nz, sizes, True),
        [scalar] * 3 + [vector, result],
        (full, ya, yb, xa, flags, *early),
        [VMEM] * 4 + [SMEM] + [VMEM] * len(early),
        scratch,
        heavy // 2,
        "first_near",
    )
    outs = call(
        functools.partial(first_side, nz, sizes, False),
        v_shape + sent + [scalar] * 3 + [vector],
        (full, ya, yb, xb, flags, *early, near[-1]),
        [VMEM] * 4 + [SMEM] + [VMEM] * (len(early) + 1),
        scratch,
        heavy // 2,
        "first",
    )
    coefs = call(
        functools.partial(join_kernel, total, rows),
        [scalar] * 3 + [vector],
        (*early[:4], *near[:4], *outs[nz + 3 :]),
        name="join",
    )
    vs, ps, moments = [list(outs[:nz])], [outs[nz]], []
    ya, yb = outs[nz + 1 : nz + 3]
    placed = []
    for step in range(1, ITERS + 1):
        last = step == ITERS
        p, v = ps[-1], vs[-1]
        placed.append([v[0]] + [core_shift(v[j], nz, j) for j in range(1, nz)])
        count = 2 if step == 1 else 2 + step
        moments.append(
            call(
                functools.partial(moments_kernel, nz, step - 1),
                [sds(count, 8, LANES)],
                (p, *ps[:-1][-1:], *[q for v in vs for q in v]),
                None,
                [pltpu.VMEM((count, ys, zs), F32)],
                name="moments",
            )[0]
        )
        ya, yb = exchange_y(ya, yb, ny, nz)
        edge = sds(h, slots, zs)
        xa, xb = call(edges_kernel, [edge, edge], (p, ya, yb, moments[-1]), name="edges")
        xa, xb = exchange_x(xa, xb, chain)
        early = call(
            functools.partial(next_inner, nz - 1),
            [scalar] + [vector] * SWEEPS + [sds(rows, slots, zs)],
            (p, ya, yb, *coefs, *placed[-1][1:]),
            None,
            (),
            heavy,
            "next_inner",
        )
        scratch = [pltpu.VMEM((total, slots, zs), F32)] + [field] * SWEEPS
        near = call(
            functools.partial(next_side, nz, True, last),
            [result],
            (p, xa, *coefs, *early[:-1]),
            None,
            scratch,
            heavy // 4,
            "next_near",
        )
        joint = v_shape[:-1] + [sds(rows + 1, ys, lanes)]
        outs = call(
            functools.partial(next_side, nz, False, last),
            joint if last else v_shape + sent,
            (p, xb, *coefs, *early[:-1], full, early[-1], *near, *(moments if last else ())),
            None,
            scratch + ([pltpu.VMEM((ys, zs), F32)] if last else []),
            heavy // 4,
            "next",
        )
        vs.append(list(outs[:nz]))
        if not last:
            ps.append(outs[nz])
            ya, yb = outs[nz + 1 : nz + 3]

    v = vs[-1]
    moved = [v[0]] + [core_shift(v[j], nz, j) for j in range(1, nz)]
    placed.append(moved)
    mine, theirs = v[-1][rows], moved[-1][rows]
    if nz > 2:
        theirs = lax.ppermute(mine, "gz", [(k, k ^ 1) for k in range(nz)])
    pair = jnp.stack(two_sum(mine, theirs))
    pair = sum_along(pair, "gz", nz, 2)
    pair = sum_along(sum_along(pair, "gx", nx), "gy", ny)
    pressure, residual, norms = call(
        functools.partial(last_kernel, nz, cells),
        [sds(*phase.shape), sds(*phase.shape), sds(ITERS)],
        (pair, eta, *[q for v in placed for q in v]),
        name="last",
        out_specs=[VMEM, VMEM, SMEM],
    )
    return pressure, residual, norms


def solution(mesh):
    placed = (P(None, "gx", "gy", "gz"), P("gx", "gy", "gz"), P(), P())
    return jax.shard_map(
        functools.partial(per_device, mesh.shape["gx"], mesh.shape["gy"], mesh.shape["gz"]),
        mesh=mesh,
        in_specs=placed,
        out_specs=(P("gx", "gy", "gz"), P("gx", "gy", "gz"), P()),
        check_vma=False,
    )
```

```python
import functools

import jax
import jax.numpy as jnp
from jax import lax
from jax.experimental import pallas as pl
from jax.experimental.pallas import tpu as pltpu
from jax.sharding import PartitionSpec as P

ITERS = 3
SWEEPS = 4
OMEGA = 0.8
HALO = 4
LANES = 128
F32 = jnp.float32

VMEM = pl.BlockSpec(memory_space=pltpu.VMEM)
SMEM = pl.BlockSpec(memory_space=pltpu.SMEM)


def sds(*shape):
    return jax.ShapeDtypeStruct(shape, F32)


def call(kernel, outs, ins, specs=None, scratch=(), flops=10**6, name=None, out_specs=None):
    return pl.pallas_call(
        kernel,
        out_shape=outs,
        in_specs=specs or [VMEM] * len(ins),
        out_specs=out_specs or jax.tree.map(lambda _: VMEM, outs),
        scratch_shapes=list(scratch),
        compiler_params=pltpu.CompilerParams(vmem_limit_bytes=24 * 2**20),
        cost_estimate=pl.CostEstimate(flops=flops, bytes_accessed=2**20, transcendentals=0),
        name=name,
    )(*ins)


def pick(items, index):
    value = items[0]
    for k in range(1, len(items)):
        value = jnp.where(index == k, items[k], value)
    return value


def split_z(value, core, n):
    blocks = [value[..., t * LANES : (t + 1) * LANES] for t in range(n)]
    return [pick(blocks, lax.rem(core + j, n)) for j in range(n)]


def join_own(parts, core):
    n = len(parts)
    return jnp.concatenate([pick(parts, lax.rem(t - core + n, n)) for t in range(n)], -1)


def join_received(parts, core):
    n = len(parts)
    return jnp.concatenate([pick(parts, lax.rem(core - t + n, n)) for t in range(n)], -1)


def up_y(row):
    return pltpu.roll(row, row.shape[0] - 1, 0)


def down_y(row):
    return pltpu.roll(row, 1, 0)


def up_z(row):
    return pltpu.roll(row, row.shape[1] - 1, 1)


def down_z(row):
    return pltpu.roll(row, 1, 1)


def rows_loop(start, stop, body, step=3):
    count = stop - start
    whole = count // step

    def chunk(i, carry):
        for k in range(step):
            body(start + i * step + k)
        return carry

    if whole > 1:
        lax.fori_loop(0, whole, chunk, 0)
        rest = start + whole * step
    else:
        rest = start
    for r in range(rest, stop):
        body(r)


def exchange_y(a, b, ny, nz):
    even = [(i, i ^ 1) for i in range(ny)]
    odd = []
    for y in range(ny):
        for z in range(nz):
            other = (y + (1 if y % 2 else -1), z) if 0 < y < ny - 1 else (y, z ^ 1)
            odd.append((y * nz + z, other[0] * nz + other[1]))
    return lax.ppermute(a, "gy", even), lax.ppermute(b, ("gy", "gz"), odd)


def exchange_x(a, b, n):
    even = [(i, i ^ 1) for i in range(n)]
    odd = [(i, (i + (1 if i % 2 else -1)) % n) for i in range(n)]
    return lax.ppermute(a, ("gx", "gz"), even), lax.ppermute(b, ("gx", "gz"), odd)


def core_shift(value, n, j):
    return lax.ppermute(value, "gz", [(i, (i + j) % n) for i in range(n)])


def lookup(ids, table):
    eta = jnp.zeros(ids.shape, F32)
    for level in range(table.shape[0]):
        eta = jnp.where(ids == level, table[level], eta)
    return eta


def eta_kernel(n, table, after, *refs):
    slices, eta = refs[:n], refs[n]
    rows = slices[0].shape[0]
    for j in range(n):
        base = lax.rem(lax.axis_index("gz") + j, n) * rows

        def one(r, j=j, base=base):
            eta[base + r] = lookup(slices[j][r], table)

        rows_loop(0, rows, one, 4)


def gather_kernel(n, table, *refs):
    forces, phases = refs[:n], refs[n : 2 * n]
    full, send_a, send_b = refs[2 * n :]
    core = lax.axis_index("gz")
    odd = Place().odd_y
    fields, rows, ys, _ = full.shape
    h = HALO

    for c in range(fields):

        def one(r, c=c):
            row = join_received([q[c, r] for q in forces] if c < 3 else [q[r] for q in phases], core)
            row = row if c < 3 else lookup(row, table)
            full[c, r] = row
            send_a[c * rows + r] = jnp.where(odd, row[:h], row[ys - h :])
            send_b[c * rows + r] = jnp.where(odd, row[ys - h :], row[:h])

        rows_loop(0, rows, one, 4)
    for r in range(rows):
        line = full[3, r, ys - h - 1 : ys - h, :]
        send_a[fields * rows + r // 4, r % 4 : r % 4 + 1, :] = line
        send_b[fields * rows + r // 4, r % 4 : r % 4 + 1, :] = line


def edge_list():
    tiles = []
    for c in range(4):
        far = 1 if c in (1, 2) else 0
        tiles += [(c, k, q) for k in range(far, HALO) for q in range(2)]
        tiles += [(c, 3, 2), ("pack", c, 2, 1)] if c < 3 else [(c, 3, 2), (c, 2, 2), ("pack", c, 1, 0)]
    return tiles + [(3, -1, 0), (3, -1, 1)]


def face_list():
    return [(0, k, q) for k in range(HALO) for q in range(2)] + [(0, 3, 2), ("pack", 0, 2, 1)]


def put_tile(send, t, tile, row, halo):
    h = HALO
    if tile[0] == "pack":
        _, c, j, k = tile
        (up, low), (up_k, low_k) = halo(c, j), halo(c, k)
        send[t, 0:2, :] = up[0:2]
        send[t, 2:3, :] = low_k[h - 1 :]
        send[t, 3:4, :] = up_k[0:1]
        send[t, 4:6, :] = low[0:2]
        send[t, 6:8, :] = low[h - 2 :]
    elif tile[2] < 2:
        send[t] = row(tile[0], tile[1])[8 * tile[2] : 8 * tile[2] + 8]
    else:
        up, low = halo(tile[0], tile[1])
        send[t, :h, :] = up
        send[t, h:, :] = low


def take_tile(tile, value, ys, target):
    if tile[0] == "pack":
        _, c, j, k = tile
        ref, index = target(c, j)
        ref[(*index, slice(ys, ys + 8), slice(None))] = value
        ref, index = target(c, k)
        ref[(*index, slice(ys, ys + 1), slice(None))] = value[3:4]
        ref[(*index, slice(ys + 7, ys + 8), slice(None))] = value[2:3]
    else:
        ref, index = target(tile[0], tile[1])
        ref[(*index, slice(8 * tile[2], 8 * tile[2] + 8), slice(None))] = value


def force_edges_kernel(full, ya, yb, send_a, send_b):
    place = Place()
    _, rows, ys, _ = full.shape
    h = HALO
    for send, first in ((send_a, place.odd), (send_b, jnp.logical_not(place.odd))):

        def at(k, first=first):
            return jnp.where(first, h - 1 - k, rows - h + k)

        def halo(c, k, at=at):
            a, b = ya[c * rows + at(k)], yb[c * rows + at(k)]
            return place.up(a, b), place.low(a, b)

        for t, tile in enumerate(edge_list()):
            put_tile(send, t, tile, lambda c, k, at=at: full[c, at(k)], halo)


def edges_kernel(p, ya, yb, *rest):
    send_a, send_b = rest[-2:]
    place = Place()
    rows = p.shape[0]
    h = HALO
    for send, first in ((send_a, place.odd), (send_b, jnp.logical_not(place.odd))):

        def at(k, first=first):
            return jnp.where(first, h - 1 - k, rows - h + k)

        def halo(c, k, at=at):
            a, b = ya[at(k)], yb[at(k)]
            return place.up(a, b), place.low(a, b)

        for t, tile in enumerate(face_list()):
            put_tile(send, t, tile, lambda c, k, at=at: p[at(k)], halo)


class Rows:
    def __init__(self, early, late, first, end):
        self.early, self.late, self.first, self.end = early, late, first, end

    def __getitem__(self, index):
        r = index[-1] if isinstance(index, tuple) else index
        mine = not isinstance(r, int) or not self.first <= r < self.end
        return (self.late if mine else self.early)[index]


def spans(lo, hi, total):
    full = [(s, total - 1 - s) for s in range(SWEEPS)] + [(HALO, total - HALO)]
    inner = [(lo + s, hi - s) for s in range(SWEEPS)] + [(lo + SWEEPS, hi - SWEEPS + 1)]
    inner = [i if i[0] < i[1] else (f[0], f[0]) for f, i in zip(full, inner)]
    return full, inner


def outside(full, inner, side):
    return range(full[0], inner[0]) if side == "low" else range(inner[1], full[1])


def on_side(near, body):
    odd = Place().odd
    pl.when(odd)(lambda: body("low" if near else "high"))
    pl.when(jnp.logical_not(odd))(lambda: body("high" if near else "low"))


def update(source, b, w, kx, ky, kz, target, r):
    keep = 1.0 - OMEGA
    here_x, past_x, here_y, here_z = kx[r], kx[r - 1], ky[r], kz[r]
    for c in range(3):
        u = source[c, r]
        near = here_x * source[c, r + 1] + past_x * source[c, r - 1]
        near = near + here_y * up_y(u) + down_y(here_y * u)
        near = near + here_z * up_z(u) + down_z(here_z * u)
        target[c, r] = keep * u + (b[c, r] + w[c, r] * near)


def diverge(v, r):
    vy, vz = v[1, r], v[2, r]
    lane = lax.broadcasted_iota(jnp.int32, vz.shape, 1)
    out = v[0, r - 1] - v[0, r]
    out = out + (down_y(vy) - vy)
    return out + (jnp.where(lane == 0, 0.0, down_z(vz)) - vz)


def emit_early(emit, near_side, full, inner, out_inner, out_near):
    for r in outside(full[SWEEPS], inner[SWEEPS], near_side):
        emit(r - HALO, out_near[r - HALO])
    rows_loop(inner[SWEEPS][0] - HALO, inner[SWEEPS][1] - HALO, lambda r: emit(r, out_inner[r]), 4)


def inner_solve(b, levels, out, inner, w, kx, ky, kz, step):
    source = b
    for s in range(1, SWEEPS):
        target = levels[s - 1]

        def one(r, source=source, target=target):
            update(source, b, w, kx, ky, kz, target, r)

        rows_loop(*inner[s], one, step)
        source = target

    def last(r):
        out[r - HALO] = diverge(source, r)

    rows_loop(*inner[SWEEPS], last, 2)


def outer_solve(side, b, levels, buffers, inner, full, w, kx, ky, kz, emit):
    source = b
    for s in range(1, SWEEPS):
        target = buffers[s - 1]
        for r in outside(full[s], inner[s], side):
            update(source, b, w, kx, ky, kz, target, r)
        source = Rows(levels[s - 1], target, *inner[s])
    for r in outside(full[SWEEPS], inner[SWEEPS], side):
        emit(r - HALO, diverge(source, r))


def emit_result(v_own, v_others, p_out, send_a, send_b, eta_at, sums=None):
    n = 1 + len(v_others)
    core = lax.axis_index("gz")
    odd = Place().odd_y
    h = HALO

    def emit(r, out):
        ys = v_own.shape[1]
        out = out[:ys]
        parts = split_z(out, core, n)
        v_own[r] = parts[0]
        for ref, part in zip(v_others, parts[1:]):
            ref[r] = part
        if p_out is not None:
            p = eta_at(r) * out
            p_out[r] = p
            send_a[r] = jnp.where(odd, p[:h], p[ys - h :])
            send_b[r] = jnp.where(odd, p[ys - h :], p[:h])
        if sums is not None:
            sums(r, out)

    return emit


def fold(value):
    total = value[:8]
    for k in range(1, value.shape[0] // 8):
        total = total + value[8 * k : 8 * k + 8]
    lanes = total[:, :LANES]
    for t in range(1, total.shape[1] // LANES):
        lanes = lanes + total[:, t * LANES : (t + 1) * LANES]
    return lanes


class Place:
    def __init__(self):
        chain = lax.axis_size("gx") * lax.axis_size("gz")
        self.x = lax.axis_index("gx") * lax.axis_size("gz") + lax.axis_index("gz")
        self.odd = lax.rem(self.x, 2) == 1
        self.below_x, self.above_x = self.x > 0, self.x < chain - 1
        y = lax.axis_index("gy")
        self.odd_y = lax.rem(y, 2) == 1
        self.below_y, self.above_y = y > 0, y < lax.axis_size("gy") - 1

    def up(self, a, b):
        return jnp.where(self.above_y, jnp.where(self.odd_y, b, a), 0.0)

    def low(self, a, b):
        return jnp.where(self.below_y, jnp.where(self.odd_y, a, b), 0.0)


def set_row(ref, index, row, a, b, place):
    ys, h = row.shape[0], a.shape[0]
    ref[(*index, slice(0, ys), slice(None))] = row
    ref[(*index, slice(ys, ys + h), slice(None))] = place.up(a, b)
    ref[(*index, slice(ys + h, ys + 2 * h), slice(None))] = place.low(a, b)


def coefs_at(sizes, place, slots, lanes, rows, ys, flags):
    h = HALO
    slot = lax.broadcasted_iota(jnp.int32, (slots, lanes), 0)
    at_y = lax.axis_index("gy") * ys + slot - jnp.where(slot >= ys + h, slots, 0)
    at_z = lax.broadcasted_iota(jnp.int32, (slots, lanes), 1)
    in_y = (at_y >= 0) & (at_y < sizes[1])
    y_up, y_low = at_y + 1 < sizes[1], at_y >= 1
    z_up, z_low = at_z + 1 < sizes[2], at_z >= 1
    wall = [jnp.where(flags[k] == 0, 1.0, 0.0).astype(F32) for k in range(6)]

    def coefs(r, mid, before, after, line, force_at, kx, ky, kz, w, b):
        at_x = place * rows - h + r
        x_up = jnp.full(mid.shape, at_x + 1, jnp.int32) < sizes[0]
        x_low = jnp.full(mid.shape, at_x, jnp.int32) >= 1
        inside = in_y & jnp.broadcast_to((at_x >= 0) & (at_x < sizes[0]), mid.shape)
        y_before = jnp.where(slot == ys + h, line, down_y(mid))
        sides = (
            (x_up, after, x_low, before),
            (y_up, up_y(mid), y_low, y_before),
            (z_up, up_z(mid), z_low, down_z(mid)),
        )
        diag = [jnp.zeros_like(mid) for _ in range(3)]
        for axis, (up_in, up, low_in, low) in enumerate(sides):
            up, low = 0.5 * (mid + up), 0.5 * (mid + low)
            (kx, ky, kz)[axis][r] = jnp.where(up_in, up, 0.0)
            for c in range(3):
                low_wall = 1.0 if c == axis else wall[2 * axis]
                up_wall = 1.0 if c == axis else wall[2 * axis + 1]
                diag[c] = diag[c] + jnp.where(up_in, up, up_wall * mid)
                diag[c] = diag[c] + jnp.where(low_in, low, low_wall * mid)
        for c in range(3):
            weight = jnp.where(inside, OMEGA / diag[c], 0.0)
            w[c, r] = weight
            b[c, r] = weight * force_at(c)

    return coefs


def first_inner(sizes, full, ya, yb, flags, kx, ky, kz, w, b, *rest):
    levels, (out, force, eta, line) = rest[: SWEEPS - 1], rest[SWEEPS - 1 :]
    fields, rows, ys, lanes = full.shape
    h = HALO
    place = Place()
    slots, total = ys + 2 * h, rows + 2 * h
    for c in range(fields):

        def one(r, c=c):
            to, index = (force, (c, r + h)) if c < 3 else (eta, (r + h,))
            set_row(to, index, full[c, r], ya[c * rows + r], yb[c * rows + r], place)

        rows_loop(0, rows, one, 4)
    for q in range(rows // 4):
        block = place.low(ya[fields * rows + q], yb[fields * rows + q])
        for k in range(4):
            line[h + 4 * q + k] = block[k : k + 1]
    coefs = coefs_at(sizes, place.x, slots, lanes, rows, ys, flags)

    def at(r):
        coefs(r, eta[r], eta[r - 1], eta[r + 1], line[r], lambda c: force[c, r], kx, ky, kz, w, b)

    _, inner = spans(h + 1, h + rows - 1, total)
    rows_loop(*inner[0], at, 1)
    inner_solve(b, levels, out, inner, w, kx, ky, kz, 3)


def first_side(n, sizes, near, *refs):
    count = 10 + SWEEPS
    full, ya, yb, xs, flags, *early = refs[:count]
    kx0, ky0, kz0, w0, b0, *levels, out0 = early
    if near:
        kx, ky, kz, w, out, *scratch = refs[count:]
    else:
        out_near, refs = refs[count], refs[count + 1 :]
        v_own, v_others, refs = refs[0], refs[1:n], refs[n:]
        p_out, send_a, send_b, kx, ky, kz, w, *scratch = refs
    force, eta, line, b, *buffers = scratch
    fields, rows, ys, lanes = full.shape
    h = HALO
    place = Place()
    slots, total = ys + 2 * h, rows + 2 * h
    ranges, inner = spans(h + 1, h + rows - 1, total)
    coefs = coefs_at(sizes, place.x, slots, lanes, rows, ys, flags)

    def body(side):
        todo = outside((0, total), inner[0], side)
        for r in sorted({min(max(q + d, h), h + rows - 1) for q in todo for d in (-1, 0, 1)}):
            k = r - h
            for c in range(fields):
                to, index = (force, (c, r)) if c < 3 else (eta, (r + 1,))
                set_row(to, index, full[c, k], ya[c * rows + k], yb[c * rows + k], place)
            block = fields * rows + k // 4
            line[r] = place.low(ya[block], yb[block])[k % 4 : k % 4 + 1]
        low = side == "low"
        blank = jnp.zeros((slots, lanes), F32)
        for k in range(h):
            line[k if low else h + rows + k] = jnp.ones((1, lanes), F32)
            for c in range(3):
                force[c, k if low else total - 1 - k] = blank
        for k in range(-1 if low else 0, h):
            eta[1 + k if low else total - k] = blank + 1.0

        def target(c, k):
            if c < 3:
                return force, (c, k if low else total - 1 - k)
            return eta, (1 + k if low else total - k,)

        for t, tile in enumerate(edge_list()):
            if low or tile[0] == "pack" or tile[1] >= 0:
                take_tile(tile, xs[t], ys, target)
        for r in todo:
            after = eta[min(r + 2, total)]
            coefs(r, eta[r + 1], eta[r], after, line[r], lambda c: force[c, r], kx, ky, kz, w, b)
        early_late = [(kx0, kx), (ky0, ky), (kz0, kz), (w0, w), (b0, b)]
        kxs, kys, kzs, ws, bs = (Rows(e, f, *inner[0]) for e, f in early_late)
        if near:

            def emit(r, value):
                out[r] = value

            outer_solve(side, bs, levels, buffers, inner, ranges, ws, kxs, kys, kzs, emit)
        else:
            emit = emit_result(v_own, v_others, p_out, send_a, send_b, lambda r: full[3, r])
            outer_solve(side, bs, levels, buffers, inner, ranges, ws, kxs, kys, kzs, emit)
            emit_early(emit, "high" if low else "low", ranges, inner, out0, out_near)

    on_side(near, body)


def join_kernel(total, rows, *refs):
    inner_refs, near_refs, far_refs, outs = (refs[4 * k : 4 * k + 4] for k in range(4))
    _, inner = spans(HALO + 1, HALO + rows - 1, total)

    def carry(source, r):
        for k in range(3):
            outs[k][r] = source[k][r]
        for c in range(3):
            outs[3][c, r] = source[3][c, r]

    rows_loop(*inner[0], lambda r: carry(inner_refs, r), 2)
    for near, source in ((True, near_refs), (False, far_refs)):

        def body(side, source=source):
            for r in outside((0, total), inner[0], side):
                carry(source, r)

        on_side(near, body)


def next_inner(extra, p_in, ya, yb, kx, ky, kz, w, *rest):
    p, b, *rest = rest[extra:]
    levels, out = rest[: SWEEPS - 1], rest[SWEEPS - 1]
    rows = p_in.shape[0]
    h = HALO
    place = Place()

    def fill(r):
        set_row(p, (r + h,), p_in[r], ya[r], yb[r], place)

    rows_loop(0, rows, fill, 4)
    _, inner = spans(h, h + rows - 1, rows + 2 * h)
    rows_loop(*inner[0], lambda r: grads(p, w, b, r), 16)
    inner_solve(b, levels, out, inner, w, kx, ky, kz, 16)


def grads(p, w, b, r):
    mid = p[r]
    lanes = mid.shape[1]
    lane = lax.broadcasted_iota(jnp.int32, mid.shape, 1)
    b[0, r] = w[0, r] * (p[r + 1] - mid)
    b[1, r] = w[1, r] * (up_y(mid) - mid)
    b[2, r] = w[2, r] * (jnp.where(lane == lanes - 1, 0.0, up_z(mid)) - mid)


def next_side(n, near, last, p_in, xs, kx, ky, kz, w, p0, b0, *refs):
    levels, refs = refs[: SWEEPS - 1], refs[SWEEPS - 1 :]
    if near:
        out, *scratch = refs
    else:
        full, out0, out_near, refs = refs[0], refs[1], refs[2], refs[3:]
        sums = p_out = send_a = send_b = None
        if last:
            partials, refs = refs[:ITERS], refs[ITERS:]
        v_own, v_others, refs = refs[0], refs[1:n], refs[n:]
        if last:
            moment, acc, refs = v_others[-1].at[p_in.shape[0]], refs[-1], refs[:-1]
            acc[...] = jnp.zeros_like(acc)

            def sums(r, v):
                acc[...] = acc[...] + v * p_in[r]
        else:
            p_out, send_a, send_b, *refs = refs
        scratch = refs
    p, b, *buffers = scratch
    rows, ys, _ = p_in.shape
    h = HALO
    total = rows + 2 * h
    place = Place()
    ranges, inner = spans(h, h + rows - 1, total)

    def body(side):
        low = side == "low"
        blank = jnp.zeros(p.shape[1:], F32)
        for k in range(h):
            p[k if low else total - 1 - k] = blank
        for t, tile in enumerate(face_list()):
            value = xs[t]
            if not near:
                value = jnp.where(place.below_x if low else place.above_x, value, 0.0)
            take_tile(tile, value, ys, lambda c, k: (p, (k if low else total - 1 - k,)))
        ps = Rows(p0, p, h, h + rows)
        for r in outside(ranges[0], inner[0], side):
            grads(ps, w, b, r)
        bs = Rows(b0, b, *inner[0])
        if near:

            def emit(r, value):
                out[r] = value

            outer_solve(side, bs, levels, buffers, inner, ranges, w, kx, ky, kz, emit)
        else:
            emit = emit_result(v_own, v_others, p_out, send_a, send_b, lambda r: full[3, r], sums)
            outer_solve(side, bs, levels, buffers, inner, ranges, w, kx, ky, kz, emit)
            emit_early(emit, "high" if low else "low", ranges, inner, out0, out_near)

    on_side(near, body)
    if not near and last:
        moment[...] = jnp.zeros_like(moment)
        at = 0
        for ref in partials:
            for k in range(ref.shape[0]):
                moment[at : at + 1, :] = jnp.sum(ref[k], 0, keepdims=True)
                at += 1
        moment[at : at + 1, :] = jnp.sum(fold(acc[...]), 0, keepdims=True)


def moments_kernel(n, step, *refs):
    moment, acc = refs[-2:]
    p, refs = refs[0], refs[1:-2]
    before, refs = (refs[0], refs[1:]) if step else (None, refs)
    groups = [refs[k * n : (k + 1) * n] for k in range(step + 1)]
    core = lax.axis_index("gz")
    acc[...] = jnp.zeros_like(acc)

    def one(r):
        v = join_own([q[r] for q in groups[-1]], core)
        others = ([before[r]] if step else []) + [p[r], v]
        others += [join_own([q[r] for q in group], core) for group in groups[:-1]]
        for k, other in enumerate(others):
            acc[k] = acc[k] + v * other

    rows_loop(0, p.shape[0], one, 4)
    for k in range(acc.shape[0]):
        moment[k] = fold(acc[k])


def two_sum(a, b):
    s = a + b
    t = s - a
    return s, (a - (s - t)) + (b - t)


def quick(a, b):
    s = a + b
    return s, b - (s - a)


def halves(a):
    t = 4097.0 * a
    high = t - (t - a)
    return high, a - high


def two_prod(a, b):
    p = a * b
    ah, al = halves(a)
    bh, bl = halves(b)
    return p, ((ah * bh - p) + ah * bl + al * bh) + al * bl


def add(a, b):
    s, e = two_sum(a[0], b[0])
    return quick(s, e + (a[1] + b[1]))


def mul(a, b):
    p, e = two_prod(a[0], b[0])
    return quick(p, e + (a[0] * b[1] + a[1] * b[0]))


def neg(a):
    return -a[0], -a[1]


def div(a, b):
    q = a[0] / b[0]
    r = add(a, neg(mul((q, jnp.zeros_like(q)), b)))
    q2 = r[0] / b[0]
    return quick(q, q2)


def twice(a):
    return 2.0 * a[0], 2.0 * a[1]


def last_kernel(n, cells, sums, eta, *refs):
    own = refs[: 4 * n]
    pressure, residual, norms = refs[4 * n :]
    core = lax.axis_index("gz")
    pair = (sums[0], sums[1])
    for shift in (64, 32, 16, 8, 4, 2, 1):
        pair = add(pair, tuple(pltpu.roll(x, shift, 1) for x in pair))
    item = [(pair[0][k : k + 1], pair[1][k : k + 1]) for k in range(12)]
    m0, n00, m1, m2, n11, n01, m3, m4, n22, n02, n12, m5 = item
    one = (jnp.ones_like(m0[0]), jnp.zeros_like(m0[0]))
    a0 = div(m0, m1)
    c11 = neg(a0)
    g1 = mul(c11, add(m1, mul(c11, m2)))
    b0 = div(g1, m0)
    d10, d11 = add(one, b0), c11
    a1 = div(g1, mul(d11, add(mul(d10, m2), mul(d11, m3))))
    c21 = add(c11, neg(mul(a1, d10)))
    c22 = neg(mul(a1, d11))
    g2 = mul(c22, add(m2, add(mul(c21, m3), mul(c22, m4))))
    b1 = div(g2, g1)
    d20 = add(one, mul(b1, d10))
    d21 = add(c21, mul(b1, d11))
    d22 = c22
    a2 = div(g2, mul(d22, add(mul(d20, m3), add(mul(d21, m4), mul(d22, m5)))))
    p0 = add(a0, add(mul(a1, d10), mul(a2, d20)))[0]
    p1 = add(mul(a1, d11), mul(a2, d21))[0]
    p2 = mul(a2, d22)[0]
    r1 = add(c21, neg(mul(a2, d20)))[0]
    r2 = add(c22, neg(mul(a2, d21)))[0]
    r3 = -p2
    norm1 = add(n00, mul(c11, add(twice(n01), mul(c11, n11))))
    norm2 = add(n00, mul(c21, add(twice(n01), mul(c21, n11))))
    norm2 = add(norm2, mul(c22, add(twice(n02), add(mul(twice(c21), n12), mul(c22, n22)))))
    for k, value in enumerate((n00, norm1, norm2)):
        norms[k] = (value[0] / cells)[0, 0]
    rows = own[0].shape[0]
    for j in range(n):
        base = lax.rem(core - j + n, n) * rows
        v0, v1, v2, v3 = (own[k * n + j] for k in range(4))

        def one_row(r, base=base, v0=v0, v1=v1, v2=v2, v3=v3):
            x0, x1, x2, x3 = v0[r], v1[r], v2[r], v3[r]
            pressure[base + r] = eta[base + r] * (p0 * x0 + p1 * x1 + p2 * x2)
            residual[base + r] = (x0 + r1 * x1) + (r2 * x2 + r3 * x3)

        rows_loop(0, rows, one_row, 4)


def add_pairs(a, b):
    s, e = two_sum(a[0], b[0])
    return jnp.stack([s, e + (a[1] + b[1])])


def sum_along(pair, axis, n, stride=1):
    count = n // stride
    if count < 2:
        return pair
    terms = [pair]
    for k in range(1, count):
        moves = [(i, (i + k * stride) % n) for i in range(n)]
        terms.append(lax.ppermute(pair, axis, moves))
    me = lax.axis_index(axis) // stride
    terms = [pick(terms, lax.rem(me - j + count, count)) for j in range(count)]
    while len(terms) > 1:
        rest = terms[len(terms) // 2 * 2 :]
        terms = [add_pairs(a, b) for a, b in zip(terms[::2], terms[1::2])] + rest
    return terms[0]


def per_device(nx, ny, nz, force, phase, table, flags):
    h = HALO
    wide, ys, lanes = phase.shape
    rows = wide // nz
    zs = lanes * nz
    sizes = (wide * nx, ys * ny, zs)
    slots, total = ys + 2 * h, rows + 2 * h
    cells = float(sizes[0] * sizes[1] * sizes[2])
    chain = nx * nz

    core = lax.axis_index("gz")
    starts = [lax.rem(core + j, nz) * rows for j in range(nz)]
    forces = [lax.dynamic_slice_in_dim(force, start, rows, 1) for start in starts]
    slices = [lax.dynamic_slice_in_dim(phase, start, rows, 0) for start in starts]
    forces = forces[:1] + [core_shift(forces[j], nz, j) for j in range(1, nz)]
    phases = slices[:1] + [core_shift(slices[j], nz, j) for j in range(1, nz)]
    full, ya, yb = call(
        functools.partial(gather_kernel, nz),
        [
            sds(4, rows, ys, zs),
            sds(4 * rows + rows // 4, h, zs),
            sds(4 * rows + rows // 4, h, zs),
        ],
        (table, *forces, *phases),
        [SMEM] + [VMEM] * (2 * nz),
        name="gather",
    )
    ya, yb = exchange_y(ya, yb, ny, nz)
    edge = sds(len(edge_list()), 8, zs)
    xa, xb = call(force_edges_kernel, [edge, edge], (full, ya, yb), name="force_edges")
    xa, xb = exchange_x(xa, xb, chain)

    v_shape = [sds(rows, ys, lanes)] * nz
    sent = [sds(rows, ys, zs), sds(rows, h, zs), sds(rows, h, zs)]
    scalar, vector = sds(total, slots, zs), sds(3, total, slots, zs)
    field = pltpu.VMEM((3, total, slots, zs), F32)
    line = pltpu.VMEM((total, 1, zs), F32)
    heavy = 4 * 10**7
    early = call(
        functools.partial(first_inner, sizes),
        [scalar] * 3 + [vector] * (1 + SWEEPS) + [sds(rows, slots, zs)],
        (full, ya, yb, flags),
        [VMEM] * 3 + [SMEM],
        [field, pltpu.VMEM((total, slots, zs), F32), line],
        heavy,
        "first_inner",
    )
    scratch = [field, pltpu.VMEM((total + 1, slots, zs), F32), line] + [field] * SWEEPS
    result = sds(rows, slots, zs)
    near = call(
        functools.partial(first_side, nz, sizes, True),
        [scalar] * 3 + [vector, result],
        (full, ya, yb, xa, flags, *early),
        [VMEM] * 4 + [SMEM] + [VMEM] * len(early),
        scratch,
        heavy // 2,
        "first_near",
    )
    outs = call(
        functools.partial(first_side, nz, sizes, False),
        v_shape + sent + [scalar] * 3 + [vector],
        (full, ya, yb, xb, flags, *early, near[-1]),
        [VMEM] * 4 + [SMEM] + [VMEM] * (len(early) + 1),
        scratch,
        heavy // 2,
        "first",
    )
    coefs = call(
        functools.partial(join_kernel, total, rows),
        [scalar] * 3 + [vector],
        (*early[:4], *near[:4], *outs[nz + 3 :]),
        name="join",
    )
    vs, ps, moments = [list(outs[:nz])], [outs[nz]], []
    eta = call(
        functools.partial(eta_kernel, nz),
        sds(*phase.shape),
        (table, outs[nz + 1], *slices),
        [SMEM] + [VMEM] * (nz + 1),
        name="eta",
    )
    ya, yb = outs[nz + 1 : nz + 3]
    placed = []
    for step in range(1, ITERS + 1):
        last = step == ITERS
        p, v = ps[-1], vs[-1]
        placed.append([v[0]] + [core_shift(v[j], nz, j) for j in range(1, nz)])
        count = 2 if step == 1 else 2 + step
        moments.append(
            call(
                functools.partial(moments_kernel, nz, step - 1),
                [sds(count, 8, LANES)],
                (p, *ps[:-1][-1:], *[q for v in vs for q in v]),
                None,
                [pltpu.VMEM((count, ys, zs), F32)],
                name="moments",
            )[0]
        )
        ya, yb = exchange_y(ya, yb, ny, nz)
        edge = sds(len(face_list()), 8, zs)
        xa, xb = call(edges_kernel, [edge, edge], (p, ya, yb, moments[-1]), name="edges")
        xa, xb = exchange_x(xa, xb, chain)
        early = call(
            functools.partial(next_inner, nz - 1),
            [scalar] + [vector] * SWEEPS + [sds(rows, slots, zs)],
            (p, ya, yb, *coefs, *placed[-1][1:]),
            None,
            (),
            heavy,
            "next_inner",
        )
        scratch = [pltpu.VMEM((total, slots, zs), F32)] + [field] * SWEEPS
        near = call(
            functools.partial(next_side, nz, True, last),
            [result],
            (p, xa, *coefs, *early[:-1]),
            None,
            scratch,
            heavy // 4,
            "next_near",
        )
        joint = v_shape[:-1] + [sds(rows + 1, ys, lanes)]
        outs = call(
            functools.partial(next_side, nz, False, last),
            joint if last else v_shape + sent,
            (p, xb, *coefs, *early[:-1], full, early[-1], *near, *(moments if last else ())),
            None,
            scratch + ([pltpu.VMEM((ys, zs), F32)] if last else []),
            heavy // 4,
            "next",
        )
        vs.append(list(outs[:nz]))
        if not last:
            ps.append(outs[nz])
            ya, yb = outs[nz + 1 : nz + 3]

    v = vs[-1]
    moved = [v[0]] + [core_shift(v[j], nz, j) for j in range(1, nz)]
    placed.append(moved)
    mine, theirs = v[-1][rows], moved[-1][rows]
    if nz > 2:
        theirs = lax.ppermute(mine, "gz", [(k, k ^ 1) for k in range(nz)])
    pair = jnp.stack(two_sum(mine, theirs))
    pair = sum_along(pair, "gz", nz, 2)
    pair = sum_along(sum_along(pair, "gx", nx), "gy", ny)
    pressure, residual, norms = call(
        functools.partial(last_kernel, nz, cells),
        [sds(*phase.shape), sds(*phase.shape), sds(ITERS)],
        (pair, eta, *[q for v in placed for q in v]),
        name="last",
        out_specs=[VMEM, VMEM, SMEM],
    )
    return pressure, residual, norms


def solution(mesh):
    placed = (P(None, "gx", "gy", "gz"), P("gx", "gy", "gz"), P(), P())
    return jax.shard_map(
        functools.partial(per_device, mesh.shape["gx"], mesh.shape["gy"], mesh.shape["gz"]),
        mesh=mesh,
        in_specs=placed,
        out_specs=(P("gx", "gy", "gz"), P("gx", "gy", "gz"), P()),
        check_vma=False,
    )
```

```python
import functools

import jax
import jax.numpy as jnp
from jax import lax
from jax.experimental import pallas as pl
from jax.experimental.pallas import tpu as pltpu
from jax.sharding import PartitionSpec as P


ITERS = 3
SWEEPS = 4
OMEGA = 0.8
HALO = 4
LANES = 128
F32 = jnp.float32

VMEM = pl.BlockSpec(memory_space=pltpu.VMEM)
SMEM = pl.BlockSpec(memory_space=pltpu.SMEM)


def sds(*shape):
    return jax.ShapeDtypeStruct(shape, F32)


def call(kernel, outs, ins, specs=None, scratch=(), flops=10**6, out_specs=None):
    return pl.pallas_call(
        kernel,
        out_shape=outs,
        in_specs=specs or [VMEM] * len(ins),
        out_specs=out_specs or jax.tree.map(lambda _: VMEM, outs),
        scratch_shapes=list(scratch),
        compiler_params=pltpu.CompilerParams(vmem_limit_bytes=24 * 2**20),
        cost_estimate=pl.CostEstimate(flops=flops, bytes_accessed=2**20, transcendentals=0),
    )(*ins)


def pick(items, index):
    value = items[0]
    for k in range(1, len(items)):
        value = jnp.where(index == k, items[k], value)
    return value


def split_z(value, core, n):
    blocks = [value[..., t * LANES : (t + 1) * LANES] for t in range(n)]
    return [pick(blocks, lax.rem(core + j, n)) for j in range(n)]


def join_own(parts, core):
    n = len(parts)
    return jnp.concatenate([pick(parts, lax.rem(t - core + n, n)) for t in range(n)], -1)


def join_received(parts, core):
    n = len(parts)
    return jnp.concatenate([pick(parts, lax.rem(core - t + n, n)) for t in range(n)], -1)


def up_y(row):
    return pltpu.roll(row, row.shape[0] - 1, 0)


def down_y(row):
    return pltpu.roll(row, 1, 0)


def up_z(row):
    return pltpu.roll(row, row.shape[1] - 1, 1)


def down_z(row):
    return pltpu.roll(row, 1, 1)


def rows_loop(start, stop, body, step=3):
    count = stop - start
    whole = count // step

    def chunk(i, carry):
        for k in range(step):
            body(start + i * step + k)
        return carry

    if whole > 1:
        lax.fori_loop(0, whole, chunk, 0)
        rest = start + whole * step
    else:
        rest = start
    for r in range(rest, stop):
        body(r)


def exchange_y(a, b, ny, nz):
    even = [(i, i ^ 1) for i in range(ny)]
    odd = []
    for y in range(ny):
        for z in range(nz):
            other = (y + (1 if y % 2 else -1), z) if 0 < y < ny - 1 else (y, z ^ 1)
            odd.append((y * nz + z, other[0] * nz + other[1]))
    return lax.ppermute(a, "gy", even), lax.ppermute(b, ("gy", "gz"), odd)


def exchange_x(a, b, n):
    even = [(i, i ^ 1) for i in range(n)]
    odd = [(i, (i + (1 if i % 2 else -1)) % n) for i in range(n)]
    b = lax.ppermute(b, ("gx", "gz"), odd)
    a = lax.ppermute(a, ("gx", "gz"), even)
    return a, b


def core_shift(value, n, j):
    return lax.ppermute(value, "gz", [(i, (i + j) % n) for i in range(n)])


def lookup(ids, table):
    eta = jnp.zeros(ids.shape, F32)
    for level in range(table.shape[0]):
        eta = jnp.where(ids == level, table[level], eta)
    return eta


def eta_kernel(n, table, after, *refs):
    slices, eta = refs[:n], refs[n]
    rows = slices[0].shape[0]
    for j in range(n):
        base = lax.rem(lax.axis_index("gz") + j, n) * rows

        def one(r, j=j, base=base):
            eta[base + r] = lookup(slices[j][r], table)

        rows_loop(0, rows, one, 4)


def gather_kernel(n, table, *refs):
    forces, phases = refs[:n], refs[n : 2 * n]
    full, send_a, send_b = refs[2 * n :]
    core = lax.axis_index("gz")
    odd = Place().odd_y
    fields, rows, ys, _ = full.shape
    h = HALO

    for c in range(fields):

        def one(r, c=c):
            row = join_received([q[c, r] for q in forces] if c < 3 else [q[r] for q in phases], core)
            row = row if c < 3 else lookup(row, table)
            full[c, r] = row
            send_a[c * rows + r] = jnp.where(odd, row[:h], row[ys - h :])
            send_b[c * rows + r] = jnp.where(odd, row[ys - h :], row[:h])

        rows_loop(0, rows, one, 16 if c == 3 else 4)
    for r in range(rows):
        line = full[3, r, ys - h - 1 : ys - h, :]
        send_a[fields * rows + r // 4, r % 4 : r % 4 + 1, :] = line
        send_b[fields * rows + r // 4, r % 4 : r % 4 + 1, :] = line


def edge_list():
    tiles = []
    for c in range(4):
        far = 1 if c in (1, 2) else 0
        tiles += [(c, k, q) for k in range(far, HALO) for q in range(2)]
        tiles += [(c, 3, 2), ("pack", c, 2, 1)] if c < 3 else [(c, 3, 2), (c, 2, 2), ("pack", c, 1, 0)]
    return tiles + [(3, -1, 0), (3, -1, 1)]


def face_list():
    return [(0, k, q) for k in range(HALO) for q in range(2)] + [(0, 3, 2), ("pack", 0, 2, 1)]


def put_tile(send, t, tile, row, halo):
    h = HALO
    if tile[0] == "pack":
        _, c, j, k = tile
        (up, low), (up_k, low_k) = halo(c, j), halo(c, k)
        send[t, 0:2, :] = up[0:2]
        send[t, 2:3, :] = low_k[h - 1 :]
        send[t, 3:4, :] = up_k[0:1]
        send[t, 4:6, :] = low[0:2]
        send[t, 6:8, :] = low[h - 2 :]
    elif tile[2] < 2:
        send[t] = row(tile[0], tile[1])[8 * tile[2] : 8 * tile[2] + 8]
    else:
        up, low = halo(tile[0], tile[1])
        send[t, :h, :] = up
        send[t, h:, :] = low


def take_tile(tile, value, ys, target):
    if tile[0] == "pack":
        _, c, j, k = tile
        ref, index = target(c, j)
        ref[(*index, slice(ys, ys + 8), slice(None))] = value
        ref, index = target(c, k)
        ref[(*index, slice(ys, ys + 1), slice(None))] = value[3:4]
        ref[(*index, slice(ys + 7, ys + 8), slice(None))] = value[2:3]
    else:
        ref, index = target(tile[0], tile[1])
        ref[(*index, slice(8 * tile[2], 8 * tile[2] + 8), slice(None))] = value


def force_edges_kernel(full, ya, yb, send_a, send_b):
    place = Place()
    _, rows, _, _ = full.shape
    h = HALO
    for send, first in ((send_a, place.odd), (send_b, jnp.logical_not(place.odd))):

        def at(k, first=first):
            return jnp.where(first, h - 1 - k, rows - h + k)

        def halo(c, k, at=at):
            a, b = ya[c * rows + at(k)], yb[c * rows + at(k)]
            return place.up(a, b), place.low(a, b)

        for t, tile in enumerate(edge_list()):
            put_tile(send, t, tile, lambda c, k, at=at: full[c, at(k)], halo)


def edges_kernel(near, p, ya, yb, *rest):
    send = rest[-1]
    place = Place()
    first = place.odd if near else jnp.logical_not(place.odd)
    rows = p.shape[0]
    h = HALO

    def at(k):
        return jnp.where(first, h - 1 - k, rows - h + k)

    def halo(c, k):
        a, b = ya[at(k)], yb[at(k)]
        return place.up(a, b), place.low(a, b)

    for t, tile in enumerate(face_list()):
        put_tile(send, t, tile, lambda c, k: p[at(k)], halo)


class Rows:
    def __init__(self, early, late, first, end):
        self.early, self.late, self.first, self.end = early, late, first, end

    def __getitem__(self, index):
        r = index[-1] if isinstance(index, tuple) else index
        mine = not isinstance(r, int) or not self.first <= r < self.end
        return (self.late if mine else self.early)[index]


def spans(lo, hi, total):
    full = [(s, total - 1 - s) for s in range(SWEEPS)] + [(HALO, total - HALO)]
    inner = [(lo + s, hi - s) for s in range(SWEEPS)] + [(lo + SWEEPS, hi - SWEEPS + 1)]
    inner = [i if i[0] < i[1] else (f[0], f[0]) for f, i in zip(full, inner)]
    return full, inner


def outside(full, inner, side):
    return range(full[0], inner[0]) if side == "low" else range(inner[1], full[1])


def on_side(near, body):
    odd = Place().odd
    pl.when(odd)(lambda: body("low" if near else "high"))
    pl.when(jnp.logical_not(odd))(lambda: body("high" if near else "low"))


def update(source, b, w, kx, ky, kz, target, r):
    keep = 1.0 - OMEGA
    here_x, past_x, here_y, here_z = kx[r], kx[r - 1], ky[r], kz[r]
    for c in range(3):
        u = source[c, r]
        near = here_x * source[c, r + 1] + past_x * source[c, r - 1]
        near = near + here_y * up_y(u) + down_y(here_y * u)
        near = near + here_z * up_z(u) + down_z(here_z * u)
        target[c, r] = keep * u + (b[c, r] + w[c, r] * near)


def diverge(v, r):
    vy, vz = v[1, r], v[2, r]
    lane = lax.broadcasted_iota(jnp.int32, vz.shape, 1)
    out = v[0, r - 1] - v[0, r]
    out = out + (down_y(vy) - vy)
    return out + (jnp.where(lane == 0, 0.0, down_z(vz)) - vz)


def emit_early(emit, near_side, full, inner, out_inner, out_near):
    for r in outside(full[SWEEPS], inner[SWEEPS], near_side):
        emit(r - HALO, out_near[r - HALO])
    rows_loop(inner[SWEEPS][0] - HALO, inner[SWEEPS][1] - HALO, lambda r: emit(r, out_inner[r]), 4)


def inner_solve(b, levels, out, inner, w, kx, ky, kz, step):
    source = b
    for s in range(1, SWEEPS):
        target = levels[s - 1]

        def one(r, source=source, target=target):
            update(source, b, w, kx, ky, kz, target, r)

        rows_loop(*inner[s], one, step)
        source = target

    def last(r):
        out[r - HALO] = diverge(source, r)

    rows_loop(*inner[SWEEPS], last, 2)


def outer_solve(side, b, levels, buffers, inner, full, w, kx, ky, kz, emit):
    source = b
    for s in range(1, SWEEPS):
        target = buffers[s - 1]
        for r in outside(full[s], inner[s], side):
            update(source, b, w, kx, ky, kz, target, r)
        source = Rows(levels[s - 1], target, *inner[s])
    for r in outside(full[SWEEPS], inner[SWEEPS], side):
        emit(r - HALO, diverge(source, r))


def emit_result(v_own, v_others, p_out, send_a, send_b, eta_at, sums=None):
    n = 1 + len(v_others)
    core = lax.axis_index("gz")
    odd = Place().odd_y
    h = HALO

    def emit(r, out):
        ys = v_own.shape[1]
        out = out[:ys]
        parts = split_z(out, core, n)
        v_own[r] = parts[0]
        for ref, part in zip(v_others, parts[1:]):
            ref[r] = part
        if p_out is not None:
            p = eta_at(r) * out
            p_out[r] = p
            send_a[r] = jnp.where(odd, p[:h], p[ys - h :])
            send_b[r] = jnp.where(odd, p[ys - h :], p[:h])
        if sums is not None:
            sums(r, out)

    return emit


def fold(value):
    total = value[:8]
    for k in range(1, value.shape[0] // 8):
        total = total + value[8 * k : 8 * k + 8]
    lanes = total[:, :LANES]
    for t in range(1, total.shape[1] // LANES):
        lanes = lanes + total[:, t * LANES : (t + 1) * LANES]
    return lanes


class Place:
    def __init__(self):
        chain = lax.axis_size("gx") * lax.axis_size("gz")
        self.x = lax.axis_index("gx") * lax.axis_size("gz") + lax.axis_index("gz")
        self.odd = lax.rem(self.x, 2) == 1
        self.below_x, self.above_x = self.x > 0, self.x < chain - 1
        y = lax.axis_index("gy")
        self.odd_y = lax.rem(y, 2) == 1
        self.below_y, self.above_y = y > 0, y < lax.axis_size("gy") - 1

    def up(self, a, b):
        return jnp.where(self.above_y, jnp.where(self.odd_y, b, a), 0.0)

    def low(self, a, b):
        return jnp.where(self.below_y, jnp.where(self.odd_y, a, b), 0.0)


def set_row(ref, index, row, a, b, place):
    ys, h = row.shape[0], a.shape[0]
    ref[(*index, slice(0, ys), slice(None))] = row
    ref[(*index, slice(ys, ys + h), slice(None))] = place.up(a, b)
    ref[(*index, slice(ys + h, ys + 2 * h), slice(None))] = place.low(a, b)


def coefs_at(sizes, place, slots, lanes, rows, ys, flags):
    h = HALO
    slot = lax.broadcasted_iota(jnp.int32, (slots, lanes), 0)
    at_y = lax.axis_index("gy") * ys + slot - jnp.where(slot >= ys + h, slots, 0)
    at_z = lax.broadcasted_iota(jnp.int32, (slots, lanes), 1)
    in_y = (at_y >= 0) & (at_y < sizes[1])
    y_up, y_low = at_y + 1 < sizes[1], at_y >= 1
    z_up, z_low = at_z + 1 < sizes[2], at_z >= 1
    wall = [jnp.where(flags[k] == 0, 1.0, 0.0).astype(F32) for k in range(6)]

    def coefs(r, mid, before, after, line, force_at, kx, ky, kz, w, b):
        at_x = place * rows - h + r
        x_up = jnp.full(mid.shape, at_x + 1, jnp.int32) < sizes[0]
        x_low = jnp.full(mid.shape, at_x, jnp.int32) >= 1
        inside = in_y & jnp.broadcast_to((at_x >= 0) & (at_x < sizes[0]), mid.shape)
        y_before = jnp.where(slot == ys + h, line, down_y(mid))
        sides = (
            (x_up, after, x_low, before),
            (y_up, up_y(mid), y_low, y_before),
            (z_up, up_z(mid), z_low, down_z(mid)),
        )
        diag = [jnp.zeros_like(mid) for _ in range(3)]
        for axis, (up_in, up, low_in, low) in enumerate(sides):
            up, low = 0.5 * (mid + up), 0.5 * (mid + low)
            (kx, ky, kz)[axis][r] = jnp.where(up_in, up, 0.0)
            for c in range(3):
                low_wall = 1.0 if c == axis else wall[2 * axis]
                up_wall = 1.0 if c == axis else wall[2 * axis + 1]
                diag[c] = diag[c] + jnp.where(up_in, up, up_wall * mid)
                diag[c] = diag[c] + jnp.where(low_in, low, low_wall * mid)
        for c in range(3):
            weight = jnp.where(inside, OMEGA / diag[c], 0.0)
            w[c, r] = weight
            b[c, r] = weight * force_at(c)

    return coefs


def first_inner(sizes, full, ya, yb, flags, kx, ky, kz, w, b, *rest):
    levels, (out, force, eta, line) = rest[: SWEEPS - 1], rest[SWEEPS - 1 :]
    fields, rows, ys, lanes = full.shape
    h = HALO
    place = Place()
    slots, total = ys + 2 * h, rows + 2 * h
    for c in range(fields):

        def one(r, c=c):
            to, index = (force, (c, r + h)) if c < 3 else (eta, (r + h,))
            set_row(to, index, full[c, r], ya[c * rows + r], yb[c * rows + r], place)

        rows_loop(0, rows, one, 4)
    for q in range(rows // 4):
        block = place.low(ya[fields * rows + q], yb[fields * rows + q])
        for k in range(4):
            line[h + 4 * q + k] = block[k : k + 1]
    coefs = coefs_at(sizes, place.x, slots, lanes, rows, ys, flags)

    def at(r):
        coefs(r, eta[r], eta[r - 1], eta[r + 1], line[r], lambda c: force[c, r], kx, ky, kz, w, b)

    _, inner = spans(h + 1, h + rows - 1, total)
    rows_loop(*inner[0], at, 1)
    inner_solve(b, levels, out, inner, w, kx, ky, kz, 3)


def first_side(n, sizes, near, *refs):
    count = 10 + SWEEPS
    full, ya, yb, xs, flags, *early = refs[:count]
    kx0, ky0, kz0, w0, b0, *levels, out0 = early
    if near:
        kx, ky, kz, w, out, *scratch = refs[count:]
    else:
        out_near, refs = refs[count], refs[count + 1 :]
        v_own, v_others, refs = refs[0], refs[1:n], refs[n:]
        p_out, send_a, send_b, kx, ky, kz, w, *scratch = refs
    force, eta, line, b, *buffers = scratch
    fields, rows, ys, lanes = full.shape
    h = HALO
    place = Place()
    slots, total = ys + 2 * h, rows + 2 * h
    ranges, inner = spans(h + 1, h + rows - 1, total)
    coefs = coefs_at(sizes, place.x, slots, lanes, rows, ys, flags)

    def body(side):
        todo = outside((0, total), inner[0], side)
        for r in sorted({min(max(q + d, h), h + rows - 1) for q in todo for d in (-1, 0, 1)}):
            k = r - h
            for c in range(fields):
                to, index = (force, (c, r)) if c < 3 else (eta, (r + 1,))
                set_row(to, index, full[c, k], ya[c * rows + k], yb[c * rows + k], place)
            block = fields * rows + k // 4
            line[r] = place.low(ya[block], yb[block])[k % 4 : k % 4 + 1]
        low = side == "low"
        blank = jnp.zeros((slots, lanes), F32)
        for k in range(h):
            line[k if low else h + rows + k] = jnp.ones((1, lanes), F32)
            for c in range(3):
                force[c, k if low else total - 1 - k] = blank
        for k in range(-1 if low else 0, h):
            eta[1 + k if low else total - k] = blank + 1.0

        def target(c, k):
            if c < 3:
                return force, (c, k if low else total - 1 - k)
            return eta, (1 + k if low else total - k,)

        for t, tile in enumerate(edge_list()):
            if low or tile[0] == "pack" or tile[1] >= 0:
                take_tile(tile, xs[t], ys, target)
        for r in todo:
            after = eta[min(r + 2, total)]
            coefs(r, eta[r + 1], eta[r], after, line[r], lambda c: force[c, r], kx, ky, kz, w, b)
        early_late = [(kx0, kx), (ky0, ky), (kz0, kz), (w0, w), (b0, b)]
        kxs, kys, kzs, ws, bs = (Rows(e, f, *inner[0]) for e, f in early_late)
        if near:

            def emit(r, value):
                out[r] = value

            outer_solve(side, bs, levels, buffers, inner, ranges, ws, kxs, kys, kzs, emit)
        else:
            emit = emit_result(v_own, v_others, p_out, send_a, send_b, lambda r: full[3, r])
            outer_solve(side, bs, levels, buffers, inner, ranges, ws, kxs, kys, kzs, emit)
            emit_early(emit, "high" if low else "low", ranges, inner, out0, out_near)

    on_side(near, body)


def join_kernel(total, rows, *refs):
    inner_refs, near_refs, far_refs, outs = (refs[4 * k : 4 * k + 4] for k in range(4))
    _, inner = spans(HALO + 1, HALO + rows - 1, total)

    def carry(source, r):
        for k in range(3):
            outs[k][r] = source[k][r]
        for c in range(3):
            outs[3][c, r] = source[3][c, r]

    rows_loop(*inner[0], lambda r: carry(inner_refs, r), 2)
    for near, source in ((True, near_refs), (False, far_refs)):

        def body(side, source=source):
            for r in outside((0, total), inner[0], side):
                carry(source, r)

        on_side(near, body)


def next_inner(extra, p_in, ya, yb, kx, ky, kz, w, *rest):
    p, b, *rest = rest[extra:]
    levels, out = rest[: SWEEPS - 1], rest[SWEEPS - 1]
    rows = p_in.shape[0]
    h = HALO
    place = Place()

    def fill(r):
        set_row(p, (r + h,), p_in[r], ya[r], yb[r], place)

    rows_loop(0, rows, fill, 4)
    _, inner = spans(h, h + rows - 1, rows + 2 * h)
    rows_loop(*inner[0], lambda r: grads(p, w, b, r), 16)
    inner_solve(b, levels, out, inner, w, kx, ky, kz, 16)


def grads(p, w, b, r):
    mid = p[r]
    lanes = mid.shape[1]
    lane = lax.broadcasted_iota(jnp.int32, mid.shape, 1)
    b[0, r] = w[0, r] * (p[r + 1] - mid)
    b[1, r] = w[1, r] * (up_y(mid) - mid)
    b[2, r] = w[2, r] * (jnp.where(lane == lanes - 1, 0.0, up_z(mid)) - mid)


def next_side(n, near, last, p_in, xs, kx, ky, kz, w, p0, b0, *refs):
    levels, refs = refs[: SWEEPS - 1], refs[SWEEPS - 1 :]
    if near:
        out, *scratch = refs
    else:
        full, out0, out_near, refs = refs[0], refs[1], refs[2], refs[3:]
        sums = p_out = send_a = send_b = None
        if last:
            partials, refs = refs[:ITERS], refs[ITERS:]
        v_own, v_others, refs = refs[0], refs[1:n], refs[n:]
        if last:
            moment, acc, refs = v_others[-1].at[p_in.shape[0]], refs[-1], refs[:-1]
            acc[...] = jnp.zeros_like(acc)

            def sums(r, v):
                acc[...] = acc[...] + v * p_in[r]
        else:
            p_out, send_a, send_b, *refs = refs
        scratch = refs
    p, b, *buffers = scratch
    rows, ys, _ = p_in.shape
    h = HALO
    total = rows + 2 * h
    place = Place()
    ranges, inner = spans(h, h + rows - 1, total)

    def body(side):
        low = side == "low"
        blank = jnp.zeros(p.shape[1:], F32)
        for k in range(h):
            p[k if low else total - 1 - k] = blank
        for t, tile in enumerate(face_list()):
            value = xs[t]
            if not near:
                value = jnp.where(place.below_x if low else place.above_x, value, 0.0)
            take_tile(tile, value, ys, lambda c, k: (p, (k if low else total - 1 - k,)))
        ps = Rows(p0, p, h, h + rows)
        for r in outside(ranges[0], inner[0], side):
            grads(ps, w, b, r)
        bs = Rows(b0, b, *inner[0])
        if near:

            def emit(r, value):
                out[r] = value

            outer_solve(side, bs, levels, buffers, inner, ranges, w, kx, ky, kz, emit)
        else:
            emit = emit_result(v_own, v_others, p_out, send_a, send_b, lambda r: full[3, r], sums)
            outer_solve(side, bs, levels, buffers, inner, ranges, w, kx, ky, kz, emit)
            emit_early(emit, "high" if low else "low", ranges, inner, out0, out_near)

    on_side(near, body)
    if not near and last:
        moment[...] = jnp.zeros_like(moment)
        at = 0
        for ref in partials:
            for k in range(ref.shape[0]):
                moment[at : at + 1, :] = jnp.sum(ref[k], 0, keepdims=True)
                at += 1
        moment[at : at + 1, :] = jnp.sum(fold(acc[...]), 0, keepdims=True)


def moments_kernel(n, step, *refs):
    moment, acc = refs[-2:]
    p, refs = refs[0], refs[1:-2]
    before, refs = (refs[0], refs[1:]) if step else (None, refs)
    groups = [refs[k * n : (k + 1) * n] for k in range(step + 1)]
    core = lax.axis_index("gz")
    acc[...] = jnp.zeros_like(acc)

    def one(r):
        v = join_own([q[r] for q in groups[-1]], core)
        others = ([before[r]] if step else []) + [p[r], v]
        others += [join_own([q[r] for q in group], core) for group in groups[:-1]]
        for k, other in enumerate(others):
            acc[k] = acc[k] + v * other

    rows_loop(0, p.shape[0], one, 4)
    for k in range(acc.shape[0]):
        moment[k] = fold(acc[k])


def two_sum(a, b):
    s = a + b
    t = s - a
    return s, (a - (s - t)) + (b - t)


def quick(a, b):
    s = a + b
    return s, b - (s - a)


def halves(a):
    t = 4097.0 * a
    high = t - (t - a)
    return high, a - high


def two_prod(a, b):
    p = a * b
    ah, al = halves(a)
    bh, bl = halves(b)
    return p, ((ah * bh - p) + ah * bl + al * bh) + al * bl


def add(a, b):
    s, e = two_sum(a[0], b[0])
    return quick(s, e + (a[1] + b[1]))


def mul(a, b):
    p, e = two_prod(a[0], b[0])
    return quick(p, e + (a[0] * b[1] + a[1] * b[0]))


def neg(a):
    return -a[0], -a[1]


def div(a, b):
    q = a[0] / b[0]
    r = add(a, neg(mul((q, jnp.zeros_like(q)), b)))
    q2 = r[0] / b[0]
    return quick(q, q2)


def twice(a):
    return 2.0 * a[0], 2.0 * a[1]


def last_kernel(n, cells, sums, eta, *refs):
    own = refs[: 4 * n]
    pressure, residual, norms = refs[4 * n :]
    core = lax.axis_index("gz")
    pair = (sums[0], sums[1])
    for shift in (64, 32, 16, 8, 4, 2, 1):
        pair = add(pair, tuple(pltpu.roll(x, shift, 1) for x in pair))
    item = [(pair[0][k : k + 1], pair[1][k : k + 1]) for k in range(12)]
    m0, n00, m1, m2, n11, n01, m3, m4, n22, n02, n12, m5 = item
    one = (jnp.ones_like(m0[0]), jnp.zeros_like(m0[0]))
    a0 = div(m0, m1)
    c11 = neg(a0)
    g1 = mul(c11, add(m1, mul(c11, m2)))
    b0 = div(g1, m0)
    d10, d11 = add(one, b0), c11
    a1 = div(g1, mul(d11, add(mul(d10, m2), mul(d11, m3))))
    c21 = add(c11, neg(mul(a1, d10)))
    c22 = neg(mul(a1, d11))
    g2 = mul(c22, add(m2, add(mul(c21, m3), mul(c22, m4))))
    b1 = div(g2, g1)
    d20 = add(one, mul(b1, d10))
    d21 = add(c21, mul(b1, d11))
    d22 = c22
    a2 = div(g2, mul(d22, add(mul(d20, m3), add(mul(d21, m4), mul(d22, m5)))))
    p0 = add(a0, add(mul(a1, d10), mul(a2, d20)))[0]
    p1 = add(mul(a1, d11), mul(a2, d21))[0]
    p2 = mul(a2, d22)[0]
    r1 = add(c21, neg(mul(a2, d20)))[0]
    r2 = add(c22, neg(mul(a2, d21)))[0]
    r3 = -p2
    norm1 = add(n00, mul(c11, add(twice(n01), mul(c11, n11))))
    norm2 = add(n00, mul(c21, add(twice(n01), mul(c21, n11))))
    norm2 = add(norm2, mul(c22, add(twice(n02), add(mul(twice(c21), n12), mul(c22, n22)))))
    for k, value in enumerate((n00, norm1, norm2)):
        norms[k] = (value[0] / cells)[0, 0]
    rows = own[0].shape[0]
    for j in range(n):
        base = lax.rem(core - j + n, n) * rows
        v0, v1, v2, v3 = (own[k * n + j] for k in range(4))

        def one_row(r, base=base, v0=v0, v1=v1, v2=v2, v3=v3):
            x0, x1, x2, x3 = v0[r], v1[r], v2[r], v3[r]
            pressure[base + r] = eta[base + r] * (p0 * x0 + p1 * x1 + p2 * x2)
            residual[base + r] = (x0 + r1 * x1) + (r2 * x2 + r3 * x3)

        rows_loop(0, rows, one_row, 4)


def add_pairs(a, b):
    s, e = two_sum(a[0], b[0])
    return jnp.stack([s, e + (a[1] + b[1])])


def sum_along(pair, axis, n, stride=1):
    count = n // stride
    if count < 2:
        return pair
    terms = [pair]
    for k in range(1, count):
        moves = [(i, (i + k * stride) % n) for i in range(n)]
        terms.append(lax.ppermute(pair, axis, moves))
    me = lax.axis_index(axis) // stride
    terms = [pick(terms, lax.rem(me - j + count, count)) for j in range(count)]
    while len(terms) > 1:
        rest = terms[len(terms) // 2 * 2 :]
        terms = [add_pairs(a, b) for a, b in zip(terms[::2], terms[1::2])] + rest
    return terms[0]


def per_device(nx, ny, nz, force, phase, table, flags):
    h = HALO
    wide, ys, lanes = phase.shape
    rows = wide // nz
    zs = lanes * nz
    sizes = (wide * nx, ys * ny, zs)
    slots, total = ys + 2 * h, rows + 2 * h
    cells = float(sizes[0] * sizes[1] * sizes[2])
    chain = nx * nz

    core = lax.axis_index("gz")
    starts = [lax.rem(core + j, nz) * rows for j in range(nz)]
    forces = [lax.dynamic_slice_in_dim(force, start, rows, 1) for start in starts]
    slices = [lax.dynamic_slice_in_dim(phase, start, rows, 0) for start in starts]
    forces = forces[:1] + [core_shift(forces[j], nz, j) for j in range(1, nz)]
    phases = slices[:1] + [core_shift(slices[j], nz, j) for j in range(1, nz)]
    full, ya, yb = call(
        functools.partial(gather_kernel, nz),
        [
            sds(4, rows, ys, zs),
            sds(4 * rows + rows // 4, h, zs),
            sds(4 * rows + rows // 4, h, zs),
        ],
        (table, *forces, *phases),
        [SMEM] + [VMEM] * (2 * nz),
    )
    ya, yb = exchange_y(ya, yb, ny, nz)
    edge = sds(len(edge_list()), 8, zs)
    xa, xb = call(force_edges_kernel, [edge, edge], (full, ya, yb))
    xa, xb = exchange_x(xa, xb, chain)

    v_shape = [sds(rows, ys, lanes)] * nz
    sent = [sds(rows, ys, zs), sds(rows, h, zs), sds(rows, h, zs)]
    scalar, vector = sds(total, slots, zs), sds(3, total, slots, zs)
    field = pltpu.VMEM((3, total, slots, zs), F32)
    line = pltpu.VMEM((total, 1, zs), F32)
    heavy = 4 * 10**7
    early = call(
        functools.partial(first_inner, sizes),
        [scalar] * 3 + [vector] * (1 + SWEEPS) + [sds(rows, slots, zs)],
        (full, ya, yb, flags),
        [VMEM] * 3 + [SMEM],
        [field, pltpu.VMEM((total, slots, zs), F32), line],
        heavy,
    )
    scratch = [field, pltpu.VMEM((total + 1, slots, zs), F32), line] + [field] * SWEEPS
    result = sds(rows, slots, zs)
    near = call(
        functools.partial(first_side, nz, sizes, True),
        [scalar] * 3 + [vector, result],
        (full, ya, yb, xa, flags, *early),
        [VMEM] * 4 + [SMEM] + [VMEM] * len(early),
        scratch,
        heavy // 2,
    )
    outs = call(
        functools.partial(first_side, nz, sizes, False),
        v_shape + sent + [scalar] * 3 + [vector],
        (full, ya, yb, xb, flags, *early, near[-1]),
        [VMEM] * 4 + [SMEM] + [VMEM] * (len(early) + 1),
        scratch,
        heavy // 2,
    )
    coefs = call(
        functools.partial(join_kernel, total, rows),
        [scalar] * 3 + [vector],
        (*early[:4], *near[:4], *outs[nz + 3 :]),
    )
    vs, ps, moments = [list(outs[:nz])], [outs[nz]], []
    eta = call(
        functools.partial(eta_kernel, nz),
        sds(*phase.shape),
        (table, outs[nz + 1], *slices),
        [SMEM] + [VMEM] * (nz + 1),
    )
    ya, yb = outs[nz + 1 : nz + 3]
    placed = []
    for step in range(1, ITERS + 1):
        last = step == ITERS
        p, v = ps[-1], vs[-1]
        placed.append([v[0]] + [core_shift(v[j], nz, j) for j in range(1, nz)])
        count = 2 if step == 1 else 2 + step
        moments.append(
            call(
                functools.partial(moments_kernel, nz, step - 1),
                [sds(count, 8, LANES)],
                (p, *ps[:-1][-1:], *[q for v in vs for q in v]),
                None,
                [pltpu.VMEM((count, ys, zs), F32)],
            )[0]
        )
        ya, yb = exchange_y(ya, yb, ny, nz)
        edge = sds(len(face_list()), 8, zs)
        far_edges = functools.partial(edges_kernel, False)
        xb = call(far_edges, edge, (p, ya, yb, moments[-1]))
        near_edges = functools.partial(edges_kernel, True)
        xa = call(near_edges, edge, (p, ya, yb, xb))
        xa, xb = exchange_x(xa, xb, chain)
        early = call(
            functools.partial(next_inner, nz - 1),
            [scalar] + [vector] * SWEEPS + [sds(rows, slots, zs)],
            (p, ya, yb, *coefs, *placed[-1][1:]),
            None,
            (),
            heavy,
        )
        scratch = [pltpu.VMEM((total, slots, zs), F32)] + [field] * SWEEPS
        near = call(
            functools.partial(next_side, nz, True, last),
            [result],
            (p, xa, *coefs, *early[:-1]),
            None,
            scratch,
            heavy // 4,
        )
        joint = v_shape[:-1] + [sds(rows + 1, ys, lanes)]
        outs = call(
            functools.partial(next_side, nz, False, last),
            joint if last else v_shape + sent,
            (p, xb, *coefs, *early[:-1], full, early[-1], *near, *(moments if last else ())),
            None,
            scratch + ([pltpu.VMEM((ys, zs), F32)] if last else []),
            heavy // 4,
        )
        vs.append(list(outs[:nz]))
        if not last:
            ps.append(outs[nz])
            ya, yb = outs[nz + 1 : nz + 3]

    v = vs[-1]
    moved = [v[0]] + [core_shift(v[j], nz, j) for j in range(1, nz)]
    placed.append(moved)
    mine, theirs = v[-1][rows], moved[-1][rows]
    if nz > 2:
        theirs = lax.ppermute(mine, "gz", [(k, k ^ 1) for k in range(nz)])
    pair = jnp.stack(two_sum(mine, theirs))
    pair = sum_along(pair, "gz", nz, 2)
    pair = sum_along(sum_along(pair, "gx", nx), "gy", ny)
    pressure, residual, norms = call(
        functools.partial(last_kernel, nz, cells),
        [sds(*phase.shape), sds(*phase.shape), sds(ITERS)],
        (pair, eta, *[q for v in placed for q in v]),
        out_specs=[VMEM, VMEM, SMEM],
    )
    return pressure, residual, norms


def solution(mesh):
    placed = (P(None, "gx", "gy", "gz"), P("gx", "gy", "gz"), P(), P())
    return jax.shard_map(
        functools.partial(per_device, mesh.shape["gx"], mesh.shape["gy"], mesh.shape["gz"]),
        mesh=mesh,
        in_specs=placed,
        out_specs=(P("gx", "gy", "gz"), P("gx", "gy", "gz"), P()),
        check_vma=False,
    )
```

```python
import functools

import jax
import jax.numpy as jnp
from jax import lax
from jax.experimental import pallas as pl
from jax.experimental.pallas import tpu as pltpu
from jax.sharding import PartitionSpec as P


ITERS = 3
SWEEPS = 4
OMEGA = 0.8
HALO = 4
LANES = 128
F32 = jnp.float32

VMEM = pl.BlockSpec(memory_space=pltpu.VMEM)
SMEM = pl.BlockSpec(memory_space=pltpu.SMEM)


def sds(*shape):
    return jax.ShapeDtypeStruct(shape, F32)


def call(kernel, outs, ins, specs=None, scratch=(), flops=10**6, out_specs=None):
    return pl.pallas_call(
        kernel,
        out_shape=outs,
        in_specs=specs or [VMEM] * len(ins),
        out_specs=out_specs or jax.tree.map(lambda _: VMEM, outs),
        scratch_shapes=list(scratch),
        compiler_params=pltpu.CompilerParams(vmem_limit_bytes=24 * 2**20),
        cost_estimate=pl.CostEstimate(flops=flops, bytes_accessed=2**20, transcendentals=0),
    )(*ins)


def pick(items, index):
    value = items[0]
    for k in range(1, len(items)):
        value = jnp.where(index == k, items[k], value)
    return value


def split_z(value, core, n):
    blocks = [value[..., t * LANES : (t + 1) * LANES] for t in range(n)]
    return [pick(blocks, lax.rem(core + j, n)) for j in range(n)]


def join_own(parts, core):
    n = len(parts)
    return jnp.concatenate([pick(parts, lax.rem(t - core + n, n)) for t in range(n)], -1)


def join_received(parts, core):
    n = len(parts)
    return jnp.concatenate([pick(parts, lax.rem(core - t + n, n)) for t in range(n)], -1)


def up_y(row):
    return pltpu.roll(row, row.shape[0] - 1, 0)


def down_y(row):
    return pltpu.roll(row, 1, 0)


def up_z(row):
    return pltpu.roll(row, row.shape[1] - 1, 1)


def down_z(row):
    return pltpu.roll(row, 1, 1)


def rows_loop(start, stop, body, step=3):
    count = stop - start
    whole = count // step

    def chunk(i, carry):
        for k in range(step):
            body(start + i * step + k)
        return carry

    if whole > 1:
        lax.fori_loop(0, whole, chunk, 0)
        rest = start + whole * step
    else:
        rest = start
    for r in range(rest, stop):
        body(r)


def exchange_y(a, b, ny, nz):
    even = [(i, i ^ 1) for i in range(ny)]
    odd = []
    for y in range(ny):
        for z in range(nz):
            other = (y + (1 if y % 2 else -1), z) if 0 < y < ny - 1 else (y, z ^ 1)
            odd.append((y * nz + z, other[0] * nz + other[1]))
    return lax.ppermute(a, "gy", even), lax.ppermute(b, ("gy", "gz"), odd)


def exchange_x(a, b, n):
    even = [(i, i ^ 1) for i in range(n)]
    odd = [(i, (i + (1 if i % 2 else -1)) % n) for i in range(n)]
    b = lax.ppermute(b, ("gx", "gz"), odd)
    a = lax.ppermute(a, ("gx", "gz"), even)
    return a, b


def core_shift(value, n, j):
    return lax.ppermute(value, "gz", [(i, (i + j) % n) for i in range(n)])


def lookup(ids, table):
    eta = jnp.zeros(ids.shape, F32)
    for level in range(table.shape[0]):
        eta = jnp.where(ids == level, table[level : level + 1, : ids.shape[1]], eta)
    return eta


def eta_kernel(n, table, after, *refs):
    slices, eta = refs[:n], refs[n]
    rows = slices[0].shape[0]
    for j in range(n):
        base = lax.rem(lax.axis_index("gz") + j, n) * rows

        def one(r, j=j, base=base):
            eta[base + r] = lookup(slices[j][r], table)

        rows_loop(0, rows, one, 4)


def gather_kernel(n, table, *refs):
    forces, phases = refs[:n], refs[n : 2 * n]
    full, send_a, send_b = refs[2 * n :]
    core = lax.axis_index("gz")
    odd = Place().odd_y
    fields, rows, ys, _ = full.shape
    h = HALO

    for c in range(fields):

        def one(r, c=c):
            row = join_received([q[c, r] for q in forces] if c < 3 else [q[r] for q in phases], core)
            row = row if c < 3 else lookup(row, table)
            full[c, r] = row
            send_a[c * rows + r] = jnp.where(odd, row[:h], row[ys - h :])
            send_b[c * rows + r] = jnp.where(odd, row[ys - h :], row[:h])

        rows_loop(0, rows, one, 16 if c == 3 else 4)
    for r in range(rows):
        line = full[3, r, ys - h - 1 : ys - h, :]
        send_a[fields * rows + r // 4, r % 4 : r % 4 + 1, :] = line
        send_b[fields * rows + r // 4, r % 4 : r % 4 + 1, :] = line


def edge_list():
    tiles = []
    for c in range(4):
        far = 1 if c in (1, 2) else 0
        tiles += [(c, k, q) for k in range(far, HALO) for q in range(2)]
        tiles += [(c, 3, 2), ("pack", c, 2, 1)] if c < 3 else [(c, 3, 2), (c, 2, 2), ("pack", c, 1, 0)]
    return tiles + [(3, -1, 0), (3, -1, 1)]


def face_list():
    return [(0, k, q) for k in range(HALO) for q in range(2)] + [(0, 3, 2), ("pack", 0, 2, 1)]


def put_tile(send, t, tile, row, halo):
    h = HALO
    if tile[0] == "pack":
        _, c, j, k = tile
        (up, low), (up_k, low_k) = halo(c, j), halo(c, k)
        send[t, 0:2, :] = up[0:2]
        send[t, 2:3, :] = low_k[h - 1 :]
        send[t, 3:4, :] = up_k[0:1]
        send[t, 4:6, :] = low[0:2]
        send[t, 6:8, :] = low[h - 2 :]
    elif tile[2] < 2:
        send[t] = row(tile[0], tile[1])[8 * tile[2] : 8 * tile[2] + 8]
    else:
        up, low = halo(tile[0], tile[1])
        send[t, :h, :] = up
        send[t, h:, :] = low


def take_tile(tile, value, ys, target):
    if tile[0] == "pack":
        _, c, j, k = tile
        ref, index = target(c, j)
        ref[(*index, slice(ys, ys + 8), slice(None))] = value
        ref, index = target(c, k)
        ref[(*index, slice(ys, ys + 1), slice(None))] = value[3:4]
        ref[(*index, slice(ys + 7, ys + 8), slice(None))] = value[2:3]
    else:
        ref, index = target(tile[0], tile[1])
        ref[(*index, slice(8 * tile[2], 8 * tile[2] + 8), slice(None))] = value


def force_edges_kernel(full, ya, yb, send_a, send_b):
    place = Place()
    _, rows, _, _ = full.shape
    h = HALO
    for send, first in ((send_a, place.odd), (send_b, jnp.logical_not(place.odd))):

        def at(k, first=first):
            return jnp.where(first, h - 1 - k, rows - h + k)

        def halo(c, k, at=at):
            a, b = ya[c * rows + at(k)], yb[c * rows + at(k)]
            return place.up(a, b), place.low(a, b)

        for t, tile in enumerate(edge_list()):
            put_tile(send, t, tile, lambda c, k, at=at: full[c, at(k)], halo)


def edges_kernel(near, p, ya, yb, *rest):
    send = rest[-1]
    place = Place()
    first = place.odd if near else jnp.logical_not(place.odd)
    rows = p.shape[0]
    h = HALO

    def at(k):
        return jnp.where(first, h - 1 - k, rows - h + k)

    def halo(c, k):
        a, b = ya[at(k)], yb[at(k)]
        return place.up(a, b), place.low(a, b)

    for t, tile in enumerate(face_list()):
        put_tile(send, t, tile, lambda c, k: p[at(k)], halo)


class Rows:
    def __init__(self, early, late, first, end):
        self.early, self.late, self.first, self.end = early, late, first, end

    def __getitem__(self, index):
        r = index[-1] if isinstance(index, tuple) else index
        mine = not isinstance(r, int) or not self.first <= r < self.end
        return (self.late if mine else self.early)[index]


def spans(lo, hi, total):
    full = [(s, total - 1 - s) for s in range(SWEEPS)] + [(HALO, total - HALO)]
    inner = [(lo + s, hi - s) for s in range(SWEEPS)] + [(lo + SWEEPS, hi - SWEEPS + 1)]
    inner = [i if i[0] < i[1] else (f[0], f[0]) for f, i in zip(full, inner)]
    return full, inner


def outside(full, inner, side):
    return range(full[0], inner[0]) if side == "low" else range(inner[1], full[1])


def on_side(near, body):
    odd = Place().odd
    pl.when(odd)(lambda: body("low" if near else "high"))
    pl.when(jnp.logical_not(odd))(lambda: body("high" if near else "low"))


def update(source, b, w, kx, ky, kz, target, r):
    keep = 1.0 - OMEGA
    here_x, past_x, here_y, here_z = kx[r], kx[r - 1], ky[r], kz[r]
    for c in range(3):
        u = source[c, r]
        near = here_x * source[c, r + 1] + past_x * source[c, r - 1]
        near = near + here_y * up_y(u) + down_y(here_y * u)
        near = near + here_z * up_z(u) + down_z(here_z * u)
        target[c, r] = keep * u + (b[c, r] + w[c, r] * near)


def diverge(v, r):
    vy, vz = v[1, r], v[2, r]
    lane = lax.broadcasted_iota(jnp.int32, vz.shape, 1)
    out = v[0, r - 1] - v[0, r]
    out = out + (down_y(vy) - vy)
    return out + (jnp.where(lane == 0, 0.0, down_z(vz)) - vz)


def emit_early(emit, near_side, full, inner, out_inner, out_near):
    for r in outside(full[SWEEPS], inner[SWEEPS], near_side):
        emit(r - HALO, out_near[r - HALO])
    rows_loop(inner[SWEEPS][0] - HALO, inner[SWEEPS][1] - HALO, lambda r: emit(r, out_inner[r]), 16)


def inner_solve(b, levels, out, inner, w, kx, ky, kz, step):
    source = b
    for s in range(1, SWEEPS):
        target = levels[s - 1]

        def one(r, source=source, target=target):
            update(source, b, w, kx, ky, kz, target, r)

        rows_loop(*inner[s], one, step)
        source = target

    def last(r):
        out[r - HALO] = diverge(source, r)

    rows_loop(*inner[SWEEPS], last, 2)


def outer_solve(side, b, levels, buffers, inner, full, w, kx, ky, kz, emit):
    source = b
    for s in range(1, SWEEPS):
        target = buffers[s - 1]
        for r in outside(full[s], inner[s], side):
            update(source, b, w, kx, ky, kz, target, r)
        source = Rows(levels[s - 1], target, *inner[s])
    for r in outside(full[SWEEPS], inner[SWEEPS], side):
        emit(r - HALO, diverge(source, r))


def emit_result(v_own, v_others, p_out, send_a, send_b, eta_at, sums=None):
    n = 1 + len(v_others)
    core = lax.axis_index("gz")
    odd = Place().odd_y
    h = HALO

    def emit(r, out):
        ys = v_own.shape[1]
        out = out[:ys]
        parts = split_z(out, core, n)
        v_own[r] = parts[0]
        for ref, part in zip(v_others, parts[1:]):
            ref[r] = part
        if p_out is not None:
            p = eta_at(r) * out
            p_out[r] = p
            send_a[r] = jnp.where(odd, p[:h], p[ys - h :])
            send_b[r] = jnp.where(odd, p[ys - h :], p[:h])
        if sums is not None:
            sums(r, out)

    return emit


def fold(value):
    total = value[:8]
    for k in range(1, value.shape[0] // 8):
        total = total + value[8 * k : 8 * k + 8]
    lanes = total[:, :LANES]
    for t in range(1, total.shape[1] // LANES):
        lanes = lanes + total[:, t * LANES : (t + 1) * LANES]
    return lanes


class Place:
    def __init__(self):
        chain = lax.axis_size("gx") * lax.axis_size("gz")
        self.x = lax.axis_index("gx") * lax.axis_size("gz") + lax.axis_index("gz")
        self.odd = lax.rem(self.x, 2) == 1
        self.below_x, self.above_x = self.x > 0, self.x < chain - 1
        y = lax.axis_index("gy")
        self.odd_y = lax.rem(y, 2) == 1
        self.below_y, self.above_y = y > 0, y < lax.axis_size("gy") - 1

    def up(self, a, b):
        return jnp.where(self.above_y, jnp.where(self.odd_y, b, a), 0.0)

    def low(self, a, b):
        return jnp.where(self.below_y, jnp.where(self.odd_y, a, b), 0.0)


def set_row(ref, index, row, a, b, place):
    ys, h = row.shape[0], a.shape[0]
    ref[(*index, slice(0, ys), slice(None))] = row
    ref[(*index, slice(ys, ys + h), slice(None))] = place.up(a, b)
    ref[(*index, slice(ys + h, ys + 2 * h), slice(None))] = place.low(a, b)


def coefs_at(sizes, place, slots, lanes, rows, ys, flags):
    h = HALO
    slot = lax.broadcasted_iota(jnp.int32, (slots, lanes), 0)
    at_y = lax.axis_index("gy") * ys + slot - jnp.where(slot >= ys + h, slots, 0)
    at_z = lax.broadcasted_iota(jnp.int32, (slots, lanes), 1)
    in_y = (at_y >= 0) & (at_y < sizes[1])
    y_up, y_low = at_y + 1 < sizes[1], at_y >= 1
    z_up, z_low = at_z + 1 < sizes[2], at_z >= 1
    wall = [flags[k : k + 1, :] for k in range(6)]

    def coefs(r, mid, before, after, line, force_at, kx, ky, kz, w, b):
        at_x = place * rows - h + r
        x_up = jnp.full(mid.shape, at_x + 1, jnp.int32) < sizes[0]
        x_low = jnp.full(mid.shape, at_x, jnp.int32) >= 1
        inside = in_y & jnp.broadcast_to((at_x >= 0) & (at_x < sizes[0]), mid.shape)
        y_before = jnp.where(slot == ys + h, line, down_y(mid))
        sides = (
            (x_up, after, x_low, before),
            (y_up, up_y(mid), y_low, y_before),
            (z_up, up_z(mid), z_low, down_z(mid)),
        )
        diag = [jnp.zeros_like(mid) for _ in range(3)]
        for axis, (up_in, up, low_in, low) in enumerate(sides):
            up, low = 0.5 * (mid + up), 0.5 * (mid + low)
            (kx, ky, kz)[axis][r] = jnp.where(up_in, up, 0.0)
            for c in range(3):
                low_wall = 1.0 if c == axis else wall[2 * axis]
                up_wall = 1.0 if c == axis else wall[2 * axis + 1]
                diag[c] = diag[c] + jnp.where(up_in, up, up_wall * mid)
                diag[c] = diag[c] + jnp.where(low_in, low, low_wall * mid)
        for c in range(3):
            weight = jnp.where(inside, OMEGA / diag[c], 0.0)
            w[c, r] = weight
            b[c, r] = weight * force_at(c)

    return coefs


def first_inner(sizes, full, ya, yb, flags, kx, ky, kz, w, b, *rest):
    levels, (out, force, eta, line) = rest[: SWEEPS - 1], rest[SWEEPS - 1 :]
    fields, rows, ys, lanes = full.shape
    h = HALO
    place = Place()
    slots, total = ys + 2 * h, rows + 2 * h
    for c in range(fields):

        def one(r, c=c):
            to, index = (force, (c, r + h)) if c < 3 else (eta, (r + h,))
            set_row(to, index, full[c, r], ya[c * rows + r], yb[c * rows + r], place)

        rows_loop(0, rows, one, 4)
    for q in range(rows // 4):
        block = place.low(ya[fields * rows + q], yb[fields * rows + q])
        for k in range(4):
            line[h + 4 * q + k] = block[k : k + 1]
    coefs = coefs_at(sizes, place.x, slots, lanes, rows, ys, flags)

    def at(r):
        coefs(r, eta[r], eta[r - 1], eta[r + 1], line[r], lambda c: force[c, r], kx, ky, kz, w, b)

    _, inner = spans(h + 1, h + rows - 1, total)
    rows_loop(*inner[0], at, 1)
    inner_solve(b, levels, out, inner, w, kx, ky, kz, 3)


def first_side(n, sizes, near, *refs):
    count = 10 + SWEEPS
    full, ya, yb, xs, flags, *early = refs[:count]
    kx0, ky0, kz0, w0, b0, *levels, out0 = early
    if near:
        kx, ky, kz, w, out, *scratch = refs[count:]
    else:
        out_near, refs = refs[count], refs[count + 1 :]
        v_own, v_others, refs = refs[0], refs[1:n], refs[n:]
        p_out, send_a, send_b, kx, ky, kz, w, *scratch = refs
    force, eta, line, b, *buffers = scratch
    fields, rows, ys, lanes = full.shape
    h = HALO
    place = Place()
    slots, total = ys + 2 * h, rows + 2 * h
    ranges, inner = spans(h + 1, h + rows - 1, total)
    coefs = coefs_at(sizes, place.x, slots, lanes, rows, ys, flags)

    def body(side):
        todo = outside((0, total), inner[0], side)
        for r in sorted({min(max(q + d, h), h + rows - 1) for q in todo for d in (-1, 0, 1)}):
            k = r - h
            for c in range(fields):
                to, index = (force, (c, r)) if c < 3 else (eta, (r + 1,))
                set_row(to, index, full[c, k], ya[c * rows + k], yb[c * rows + k], place)
            block = fields * rows + k // 4
            line[r] = place.low(ya[block], yb[block])[k % 4 : k % 4 + 1]
        low = side == "low"
        blank = jnp.zeros((slots, lanes), F32)
        for k in range(h):
            line[k if low else h + rows + k] = jnp.ones((1, lanes), F32)
            for c in range(3):
                force[c, k if low else total - 1 - k] = blank
        for k in range(-1 if low else 0, h):
            eta[1 + k if low else total - k] = blank + 1.0

        def target(c, k):
            if c < 3:
                return force, (c, k if low else total - 1 - k)
            return eta, (1 + k if low else total - k,)

        for t, tile in enumerate(edge_list()):
            if low or tile[0] == "pack" or tile[1] >= 0:
                take_tile(tile, xs[t], ys, target)
        for r in todo:
            after = eta[min(r + 2, total)]
            coefs(r, eta[r + 1], eta[r], after, line[r], lambda c: force[c, r], kx, ky, kz, w, b)
        early_late = [(kx0, kx), (ky0, ky), (kz0, kz), (w0, w), (b0, b)]
        kxs, kys, kzs, ws, bs = (Rows(e, f, *inner[0]) for e, f in early_late)
        if near:

            def emit(r, value):
                out[r] = value

            outer_solve(side, bs, levels, buffers, inner, ranges, ws, kxs, kys, kzs, emit)
        else:
            emit = emit_result(v_own, v_others, p_out, send_a, send_b, lambda r: full[3, r])
            outer_solve(side, bs, levels, buffers, inner, ranges, ws, kxs, kys, kzs, emit)
            emit_early(emit, "high" if low else "low", ranges, inner, out0, out_near)

    on_side(near, body)


def join_kernel(total, rows, *refs):
    inner_refs, near_refs, far_refs, outs = (refs[4 * k : 4 * k + 4] for k in range(4))
    _, inner = spans(HALO + 1, HALO + rows - 1, total)

    def carry(source, r):
        for k in range(3):
            outs[k][r] = source[k][r]
        for c in range(3):
            outs[3][c, r] = source[3][c, r]

    rows_loop(*inner[0], lambda r: carry(inner_refs, r), 2)
    for near, source in ((True, near_refs), (False, far_refs)):

        def body(side, source=source):
            for r in outside((0, total), inner[0], side):
                carry(source, r)

        on_side(near, body)


def next_inner(extra, p_in, ya, yb, kx, ky, kz, w, *rest):
    p, b, *rest = rest[extra:]
    levels, out = rest[: SWEEPS - 1], rest[SWEEPS - 1]
    rows = p_in.shape[0]
    h = HALO
    place = Place()

    def fill(r):
        set_row(p, (r + h,), p_in[r], ya[r], yb[r], place)

    rows_loop(0, rows, fill, 4)
    _, inner = spans(h, h + rows - 1, rows + 2 * h)
    rows_loop(*inner[0], lambda r: grads(p, w, b, r), 16)
    inner_solve(b, levels, out, inner, w, kx, ky, kz, 16)


def grads(p, w, b, r):
    mid = p[r]
    lanes = mid.shape[1]
    lane = lax.broadcasted_iota(jnp.int32, mid.shape, 1)
    b[0, r] = w[0, r] * (p[r + 1] - mid)
    b[1, r] = w[1, r] * (up_y(mid) - mid)
    b[2, r] = w[2, r] * (jnp.where(lane == lanes - 1, 0.0, up_z(mid)) - mid)


def next_side(n, near, last, p_in, xs, kx, ky, kz, w, p0, b0, *refs):
    levels, refs = refs[: SWEEPS - 1], refs[SWEEPS - 1 :]
    if near:
        out, *scratch = refs
    else:
        full, out0, out_near, refs = refs[0], refs[1], refs[2], refs[3:]
        sums = p_out = send_a = send_b = None
        if last:
            partials, refs = refs[:ITERS], refs[ITERS:]
        v_own, v_others, refs = refs[0], refs[1:n], refs[n:]
        if last:
            moment, acc, refs = v_others[-1].at[p_in.shape[0]], refs[-1], refs[:-1]
            acc[...] = jnp.zeros_like(acc)

            def sums(r, v):
                acc[...] = acc[...] + v * p_in[r]
        else:
            p_out, send_a, send_b, *refs = refs
        scratch = refs
    p, b, *buffers = scratch
    rows, ys, _ = p_in.shape
    h = HALO
    total = rows + 2 * h
    place = Place()
    ranges, inner = spans(h, h + rows - 1, total)

    def body(side):
        low = side == "low"
        blank = jnp.zeros(p.shape[1:], F32)
        for k in range(h):
            p[k if low else total - 1 - k] = blank
        for t, tile in enumerate(face_list()):
            value = xs[t]
            if not near:
                value = jnp.where(place.below_x if low else place.above_x, value, 0.0)
            take_tile(tile, value, ys, lambda c, k: (p, (k if low else total - 1 - k,)))
        ps = Rows(p0, p, h, h + rows)
        for r in outside(ranges[0], inner[0], side):
            grads(ps, w, b, r)
        bs = Rows(b0, b, *inner[0])
        if near:

            def emit(r, value):
                out[r] = value

            outer_solve(side, bs, levels, buffers, inner, ranges, w, kx, ky, kz, emit)
        else:
            emit = emit_result(v_own, v_others, p_out, send_a, send_b, lambda r: full[3, r], sums)
            outer_solve(side, bs, levels, buffers, inner, ranges, w, kx, ky, kz, emit)
            emit_early(emit, "high" if low else "low", ranges, inner, out0, out_near)

    on_side(near, body)
    if not near and last:
        moment[...] = jnp.zeros_like(moment)
        at = 0
        for ref in partials:
            for k in range(ref.shape[0]):
                moment[at : at + 1, :] = jnp.sum(ref[k], 0, keepdims=True)
                at += 1
        moment[at : at + 1, :] = jnp.sum(fold(acc[...]), 0, keepdims=True)


def moments_kernel(n, step, *refs):
    moment, acc = refs[-2:]
    p, refs = refs[0], refs[1:-2]
    before, refs = (refs[0], refs[1:]) if step else (None, refs)
    groups = [refs[k * n : (k + 1) * n] for k in range(step + 1)]
    core = lax.axis_index("gz")
    acc[...] = jnp.zeros_like(acc)

    def one(r):
        v = join_own([q[r] for q in groups[-1]], core)
        others = ([before[r]] if step else []) + [p[r], v]
        others += [join_own([q[r] for q in group], core) for group in groups[:-1]]
        for k, other in enumerate(others):
            acc[k] = acc[k] + v * other

    rows_loop(0, p.shape[0], one, 4)
    for k in range(acc.shape[0]):
        moment[k] = fold(acc[k])


def two_sum(a, b):
    s = a + b
    t = s - a
    return s, (a - (s - t)) + (b - t)


def quick(a, b):
    s = a + b
    return s, b - (s - a)


def halves(a):
    t = 4097.0 * a
    high = t - (t - a)
    return high, a - high


def two_prod(a, b):
    p = a * b
    ah, al = halves(a)
    bh, bl = halves(b)
    return p, ((ah * bh - p) + ah * bl + al * bh) + al * bl


def add(a, b):
    s, e = two_sum(a[0], b[0])
    return quick(s, e + (a[1] + b[1]))


def mul(a, b):
    p, e = two_prod(a[0], b[0])
    return quick(p, e + (a[0] * b[1] + a[1] * b[0]))


def neg(a):
    return -a[0], -a[1]


def div(a, b):
    q = a[0] / b[0]
    r = add(a, neg(mul((q, jnp.zeros_like(q)), b)))
    q2 = r[0] / b[0]
    return quick(q, q2)


def twice(a):
    return 2.0 * a[0], 2.0 * a[1]


def last_kernel(n, cells, sums, eta, *refs):
    own = refs[: 4 * n]
    pressure, residual, norms = refs[4 * n :]
    core = lax.axis_index("gz")
    pair = (sums[0], sums[1])
    for shift in (64, 32, 16, 8, 4, 2, 1):
        pair = add(pair, tuple(pltpu.roll(x, shift, 1) for x in pair))
    item = [(pair[0][k : k + 1], pair[1][k : k + 1]) for k in range(12)]
    m0, n00, m1, m2, n11, n01, m3, m4, n22, n02, n12, m5 = item
    one = (jnp.ones_like(m0[0]), jnp.zeros_like(m0[0]))
    a0 = div(m0, m1)
    c11 = neg(a0)
    g1 = mul(c11, add(m1, mul(c11, m2)))
    b0 = div(g1, m0)
    d10, d11 = add(one, b0), c11
    a1 = div(g1, mul(d11, add(mul(d10, m2), mul(d11, m3))))
    c21 = add(c11, neg(mul(a1, d10)))
    c22 = neg(mul(a1, d11))
    g2 = mul(c22, add(m2, add(mul(c21, m3), mul(c22, m4))))
    b1 = div(g2, g1)
    d20 = add(one, mul(b1, d10))
    d21 = add(c21, mul(b1, d11))
    d22 = c22
    a2 = div(g2, mul(d22, add(mul(d20, m3), add(mul(d21, m4), mul(d22, m5)))))
    p0 = add(a0, add(mul(a1, d10), mul(a2, d20)))[0]
    p1 = add(mul(a1, d11), mul(a2, d21))[0]
    p2 = mul(a2, d22)[0]
    r1 = add(c21, neg(mul(a2, d20)))[0]
    r2 = add(c22, neg(mul(a2, d21)))[0]
    r3 = -p2
    norm1 = add(n00, mul(c11, add(twice(n01), mul(c11, n11))))
    norm2 = add(n00, mul(c21, add(twice(n01), mul(c21, n11))))
    norm2 = add(norm2, mul(c22, add(twice(n02), add(mul(twice(c21), n12), mul(c22, n22)))))
    for k, value in enumerate((n00, norm1, norm2)):
        norms[k] = (value[0] / cells)[0, 0]
    rows = own[0].shape[0]
    for j in range(n):
        base = lax.rem(core - j + n, n) * rows
        v0, v1, v2, v3 = (own[k * n + j] for k in range(4))

        def one_row(r, base=base, v0=v0, v1=v1, v2=v2, v3=v3):
            x0, x1, x2, x3 = v0[r], v1[r], v2[r], v3[r]
            pressure[base + r] = eta[base + r] * (p0 * x0 + p1 * x1 + p2 * x2)
            residual[base + r] = (x0 + r1 * x1) + (r2 * x2 + r3 * x3)

        rows_loop(0, rows, one_row, 16)


def add_pairs(a, b):
    s, e = two_sum(a[0], b[0])
    return jnp.stack([s, e + (a[1] + b[1])])


def sum_along(pair, axis, n, stride=1):
    count = n // stride
    if count < 2:
        return pair
    terms = [pair]
    for k in range(1, count):
        moves = [(i, (i + k * stride) % n) for i in range(n)]
        terms.append(lax.ppermute(pair, axis, moves))
    me = lax.axis_index(axis) // stride
    terms = [pick(terms, lax.rem(me - j + count, count)) for j in range(count)]
    while len(terms) > 1:
        rest = terms[len(terms) // 2 * 2 :]
        terms = [add_pairs(a, b) for a, b in zip(terms[::2], terms[1::2])] + rest
    return terms[0]


def per_device(nx, ny, nz, force, phase, table, flags):
    h = HALO
    wide, ys, lanes = phase.shape
    rows = wide // nz
    zs = lanes * nz
    sizes = (wide * nx, ys * ny, zs)
    slots, total = ys + 2 * h, rows + 2 * h
    cells = float(sizes[0] * sizes[1] * sizes[2])
    chain = nx * nz

    table = jnp.broadcast_to(table[:, None], (table.shape[0], zs))
    flags = jnp.broadcast_to(jnp.where(flags == 0, 1.0, 0.0).astype(F32)[:, None], (6, zs))
    core = lax.axis_index("gz")
    starts = [lax.rem(core + j, nz) * rows for j in range(nz)]
    forces = [lax.dynamic_slice_in_dim(force, start, rows, 1) for start in starts]
    slices = [lax.dynamic_slice_in_dim(phase, start, rows, 0) for start in starts]
    forces = forces[:1] + [core_shift(forces[j], nz, j) for j in range(1, nz)]
    phases = slices[:1] + [core_shift(slices[j], nz, j) for j in range(1, nz)]
    full, ya, yb = call(
        functools.partial(gather_kernel, nz),
        [
            sds(4, rows, ys, zs),
            sds(4 * rows + rows // 4, h, zs),
            sds(4 * rows + rows // 4, h, zs),
        ],
        (table, *forces, *phases),
    )
    ya, yb = exchange_y(ya, yb, ny, nz)
    edge = sds(len(edge_list()), 8, zs)
    xa, xb = call(force_edges_kernel, [edge, edge], (full, ya, yb))
    xa, xb = exchange_x(xa, xb, chain)

    v_shape = [sds(rows, ys, lanes)] * nz
    sent = [sds(rows, ys, zs), sds(rows, h, zs), sds(rows, h, zs)]
    scalar, vector = sds(total, slots, zs), sds(3, total, slots, zs)
    field = pltpu.VMEM((3, total, slots, zs), F32)
    line = pltpu.VMEM((total, 1, zs), F32)
    heavy = 4 * 10**7
    early = call(
        functools.partial(first_inner, sizes),
        [scalar] * 3 + [vector] * (1 + SWEEPS) + [sds(rows, slots, zs)],
        (full, ya, yb, flags),
        None,
        [field, pltpu.VMEM((total, slots, zs), F32), line],
        heavy,
    )
    scratch = [field, pltpu.VMEM((total + 1, slots, zs), F32), line] + [field] * SWEEPS
    result = sds(rows, slots, zs)
    near = call(
        functools.partial(first_side, nz, sizes, True),
        [scalar] * 3 + [vector, result],
        (full, ya, yb, xa, flags, *early),
        None,
        scratch,
        heavy // 2,
    )
    outs = call(
        functools.partial(first_side, nz, sizes, False),
        v_shape + sent + [scalar] * 3 + [vector],
        (full, ya, yb, xb, flags, *early, near[-1]),
        None,
        scratch,
        heavy // 2,
    )
    coefs = call(
        functools.partial(join_kernel, total, rows),
        [scalar] * 3 + [vector],
        (*early[:4], *near[:4], *outs[nz + 3 :]),
    )
    vs, ps, moments = [list(outs[:nz])], [outs[nz]], []
    eta = call(functools.partial(eta_kernel, nz), sds(*phase.shape), (table, outs[nz + 1], *slices))
    ya, yb = outs[nz + 1 : nz + 3]
    placed = []
    for step in range(1, ITERS + 1):
        last = step == ITERS
        p, v = ps[-1], vs[-1]
        placed.append([v[0]] + [core_shift(v[j], nz, j) for j in range(1, nz)])
        count = 2 if step == 1 else 2 + step
        moments.append(
            call(
                functools.partial(moments_kernel, nz, step - 1),
                [sds(count, 8, LANES)],
                (p, *ps[:-1][-1:], *[q for v in vs for q in v]),
                None,
                [pltpu.VMEM((count, ys, zs), F32)],
            )[0]
        )
        ya, yb = exchange_y(ya, yb, ny, nz)
        edge = sds(len(face_list()), 8, zs)
        far_edges = functools.partial(edges_kernel, False)
        xb = call(far_edges, edge, (p, ya, yb, moments[-1]))
        near_edges = functools.partial(edges_kernel, True)
        xa = call(near_edges, edge, (p, ya, yb, xb))
        xa, xb = exchange_x(xa, xb, chain)
        early = call(
            functools.partial(next_inner, nz - 1),
            [scalar] + [vector] * SWEEPS + [sds(rows, slots, zs)],
            (p, ya, yb, *coefs, *placed[-1][1:]),
            None,
            (),
            heavy,
        )
        scratch = [pltpu.VMEM((total, slots, zs), F32)] + [field] * SWEEPS
        near = call(
            functools.partial(next_side, nz, True, last),
            [result],
            (p, xa, *coefs, *early[:-1]),
            None,
            scratch,
            heavy // 4,
        )
        joint = v_shape[:-1] + [sds(rows + 1, ys, lanes)]
        outs = call(
            functools.partial(next_side, nz, False, last),
            joint if last else v_shape + sent,
            (p, xb, *coefs, *early[:-1], full, early[-1], *near, *(moments if last else ())),
            None,
            scratch + ([pltpu.VMEM((ys, zs), F32)] if last else []),
            heavy // 4,
        )
        vs.append(list(outs[:nz]))
        if not last:
            ps.append(outs[nz])
            ya, yb = outs[nz + 1 : nz + 3]

    v = vs[-1]
    moved = [v[0]] + [core_shift(v[j], nz, j) for j in range(1, nz)]
    placed.append(moved)
    mine, theirs = v[-1][rows], moved[-1][rows]
    if nz > 2:
        theirs = lax.ppermute(mine, "gz", [(k, k ^ 1) for k in range(nz)])
    pair = jnp.stack(two_sum(mine, theirs))
    pair = sum_along(pair, "gz", nz, 2)
    pair = sum_along(sum_along(pair, "gx", nx), "gy", ny)
    pressure, residual, norms = call(
        functools.partial(last_kernel, nz, cells),
        [sds(*phase.shape), sds(*phase.shape), sds(ITERS)],
        (pair, eta, *[q for v in placed for q in v]),
        out_specs=[VMEM, VMEM, SMEM],
    )
    return pressure, residual, norms


def solution(mesh):
    placed = (P(None, "gx", "gy", "gz"), P("gx", "gy", "gz"), P(), P())
    return jax.shard_map(
        functools.partial(per_device, mesh.shape["gx"], mesh.shape["gy"], mesh.shape["gz"]),
        mesh=mesh,
        in_specs=placed,
        out_specs=(P("gx", "gy", "gz"), P("gx", "gy", "gz"), P()),
        check_vma=False,
    )
```
